256 devices in a mesh: ctx: 32 (over y, x, core), head: 8 (over z).
Axes of the slice: x: 4, y: 4, z: 8, core: 2. Of those that a mesh axis runs over, the one named last changes fastest.
Arguments:
- query_in: float32 [32768, 16, 128], P('ctx', 'head'), may hold values from -6 to 6
- key_in: float32 [32768, 16, 128], P('ctx', 'head'), may hold values from -6 to 6
- value_in: float32 [32768, 32, 128], P('ctx', 'head'), may hold values from -6 to 6
- gate_in: float32 [32768, 32, 128], P('ctx', 'head'), may hold values from -6 to 6
- log_gate: float32 [32, 32768], P('head', 'ctx'), may hold values from -1 to 0, as said below
- strength: float32 [32, 32768], P('head', 'ctx'), may hold values from 0.005 to 0.05
- query_conv: float32 [4, 16, 128], P(None, 'head'), may hold values from -3 to 3
- key_conv: float32 [4, 16, 128], P(None, 'head'), may hold values from -3 to 3
- value_conv: float32 [4, 32, 128], P(None, 'head'), may hold values from -3 to 3
- norm_gain: float32 [128], replicated, may hold values from 0.1 to 1.9
- out_weight: bfloat16 [4096, 2048], P('head'), may hold values from -0.09375 to 0.09375
Outputs:
- mixed: float32 [32768, 2048], P(('ctx', 'head'))
The draws below stay inside these ranges and needn't reach their ends.
Inputs may be any that keep to these rules, and one draw needn't show every extreme that they name: `log_gate`: the logarithm of head h's decay factor at a token.
All inputs are finite; a program needn't handle non-finite values.
Results may differ from the reference program's by a relative error of at most 0.015.
Values may be sent and summed in bfloat16 or wider, within the bound.
No kernel may reach another device: no remote copies, remote signals or barrier semaphores. Data moves between devices by JAX's collectives and lax.ppermute only.
A program may use at most 128 MiB of HBM per device.

```python
import math
import jax
import jax.numpy as jnp
from jax import lax

D = 2048
PAYLOAD_GROUPS = 32
KHEADS = 16
DK = 128
DV = 128
CONV = 4
SPAN = 64
STREAM_LENGTH = 32768
N_HEAD = 8


def draw_log_gate(key, part):
    attention_group_seed, position_seed, location_seed, contiguous_seed = jax.random.split(jax.random.fold_in(key, 17), 4)
    spread = jax.random.uniform(attention_group_seed, (PAYLOAD_GROUPS, 1), jnp.float32, 0.0, 1.0)
    log_rate = math.log(1.0 / 40.0) * (1.0 - spread) + math.log(0.1 / STREAM_LENGTH) * spread
    unmasked_result = -jnp.exp(log_rate) * jax.random.uniform(position_seed, (PAYLOAD_GROUPS, STREAM_LENGTH), jnp.float32, 0.5, 1.5)
    places = jax.random.randint(location_seed, (PAYLOAD_GROUPS, 4), 0, STREAM_LENGTH)
    positions = jnp.arange(STREAM_LENGTH, dtype=jnp.int32)
    zeroed_elements = jnp.any(positions[None, None, :] == places[:, :, None], axis=1)
    contiguous_erasure = jnp.log(jax.random.uniform(contiguous_seed, (PAYLOAD_GROUPS, STREAM_LENGTH), jnp.float32, 0.5, 0.8))
    return jnp.where(zeroed_elements, unmasked_result + contiguous_erasure, unmasked_result)


def levels(key, shape, cuts, least, largest):
    level = 1.0
    for axis_at, blocks in cuts:
        steps = jax.random.uniform(jax.random.fold_in(jax.random.fold_in(key, 6), axis_at), (blocks,), jnp.float32, least / len(cuts), largest / len(cuts))
        level = level * jnp.repeat(jnp.exp(steps), shape[axis_at] // blocks).reshape((-1,) + (1,) * (len(shape) - 1 - axis_at))
    return level


def bell_draw(stream_key, shape, scale, most, shards=(), kind=jnp.bfloat16):
    values = jax.random.normal(stream_key, shape, jnp.float32) * scale
    if len(shards) > 0:
        values = levels(stream_key, shape, shards, -0.22, 0.18) * values
    return jnp.clip(values, min=-most, max=most).astype(kind)


def setup_inputs(seed: int = 0) -> dict:
    splits = jax.random.split(jax.random.key(seed), 12)
    query_in = bell_draw(splits[0], (STREAM_LENGTH, KHEADS, DK), 1.0, 6.0, ((0, 32), (1, 8)), jnp.float32)
    key_in = bell_draw(splits[1], (STREAM_LENGTH, KHEADS, DK), 1.0, 6.0, ((0, 32), (1, 8)), jnp.float32)
    value_in = bell_draw(splits[2], (STREAM_LENGTH, PAYLOAD_GROUPS, DV), 1.0, 6.0, ((0, 32), (1, 8)), jnp.float32)
    gate_in = bell_draw(splits[3], (STREAM_LENGTH, PAYLOAD_GROUPS, DV), 1.0, 6.0, ((0, 32), (1, 8)), jnp.float32)
    log_gate = draw_log_gate(jax.random.fold_in(splits[11], 71), 0)
    strength = jnp.clip(jnp.exp(math.log(0.05) - 2.3025851 * jax.random.uniform(splits[5], (PAYLOAD_GROUPS, STREAM_LENGTH), jnp.float32) ** levels(splits[5], (PAYLOAD_GROUPS, STREAM_LENGTH), ((0, 8), (1, 32)), -0.2, 0.2)), 0.005, 0.05)
    query_conv = bell_draw(splits[6], (CONV, KHEADS, DK), CONV ** -0.5, 3.0, ((1, 8),), jnp.float32)
    key_conv = bell_draw(splits[7], (CONV, KHEADS, DK), CONV ** -0.5, 3.0, ((1, 8),), jnp.float32)
    value_conv = bell_draw(splits[8], (CONV, PAYLOAD_GROUPS, DV), CONV ** -0.5, 3.0, ((1, 8),), jnp.float32)
    norm_gain = jnp.clip(1.0 + 0.18 * jax.random.normal(splits[9], (DV,), jnp.float32), 0.1, 1.9)
    out_weight = bell_draw(splits[10], (PAYLOAD_GROUPS * DV, D), (PAYLOAD_GROUPS * DV) ** -0.5, 0.09375, ((0, 8),))
    return dict(query_in=query_in, key_in=key_in, value_in=value_in, gate_in=gate_in, log_gate=log_gate, strength=strength, query_conv=query_conv, key_conv=key_conv, value_conv=value_conv, norm_gain=norm_gain, out_weight=out_weight)


exact_precision = lax.Precision.HIGHEST
norm_epsilon = 1e-06

def causal_mix(current, previous, kernel):
    kernel_width = kernel.shape[0]
    token_count = current.shape[0]
    padded = jnp.concatenate([previous, current], axis=0)
    summed = jnp.zeros(current.shape, jnp.float32)
    for offset in range(kernel_width):
        summed = summed + kernel[offset] * padded[offset:offset + token_count]
    return jax.nn.silu(summed)

def unit_rows(matrix):
    return matrix * lax.rsqrt(lax.optimization_barrier(jnp.sum(matrix * matrix, axis=-1, keepdims=True)) + norm_epsilon)

def to_blocks(matrix, block_size):
    token_count, head_count, width_count = matrix.shape
    return matrix.reshape(token_count // block_size, block_size, head_count, width_count).transpose(0, 2, 1, 3)

def gate_blocks(matrix, block_size):
    head_count, token_count = matrix.shape
    return matrix.reshape(head_count, token_count // block_size, block_size).transpose(1, 0, 2)

def prepare(query_in, key_in, value_in, query_prev, key_prev, value_prev, query_conv, key_conv, value_conv, block_size):
    group_ratio = value_in.shape[1] // query_in.shape[1]
    queries = unit_rows(causal_mix(query_in, query_prev, query_conv)) * query_in.shape[2] ** (-0.5)
    key_rows = unit_rows(causal_mix(key_in, key_prev, key_conv))
    values = causal_mix(value_in, value_prev, value_conv)
    queries = jnp.repeat(queries, group_ratio, axis=1)
    key_rows = jnp.repeat(key_rows, group_ratio, axis=1)
    return (to_blocks(queries, block_size), to_blocks(key_rows, block_size), to_blocks(values, block_size))

def unit_inverse(mixing):
    block_size = mixing.shape[-1]
    identity_map = jnp.eye(block_size, dtype=jnp.float32)
    powered = -mixing
    inverse = identity_map + powered
    reach = 2
    while reach < block_size:
        powered = jnp.einsum('nhij,nhjk->nhik', powered, powered, precision=exact_precision)
        inverse = jnp.einsum('nhij,nhjk->nhik', inverse, identity_map + powered, precision=exact_precision)
        reach = reach * 2
    return inverse

def span_setup(queries, key_rows, values, log_gate, strength):
    cumulative = jnp.cumsum(log_gate, axis=-1)
    block_size = cumulative.shape[-1]
    row_index = lax.broadcasted_iota(jnp.int32, (block_size, block_size), 0)
    col_index = lax.broadcasted_iota(jnp.int32, (block_size, block_size), 1)
    lower_mask = row_index >= col_index
    strict_mask = row_index > col_index
    differences = cumulative[..., :, None] - cumulative[..., None, :]
    decay_table = jnp.exp(jnp.where(lower_mask, differences, -jnp.inf))
    key_inner = jnp.einsum('nhcd,nhmd->nhcm', key_rows, key_rows, precision=exact_precision)
    mixing = jnp.where(strict_mask, strength[..., :, None] * key_inner * decay_table, 0.0)
    scores = jnp.where(lower_mask, jnp.einsum('nhcd,nhmd->nhcm', queries, key_rows, precision=exact_precision) * decay_table, 0.0)
    inverse = unit_inverse(mixing)
    fresh_values = jnp.einsum('nhcm,nhmw->nhcw', inverse, strength[..., None] * values, precision=exact_precision)
    solved_keys = jnp.einsum('nhcm,nhmd->nhcd', inverse, (strength * jnp.exp(cumulative))[..., None] * key_rows, precision=exact_precision)
    lifted = jnp.exp(cumulative)[..., None] * queries
    carried = jnp.exp(cumulative[..., -1:] - cumulative)[..., None] * key_rows
    ending = jnp.exp(cumulative[..., -1])
    return (fresh_values, solved_keys, scores, lifted, carried, ending)

def run_spans(start_state, setup, with_outputs):

    def advance(carry_state, per_span):
        fresh_block, solved_block, score_block, lifted_block, carried_block, ending_block = per_span
        update = fresh_block - jnp.einsum('hcd,hdw->hcw', solved_block, carry_state, precision=exact_precision)
        new_state = ending_block[:, None, None] * carry_state + jnp.einsum('hcd,hcw->hdw', carried_block, update, precision=exact_precision)
        if with_outputs:
            result = jnp.einsum('hcd,hdw->hcw', lifted_block, carry_state, precision=exact_precision)
            result = result + jnp.einsum('hcm,hmw->hcw', score_block, update, precision=exact_precision)
            return (new_state, result)
        return (new_state, None)
    return lax.scan(advance, start_state, setup)

def gated_norm(recurrent, gate_in, norm_gain):
    scaled = recurrent * lax.rsqrt(lax.optimization_barrier(jnp.mean(recurrent * recurrent, axis=-1, keepdims=True)) + norm_epsilon)
    return scaled * norm_gain * jax.nn.silu(gate_in)

def reference(query_in, key_in, value_in, gate_in, log_gate, strength, query_conv, key_conv, value_conv, norm_gain, out_weight):
    query_prev = jnp.zeros((CONV - 1, KHEADS, DK), jnp.float32)
    key_prev = jnp.zeros((CONV - 1, KHEADS, DK), jnp.float32)
    value_prev = jnp.zeros((CONV - 1, PAYLOAD_GROUPS, DV), jnp.float32)
    queries, key_rows, values = prepare(query_in, key_in, value_in, query_prev, key_prev, value_prev, query_conv, key_conv, value_conv, SPAN)
    setup = span_setup(queries, key_rows, values, gate_blocks(log_gate, SPAN), gate_blocks(strength, SPAN))
    start_state = jnp.zeros((PAYLOAD_GROUPS, DK, DV), jnp.float32)
    final_state, recurrent = run_spans(start_state, setup, True)
    recurrent = recurrent.transpose(0, 2, 1, 3).reshape(STREAM_LENGTH, PAYLOAD_GROUPS, DV)
    normed = gated_norm(recurrent, gate_in, norm_gain).astype(jnp.bfloat16).reshape(STREAM_LENGTH, PAYLOAD_GROUPS * DV)
    group_width = PAYLOAD_GROUPS // N_HEAD * DV
    mixed = jnp.zeros((STREAM_LENGTH, D), jnp.float32)
    for group_index in range(N_HEAD):
        first = group_index * group_width
        partial_value = jnp.dot(normed[:, first:first + group_width], out_weight[first:first + group_width], preferred_element_type=jnp.float32)
        rounded = lax.optimization_barrier(partial_value.astype(jnp.bfloat16))
        mixed = mixed + rounded.astype(jnp.float32)
    return mixed
```

```python
import functools
import jax
import jax.numpy as jnp
from jax import lax
from jax.experimental import pallas as pl
from jax.experimental.pallas import tpu as pltpu
from jax.sharding import Mesh
from jax.sharding import PartitionSpec as P

CTX = ("ctx_0", "ctx_1", "ctx_2")
CTX_HEAD = ("ctx_0", "ctx_1", "ctx_2", "head")
CHUNK = 128
WIDTH = 128
PAD = 8
GROUP = 4
norm_epsilon = 1e-06
f32 = jnp.float32
bf16 = jnp.bfloat16


def mm(left, right):
    return jnp.dot(left, right, preferred_element_type=f32)


def silu(u):
    half = 0.5 * u
    return half + half * jnp.tanh(half)


def paired(x):
    zero = jnp.zeros((CHUNK, CHUNK), x.dtype)
    top = jnp.concatenate([x[:, :CHUNK], zero], axis=1)
    low = jnp.concatenate([zero, x[:, CHUNK:]], axis=1)
    return jnp.concatenate([top, low], axis=0)


def local_kernel(
    q_hbm, k_hbm, v_hbm, rim_ref, qw_ref, kw_ref, vw_ref, gate_ref,
    low_ref, wide_ref, state_ref,
    q_pad, k_pad, v_pad, solved_ref, fresh_ref, read_ref, write_ref, end_ref, mask_ref, sems,
):
    chunks = gate_ref.shape[0]
    qheads = qw_ref.shape[1]
    vheads = vw_ref.shape[1]
    blocks = chunks // GROUP
    streams = ((q_hbm, q_pad, qheads), (k_hbm, k_pad, qheads), (v_hbm, v_pad, vheads))

    def copy(which, block):
        source, target, heads = streams[which]
        rows = GROUP * CHUNK * heads
        return pltpu.make_async_copy(
            source.at[pl.ds(block * rows, rows), :],
            target.at[pl.ds(PAD * heads + block * rows, rows), :],
            sems.at[which, block],
        )

    for block in range(blocks):
        for which in range(3):
            copy(which, block).start()
    first = 0
    for which in range(3):
        _, target, heads = streams[which]
        for step in range(3):
            target[pl.ds((PAD - 3 + step) * heads, heads), :] = rim_ref[step, first : first + heads, :]
        first += heads

    row = lax.broadcasted_iota(jnp.int32, (CHUNK, 2 * CHUNK), 0)
    col = lax.broadcasted_iota(jnp.int32, (CHUNK, 2 * CHUNK), 1) & (CHUNK - 1)

    def same(bits):
        return (row >> bits) == (col >> bits)

    mask_ref[0] = same(4).astype(bf16)
    for level in range(3):
        mask_ref[1 + level] = (same(5 + level) & jnp.logical_not(same(4 + level))).astype(bf16)
    eye2 = (row == col).astype(f32)
    row1 = lax.broadcasted_iota(jnp.int32, (CHUNK, CHUNK), 0)
    col1 = lax.broadcasted_iota(jnp.int32, (CHUNK, CHUNK), 1)
    lower = row1 >= col1
    strict = row1 > col1
    adder = (row1 <= col1).astype(bf16)

    def mix(target, weight_ref, heads, head, start):
        total = None
        for tap in range(4):
            piece = target[pl.ds((start + PAD - 3 + tap) * heads + head, CHUNK, stride=heads), :]
            part = weight_ref[tap, head : head + 1, :] * piece
            total = part if total is None else total + part
        return silu(total)

    def unit(x):
        return x * lax.rsqrt(jnp.sum(x * x, axis=1, keepdims=True) + norm_epsilon)

    def setup(block):
        units = []
        for inner in range(GROUP):
            chunk = block * GROUP + inner
            start = chunk * CHUNK
            gates = gate_ref[chunk]
            hi = gates.astype(bf16).astype(f32)
            rest = gates - hi
            mid = rest.astype(bf16).astype(f32)
            parts = jnp.concatenate([hi, mid, rest - mid], axis=0).astype(bf16)
            sums = mm(parts, adder)
            running = sums[0:8] + sums[8:16] + sums[16:24]
            both = jnp.concatenate([running[0:4], gates[4:8]], axis=0)
            columns = both.T
            end_row = running[:, CHUNK - 1 : CHUNK]
            tail_row = jnp.exp(end_row - running)
            end_ref[chunk] = jnp.broadcast_to(jnp.exp(end_row), (8, CHUNK))
            for g in range(qheads):
                query = unit(mix(q_pad, qw_ref, qheads, g, start)) * (WIDTH ** -0.5)
                key = unit(mix(k_pad, kw_ref, qheads, g, start))
                key_t = key.T
                inner_products = mm(
                    jnp.concatenate([key, query], axis=0).astype(bf16), key_t.astype(bf16)
                )
                kk, qk = inner_products[:CHUNK], inner_products[CHUNK:]
                mixing = []
                rights = []
                for side in range(vheads // qheads):
                    head = g * (vheads // qheads) + side
                    decay_col = jnp.broadcast_to(columns[:, head : head + 1], (CHUNK, CHUNK))
                    gain_col = jnp.broadcast_to(columns[:, 4 + head : 5 + head], (CHUNK, CHUNK))
                    table = jnp.where(
                        lower, jnp.exp(jnp.minimum(decay_col - running[head : head + 1, :], 0.0)), 0.0
                    )
                    lift = jnp.exp(decay_col)
                    mixing.append(jnp.where(strict, gain_col * kk * table, 0.0).astype(bf16))
                    value = mix(v_pad, vw_ref, vheads, head, start)
                    rights.append(
                        jnp.concatenate(
                            [(gain_col * lift * key).astype(bf16), (gain_col * value).astype(bf16)],
                            axis=1,
                        )
                    )
                    read_ref[chunk, head] = jnp.concatenate(
                        [(lift * query).astype(bf16), (qk * table).astype(bf16)], axis=1
                    )
                    write_ref[chunk, head] = (key_t * tail_row[head : head + 1, :]).astype(bf16)
                units.append((chunk, g, jnp.concatenate(mixing, axis=1), rights))
        mixings = [u[2] for u in units]
        powers = [m * mask_ref[0] for m in mixings]
        inverses = [eye2 - p.astype(f32) for p in powers]
        powers = [mm(p, paired(p)).astype(bf16) for p in powers]
        for step in range(3):
            grown = [mm(p, paired(x.astype(bf16))) for p, x in zip(powers, inverses)]
            if step < 2:
                powers = [mm(p, paired(p)).astype(bf16) for p in powers]
            inverses = [x + y for x, y in zip(inverses, grown)]
        for level in range(3):
            packed = [x.astype(bf16) for x in inverses]
            crossed = [mm(m * mask_ref[1 + level], paired(x)).astype(bf16) for m, x in zip(mixings, packed)]
            grown = [mm(x, paired(y)) for x, y in zip(packed, crossed)]
            inverses = [x - y for x, y in zip(inverses, grown)]
        for (chunk, g, _, rights), inverse in zip(units, inverses):
            packed = inverse.astype(bf16)
            for side, right in enumerate(rights):
                head = g * (vheads // qheads) + side
                answer = mm(packed[:, side * CHUNK : (side + 1) * CHUNK], right)
                solved_ref[chunk, head] = answer[:, :CHUNK].astype(bf16)
                fresh_ref[chunk, head] = answer[:, CHUNK:]

    def block_step(block, carry):
        for which in range(3):
            copy(which, block).wait()
        setup(block)
        return carry

    lax.fori_loop(0, blocks, block_step, 0)

    def chunk_step(chunk, states):
        packed = [s.astype(bf16) for s in states]
        taken = [mm(solved_ref[chunk, h], packed[h]) for h in range(vheads)]
        updates = [
            jnp.concatenate(
                [-taken[h][:, :WIDTH], fresh_ref[chunk, h] - taken[h][:, WIDTH:]], axis=1
            ).astype(bf16)
            for h in range(vheads)
        ]
        fresh_states = []
        ends = end_ref[chunk]
        for h in range(vheads):
            added = mm(write_ref[chunk, h], updates[h])
            end = ends[h : h + 1, :]
            fresh_states.append(states[h] * jnp.concatenate([end, end], axis=1) + added)
        for h in range(vheads):
            result = mm(read_ref[chunk, h], jnp.concatenate([packed[h], updates[h]], axis=0))
            rows = pl.ds(pl.multiple_of(chunk * CHUNK, CHUNK), CHUNK)
            wide_ref[h, rows, :] = result[:, :WIDTH].astype(bf16)
            low_ref[h, rows, :] = result[:, WIDTH:]
        return fresh_states

    begin = jnp.concatenate(
        [(row1 == col1).astype(f32), jnp.zeros((CHUNK, CHUNK), f32)], axis=1
    )
    states = lax.fori_loop(0, chunks, chunk_step, [begin] * vheads)
    for h in range(vheads):
        state_ref[h] = states[h].astype(bf16)


def local_call(query, key, value, rim, query_conv, key_conv, value_conv, gates, interpret=False):
    chunks = gates.shape[0]
    tokens = chunks * CHUNK
    qheads = query_conv.shape[1]
    vheads = value_conv.shape[1]
    anywhere = pl.BlockSpec(memory_space=pl.ANY)
    inside = pl.BlockSpec(memory_space=pltpu.VMEM)
    return pl.pallas_call(
        local_kernel,
        out_shape=(
            jax.ShapeDtypeStruct((vheads, tokens, WIDTH), f32),
            jax.ShapeDtypeStruct((vheads, tokens, WIDTH), bf16),
            jax.ShapeDtypeStruct((vheads, WIDTH, 2 * WIDTH), bf16),
        ),
        in_specs=[anywhere] * 3 + [inside] * 5,
        out_specs=(inside,) * 3,
        scratch_shapes=[
            pltpu.VMEM(((PAD + tokens) * qheads, WIDTH), f32),
            pltpu.VMEM(((PAD + tokens) * qheads, WIDTH), f32),
            pltpu.VMEM(((PAD + tokens) * vheads, WIDTH), f32),
            pltpu.VMEM((chunks, vheads, CHUNK, WIDTH), bf16),
            pltpu.VMEM((chunks, vheads, CHUNK, WIDTH), f32),
            pltpu.VMEM((chunks, vheads, CHUNK, 2 * CHUNK), bf16),
            pltpu.VMEM((chunks, vheads, CHUNK, CHUNK), bf16),
            pltpu.VMEM((chunks, 8, CHUNK), f32),
            pltpu.VMEM((4, CHUNK, 2 * CHUNK), bf16),
            pltpu.SemaphoreType.DMA((3, chunks // GROUP)),
        ],
        compiler_params=pltpu.CompilerParams(vmem_limit_bytes=40 * 1024 * 1024),
        interpret=interpret,
        name="local_map",
    )(
        query.reshape(tokens * qheads, WIDTH),
        key.reshape(tokens * qheads, WIDTH),
        value.reshape(tokens * vheads, WIDTH),
        rim, query_conv, key_conv, value_conv, gates,
    )


def total_kernel(place_ref, mine_ref, other_ref, total_ref, first_ref):
    core = place_ref[1]
    for h in range(mine_ref.shape[0]):
        mine, other = mine_ref[h], other_ref[h]
        first = jnp.where(core == 0, mine, other)
        second = jnp.where(core == 0, other, mine)
        joined = mm(second[:, :WIDTH], first)
        total_ref[h] = jnp.concatenate(
            [joined[:, :WIDTH], joined[:, WIDTH:] + second[:, WIDTH:].astype(f32)], axis=1
        ).astype(bf16)
        first_ref[h] = first


def prefix_kernel(place_ref, all_ref, first_ref, mine_ref, send_ref, held_ref):
    heads = first_ref.shape[0]
    core = place_ref[1]
    held_ref[...] = jnp.zeros_like(held_ref)

    def step(j, carry):
        for h in range(heads):
            moved = mm(all_ref[j, h, :, :WIDTH], held_ref[h])
            held_ref[h] = (moved + all_ref[j, h, :, WIDTH:].astype(f32)).astype(bf16)
        return carry

    lax.fori_loop(0, place_ref[0], step, 0)
    for h in range(heads):
        before = held_ref[h]
        after = mm(first_ref[h, :, :WIDTH], before) + first_ref[h, :, WIDTH:].astype(f32)
        wide = before.astype(f32)
        mine_ref[h] = jnp.where(core == 0, wide, after).astype(bf16)
        send_ref[h] = jnp.where(core == 0, after, wide).astype(bf16)


def output_kernel(place_ref, low_ref, wide_ref, near_ref, far_ref, gate_ref, gain_ref, weight_ref, out_ref):
    core = place_ref[1]
    heads = low_ref.shape[0]
    half = heads // 2
    rows = low_ref.shape[1]
    pieces = []
    for h in range(heads):
        entering = jnp.where(core == h // half, near_ref[h % half], far_ref[h % half])
        recurrent = low_ref[h] + mm(wide_ref[h], entering)
        scaled = recurrent * lax.rsqrt(
            jnp.mean(recurrent * recurrent, axis=1, keepdims=True) + norm_epsilon
        )
        gate = gate_ref[pl.ds(h, rows, stride=heads), :]
        pieces.append((scaled * gain_ref[...] * silu(gate)).astype(bf16))
    out_ref[...] = mm(jnp.concatenate(pieces, axis=1), weight_ref[...]).astype(bf16)


def output_call(place, low, wide, near, far, gate_in, norm_gain, out_weight, rows=256):
    heads, tokens, _ = low.shape
    model = out_weight.shape[1]
    scalar = pl.BlockSpec(memory_space=pltpu.SMEM)
    return pl.pallas_call(
        output_kernel,
        out_shape=jax.ShapeDtypeStruct((tokens, model), bf16),
        grid=(tokens // rows,),
        in_specs=[
            scalar,
            pl.BlockSpec((heads, rows, WIDTH), lambda i: (0, i, 0)),
            pl.BlockSpec((heads, rows, WIDTH), lambda i: (0, i, 0)),
            pl.BlockSpec(near.shape, lambda i: (0, 0, 0)),
            pl.BlockSpec(far.shape, lambda i: (0, 0, 0)),
            pl.BlockSpec((rows * heads, WIDTH), lambda i: (i, 0)),
            pl.BlockSpec((1, WIDTH), lambda i: (0, 0)),
            pl.BlockSpec(out_weight.shape, lambda i: (0, 0)),
        ],
        out_specs=pl.BlockSpec((rows, model), lambda i: (i, 0)),
        compiler_params=pltpu.CompilerParams(vmem_limit_bytes=32 * 1024 * 1024),
        name="gated_output",
    )(
        place, low, wide, near, far,
        gate_in.reshape(tokens * heads, WIDTH), norm_gain.reshape(1, WIDTH), out_weight,
    )


def on_device(
    query_in, key_in, value_in, gate_in, log_gate, strength,
    query_conv, key_conv, value_conv, norm_gain, out_weight,
):
    rim_count = query_conv.shape[0] - 1
    count = lax.axis_size(CTX)
    rim = jnp.concatenate(
        [query_in[-rim_count:], key_in[-rim_count:], value_in[-rim_count:]], axis=1
    )
    rim = lax.ppermute(rim, CTX, [(i, i + 1) for i in range(count - 1)])
    vheads, tokens = log_gate.shape
    gates = jnp.concatenate(
        [
            log_gate.reshape(vheads, tokens // CHUNK, CHUNK),
            strength.reshape(vheads, tokens // CHUNK, CHUNK),
        ],
        axis=0,
    ).transpose(1, 0, 2)
    low, wide, state = local_call(
        query_in, key_in, value_in, rim, query_conv, key_conv, value_conv, gates
    )
    core = lax.axis_index("ctx_2")
    chip = lax.axis_index(("ctx_0", "ctx_1"))
    place = jnp.stack([chip, core]).astype(jnp.int32)
    half = vheads // 2
    mine = lax.dynamic_slice_in_dim(state, core * half, half, axis=0)
    other = lax.dynamic_slice_in_dim(state, (1 - core) * half, half, axis=0)
    swap = [(0, 1), (1, 0)]
    other = lax.ppermute(other, "ctx_2", swap)
    scalar = pl.BlockSpec(memory_space=pltpu.SMEM)
    inside = pl.BlockSpec(memory_space=pltpu.VMEM)
    same = jax.ShapeDtypeStruct(mine.shape, bf16)
    total, first = pl.pallas_call(
        total_kernel,
        out_shape=(same, same),
        in_specs=[scalar, inside, inside],
        out_specs=(inside, inside),
        name="chip_total",
    )(place, mine, other)
    everyone = lax.all_gather(total, ("ctx_0", "ctx_1"))
    entering = jax.ShapeDtypeStruct((half, WIDTH, WIDTH), bf16)
    near, send = pl.pallas_call(
        prefix_kernel,
        out_shape=(entering, entering),
        in_specs=[scalar, inside, inside],
        out_specs=(inside, inside),
        scratch_shapes=[pltpu.VMEM((half, WIDTH, WIDTH), bf16)],
        name="prefix",
    )(place, everyone, first)
    far = lax.ppermute(send, "ctx_2", swap)
    partial = output_call(place, low, wide, near, far, gate_in, norm_gain, out_weight)
    return lax.psum_scatter(partial, "head", scatter_dimension=0, tiled=True).astype(f32)


def solution(mesh):
    split = Mesh(
        mesh.devices.reshape(4, 4, 2, mesh.shape["head"]), ("ctx_0", "ctx_1", "ctx_2", "head")
    )
    in_specs = (
        P(CTX, "head", None),
        P(CTX, "head", None),
        P(CTX, "head", None),
        P(CTX, "head", None),
        P("head", CTX),
        P("head", CTX),
        P(None, "head", None),
        P(None, "head", None),
        P(None, "head", None),
        P(),
        P("head", None),
    )
    return jax.shard_map(
        on_device, mesh=split, in_specs=in_specs, out_specs=P(CTX_HEAD, None), check_vma=False
    )
```

```python
import functools
import jax
import jax.numpy as jnp
from jax import lax
from jax.experimental import pallas as pl
from jax.experimental.pallas import tpu as pltpu
from jax.sharding import Mesh
from jax.sharding import PartitionSpec as P

CTX = ("ctx_0", "ctx_1", "ctx_2")
CTX_HEAD = ("ctx_0", "ctx_1", "ctx_2", "head")
CHUNK = 128
WIDTH = 128
PAD = 8
RIM = 4
GROUP = 4
norm_epsilon = 1e-06
f32 = jnp.float32
bf16 = jnp.bfloat16


def mm(left, right):
    return jnp.dot(left, right, preferred_element_type=f32)


def silu(u):
    half = 0.5 * u
    return half + half * jnp.tanh(half)


def paired(x):
    zero = jnp.zeros((CHUNK, CHUNK), x.dtype)
    top = jnp.concatenate([x[:, :CHUNK], zero], axis=1)
    low = jnp.concatenate([zero, x[:, CHUNK:]], axis=1)
    return jnp.concatenate([top, low], axis=0)


def local_kernel(
    place_ref, q_hbm, k_hbm, v_hbm, qw_hbm, kw_hbm, vw_hbm, rim_ref, gate_ref,
    low_ref, wide_ref, near_ref, far_ref,
    q_pad, k_pad, v_pad, qw_ref, kw_ref, vw_ref,
    solved_ref, fresh_ref, read_ref, write_ref, end_ref, mask_ref, sems, tap_sems,
):
    core = place_ref[2]
    chunks = gate_ref.shape[0]
    qheads = qw_ref.shape[1]
    vheads = vw_ref.shape[1]
    blocks = chunks // GROUP
    streams = ((q_hbm, q_pad, qheads), (k_hbm, k_pad, qheads), (v_hbm, v_pad, vheads))

    def copy(which, block):
        source, target, heads = streams[which]
        rows = GROUP * CHUNK * heads
        return pltpu.make_async_copy(
            source.at[pl.ds(block * rows, rows), :],
            target.at[pl.ds(PAD * heads + block * rows, rows), :],
            sems.at[which, block],
        )

    for block in range(blocks):
        for which in range(3):
            copy(which, block).start()
    taps = [
        pltpu.make_async_copy(source, target, tap_sems.at[i])
        for i, (source, target) in enumerate(
            ((qw_hbm, qw_ref), (kw_hbm, kw_ref), (vw_hbm, vw_ref))
        )
    ]
    for tap in taps:
        tap.start()
    first = 0
    for which in range(3):
        _, target, heads = streams[which]
        rows = RIM * heads
        target[pl.ds((PAD - RIM) * heads, rows), :] = rim_ref[first : first + rows, :]
        first += rows

    row = lax.broadcasted_iota(jnp.int32, (CHUNK, 2 * CHUNK), 0)
    col = lax.broadcasted_iota(jnp.int32, (CHUNK, 2 * CHUNK), 1) & (CHUNK - 1)

    def same(bits):
        return (row >> bits) == (col >> bits)

    mask_ref[0] = same(4).astype(bf16)
    for level in range(3):
        mask_ref[1 + level] = (same(5 + level) & jnp.logical_not(same(4 + level))).astype(bf16)
    eye2 = (row == col).astype(f32)
    row1 = lax.broadcasted_iota(jnp.int32, (CHUNK, CHUNK), 0)
    col1 = lax.broadcasted_iota(jnp.int32, (CHUNK, CHUNK), 1)
    lower = row1 >= col1
    strict = row1 > col1
    adder = (row1 <= col1).astype(bf16)

    def mix(target, weight_ref, heads, head, start):
        total = None
        for tap in range(4):
            piece = target[pl.ds((start + PAD - 3 + tap) * heads + head, CHUNK, stride=heads), :]
            part = weight_ref[tap, head : head + 1, :] * piece
            total = part if total is None else total + part
        return silu(total)

    def unit(x):
        return x * lax.rsqrt(jnp.sum(x * x, axis=1, keepdims=True) + norm_epsilon)

    def setup(block):
        units = []
        for inner in range(GROUP):
            chunk = block * GROUP + inner
            start = chunk * CHUNK
            gates = gate_ref[chunk]
            hi = gates.astype(bf16).astype(f32)
            rest = gates - hi
            mid = rest.astype(bf16).astype(f32)
            parts = jnp.concatenate([hi, mid, rest - mid], axis=0).astype(bf16)
            sums = mm(parts, adder)
            running = sums[0:8] + sums[8:16] + sums[16:24]
            both = jnp.concatenate([running[0:4], gates[4:8]], axis=0)
            columns = both.T
            end_row = running[:, CHUNK - 1 : CHUNK]
            tail_row = jnp.exp(end_row - running)
            end_ref[chunk] = jnp.broadcast_to(jnp.exp(end_row), (8, CHUNK))
            for g in range(qheads):
                query = unit(mix(q_pad, qw_ref, qheads, g, start)) * (WIDTH ** -0.5)
                key = unit(mix(k_pad, kw_ref, qheads, g, start))
                key_t = key.T
                inner_products = mm(
                    jnp.concatenate([key, query], axis=0).astype(bf16), key_t.astype(bf16)
                )
                kk, qk = inner_products[:CHUNK], inner_products[CHUNK:]
                mixing = []
                rights = []
                for side in range(vheads // qheads):
                    head = g * (vheads // qheads) + side
                    decay_col = jnp.broadcast_to(columns[:, head : head + 1], (CHUNK, CHUNK))
                    gain_col = jnp.broadcast_to(columns[:, 4 + head : 5 + head], (CHUNK, CHUNK))
                    table = jnp.where(
                        lower, jnp.exp(jnp.minimum(decay_col - running[head : head + 1, :], 0.0)), 0.0
                    )
                    lift = jnp.exp(decay_col)
                    mixing.append(jnp.where(strict, gain_col * kk * table, 0.0).astype(bf16))
                    value = mix(v_pad, vw_ref, vheads, head, start)
                    rights.append(
                        jnp.concatenate(
                            [(gain_col * lift * key).astype(bf16), (gain_col * value).astype(bf16)],
                            axis=1,
                        )
                    )
                    read_ref[chunk, head] = jnp.concatenate(
                        [(lift * query).astype(bf16), (qk * table).astype(bf16)], axis=1
                    )
                    write_ref[chunk, head] = (key_t * tail_row[head : head + 1, :]).astype(bf16)
                units.append((chunk, g, jnp.concatenate(mixing, axis=1), rights))
        mixings = [u[2] for u in units]
        powers = [m * mask_ref[0] for m in mixings]
        inverses = [eye2 - p.astype(f32) for p in powers]
        powers = [mm(p, paired(p)).astype(bf16) for p in powers]
        for step in range(3):
            grown = [mm(p, paired(x.astype(bf16))) for p, x in zip(powers, inverses)]
            if step < 2:
                powers = [mm(p, paired(p)).astype(bf16) for p in powers]
            inverses = [x + y for x, y in zip(inverses, grown)]
        for level in range(3):
            packed = [x.astype(bf16) for x in inverses]
            crossed = [mm(m * mask_ref[1 + level], paired(x)).astype(bf16) for m, x in zip(mixings, packed)]
            grown = [mm(x, paired(y)) for x, y in zip(packed, crossed)]
            inverses = [x - y for x, y in zip(inverses, grown)]
        for (chunk, g, _, rights), inverse in zip(units, inverses):
            packed = inverse.astype(bf16)
            for side, right in enumerate(rights):
                head = g * (vheads // qheads) + side
                answer = mm(packed[:, side * CHUNK : (side + 1) * CHUNK], right)
                solved_ref[chunk, head] = answer[:, :CHUNK].astype(bf16)
                fresh_ref[chunk, head] = answer[:, CHUNK:]

    for tap in taps:
        tap.wait()

    def block_step(block, carry):
        for which in range(3):
            copy(which, block).wait()
        setup(block)
        return carry

    lax.fori_loop(0, blocks, block_step, 0)

    def chunk_step(chunk, states):
        packed = [s.astype(bf16) for s in states]
        taken = [mm(solved_ref[chunk, h], packed[h]) for h in range(vheads)]
        updates = [
            jnp.concatenate(
                [-taken[h][:, :WIDTH], fresh_ref[chunk, h] - taken[h][:, WIDTH:]], axis=1
            ).astype(bf16)
            for h in range(vheads)
        ]
        fresh_states = []
        ends = end_ref[chunk]
        for h in range(vheads):
            added = mm(write_ref[chunk, h], updates[h])
            end = ends[h : h + 1, :]
            fresh_states.append(states[h] * jnp.concatenate([end, end], axis=1) + added)
        for h in range(vheads):
            result = mm(read_ref[chunk, h], jnp.concatenate([packed[h], updates[h]], axis=0))
            rows = pl.ds(pl.multiple_of(chunk * CHUNK, CHUNK), CHUNK)
            wide_ref[h, rows, :] = result[:, :WIDTH].astype(bf16)
            low_ref[h, rows, :] = result[:, WIDTH:]
        return fresh_states

    begin = jnp.concatenate(
        [(row1 == col1).astype(f32), jnp.zeros((CHUNK, CHUNK), f32)], axis=1
    )
    states = lax.fori_loop(0, chunks, chunk_step, [begin] * vheads)
    half = vheads // 2
    for h in range(vheads):

        @pl.when(core == h // half)
        def _():
            near_ref[h % half] = states[h].astype(bf16)

        @pl.when(core != h // half)
        def _():
            far_ref[h % half] = states[h].astype(bf16)


def stay(value):
    return pltpu.with_memory_space_constraint(value, pltpu.HBM)


def local_call(
    place, query, key, value, query_conv, key_conv, value_conv, rim, gates, interpret=False
):
    chunks = gates.shape[0]
    tokens = chunks * CHUNK
    qheads = query_conv.shape[1]
    vheads = value_conv.shape[1]
    scalar = pl.BlockSpec(memory_space=pltpu.SMEM)
    outside = pl.BlockSpec(memory_space=pltpu.HBM)
    inside = pl.BlockSpec(memory_space=pltpu.VMEM)
    pair = jax.ShapeDtypeStruct((vheads // 2, WIDTH, 2 * WIDTH), bf16)
    return pl.pallas_call(
        local_kernel,
        out_shape=(
            jax.ShapeDtypeStruct((vheads, tokens, WIDTH), f32),
            jax.ShapeDtypeStruct((vheads, tokens, WIDTH), bf16),
            pair,
            pair,
        ),
        in_specs=[scalar] + [outside] * 6 + [inside] * 2,
        out_specs=(inside,) * 4,
        scratch_shapes=[
            pltpu.VMEM(((PAD + tokens) * qheads, WIDTH), f32),
            pltpu.VMEM(((PAD + tokens) * qheads, WIDTH), f32),
            pltpu.VMEM(((PAD + tokens) * vheads, WIDTH), f32),
            pltpu.VMEM(query_conv.shape, f32),
            pltpu.VMEM(key_conv.shape, f32),
            pltpu.VMEM(value_conv.shape, f32),
            pltpu.VMEM((chunks, vheads, CHUNK, WIDTH), bf16),
            pltpu.VMEM((chunks, vheads, CHUNK, WIDTH), f32),
            pltpu.VMEM((chunks, vheads, CHUNK, 2 * CHUNK), bf16),
            pltpu.VMEM((chunks, vheads, CHUNK, CHUNK), bf16),
            pltpu.VMEM((chunks, 8, CHUNK), f32),
            pltpu.VMEM((4, CHUNK, 2 * CHUNK), bf16),
            pltpu.SemaphoreType.DMA((3, chunks // GROUP)),
            pltpu.SemaphoreType.DMA((3,)),
        ],
        compiler_params=pltpu.CompilerParams(vmem_limit_bytes=40 * 1024 * 1024),
        interpret=interpret,
        name="local_map",
    )(
        place,
        stay(query.reshape(tokens * qheads, WIDTH)),
        stay(key.reshape(tokens * qheads, WIDTH)),
        stay(value.reshape(tokens * vheads, WIDTH)),
        stay(query_conv), stay(key_conv), stay(value_conv), rim, gates,
    )


def rim_kernel(q_hbm, k_hbm, v_hbm, rim_ref, sems):
    first = 0
    copies = []
    for i, (source, heads) in enumerate(((q_hbm, 2), (k_hbm, 2), (v_hbm, 4))):
        rows = RIM * heads
        copies.append(
            pltpu.make_async_copy(
                source.at[pl.ds(source.shape[0] - rows, rows), :],
                rim_ref.at[pl.ds(first, rows), :],
                sems.at[i],
            )
        )
        first += rows
    for copy in copies:
        copy.start()
    for copy in copies:
        copy.wait()


def rim_call(query, key, value):
    flat = [stay(x.reshape(-1, WIDTH)) for x in (query, key, value)]
    rows = RIM * (query.shape[1] + key.shape[1] + value.shape[1])
    return pl.pallas_call(
        rim_kernel,
        out_shape=jax.ShapeDtypeStruct((rows, WIDTH), f32),
        in_specs=[pl.BlockSpec(memory_space=pltpu.HBM)] * 3,
        out_specs=pl.BlockSpec(memory_space=pltpu.VMEM),
        scratch_shapes=[pltpu.SemaphoreType.DMA((3,))],
        compiler_params=pltpu.CompilerParams(vmem_limit_bytes=1024 * 1024),
        name="rim",
    )(*flat)


def total_kernel(place_ref, mine_ref, other_ref, total_ref, first_ref):
    core = place_ref[2]
    for h in range(mine_ref.shape[0]):
        mine, other = mine_ref[h], other_ref[h]
        first = jnp.where(core == 0, mine, other)
        second = jnp.where(core == 0, other, mine)
        joined = mm(second[:, :WIDTH], first)
        total_ref[h] = jnp.concatenate(
            [joined[:, :WIDTH], joined[:, WIDTH:] + second[:, WIDTH:].astype(f32)], axis=1
        ).astype(bf16)
        first_ref[h] = first


def row_kernel(place_ref, a_ref, b_ref, c_ref, d_ref, total_ref, before_ref, all_ref, sum_ref):
    here = place_ref[1]
    heads = a_ref.shape[0]
    for k, ref in enumerate((a_ref, b_ref, c_ref, d_ref)):
        all_ref[(here + 4 - k) % 4] = ref[...]
    eye = lax.broadcasted_iota(jnp.int32, (WIDTH, 2 * WIDTH), 0) == lax.broadcasted_iota(
        jnp.int32, (WIDTH, 2 * WIDTH), 1
    )
    for h in range(heads):
        sum_ref[0, h] = eye.astype(f32).astype(bf16)
        sum_ref[1, h] = all_ref[0, h]
    for j in range(1, 4):
        for h in range(heads):
            joined = mm(all_ref[j, h, :, :WIDTH], sum_ref[j, h])
            value = jnp.concatenate(
                [joined[:, :WIDTH], joined[:, WIDTH:] + all_ref[j, h, :, WIDTH:].astype(f32)],
                axis=1,
            ).astype(bf16)
            if j < 3:
                sum_ref[j + 1, h] = value
            else:
                total_ref[h] = value
    before_ref[...] = sum_ref[here]


def prefix_kernel(
    place_ref, b_ref, c_ref, d_ref, before_ref, first_ref, mine_ref, send_ref, all_ref, sum_ref
):
    here = place_ref[0]
    core = place_ref[2]
    heads = b_ref.shape[0]
    for k, ref in enumerate((b_ref, c_ref, d_ref)):
        all_ref[(here + 3 - k) % 4] = ref[...]
    for h in range(heads):
        sum_ref[0, h] = jnp.zeros((WIDTH, WIDTH), bf16)
        sum_ref[1, h] = all_ref[0, h, :, WIDTH:]
    for j in range(1, 3):
        for h in range(heads):
            moved = mm(all_ref[j, h, :, :WIDTH], sum_ref[j, h])
            sum_ref[j + 1, h] = (moved + all_ref[j, h, :, WIDTH:].astype(f32)).astype(bf16)
    for h in range(heads):
        row = sum_ref[here, h]
        before = (
            mm(before_ref[h, :, :WIDTH], row) + before_ref[h, :, WIDTH:].astype(f32)
        ).astype(bf16)
        after = mm(first_ref[h, :, :WIDTH], before) + first_ref[h, :, WIDTH:].astype(f32)
        wide = before.astype(f32)
        mine_ref[h] = jnp.where(core == 0, wide, after).astype(bf16)
        send_ref[h] = jnp.where(core == 0, after, wide).astype(bf16)


def small_call(kernel, outs, scratch, name, place, *arrays):
    inside = pl.BlockSpec(memory_space=pltpu.VMEM)
    return pl.pallas_call(
        kernel,
        out_shape=tuple(jax.ShapeDtypeStruct(shape, bf16) for shape in outs),
        in_specs=[pl.BlockSpec(memory_space=pltpu.SMEM)] + [inside] * len(arrays),
        out_specs=(inside,) * len(outs),
        scratch_shapes=[pltpu.VMEM(shape, bf16) for shape in scratch],
        compiler_params=pltpu.CompilerParams(vmem_limit_bytes=8 * 1024 * 1024),
        name=name,
    )(place, *arrays)


def output_kernel(
    place_ref, low_ref, wide_ref, near_ref, far_ref, gate_ref, gain_ref, weight_ref,
    *out_refs, slots
):
    core = place_ref[2]
    heads = low_ref.shape[0]
    half = heads // 2
    rows = out_refs[0].shape[0]
    for index, slot in enumerate(slots):
        start = pl.multiple_of(place_ref[3 + slot] * rows, rows)
        pieces = []
        for h in range(heads):
            entering = jnp.where(core == h // half, near_ref[h % half], far_ref[h % half])
            recurrent = low_ref[h, pl.ds(start, rows), :] + mm(
                wide_ref[h, pl.ds(start, rows), :], entering
            )
            scaled = recurrent * lax.rsqrt(
                jnp.mean(recurrent * recurrent, axis=1, keepdims=True) + norm_epsilon
            )
            gate = gate_ref[pl.ds(start * heads + h, rows, stride=heads), :]
            pieces.append((scaled * gain_ref[...] * silu(gate)).astype(bf16))
        normed = jnp.concatenate(pieces, axis=1)
        side = out_refs[0].shape[1]
        for k in range(2):
            out_refs[2 * index + k][...] = mm(
                normed, weight_ref[:, k * side : (k + 1) * side]
            ).astype(bf16)


def output_call(place, slots, low, wide, near, far, gate_in, norm_gain, out_weight):
    heads, tokens, _ = low.shape
    model = out_weight.shape[1]
    rows = tokens // 8
    inside = pl.BlockSpec(memory_space=pltpu.VMEM)
    piece = jax.ShapeDtypeStruct((rows, model // 2), bf16)
    return pl.pallas_call(
        functools.partial(output_kernel, slots=slots),
        out_shape=(piece,) * (2 * len(slots)),
        in_specs=[pl.BlockSpec(memory_space=pltpu.SMEM)] + [inside] * 7,
        out_specs=(inside,) * (2 * len(slots)),
        compiler_params=pltpu.CompilerParams(vmem_limit_bytes=16 * 1024 * 1024),
        cost_estimate=pl.CostEstimate(
            flops=2 * rows * heads * WIDTH * model * len(slots), transcendentals=0, bytes_accessed=0
        ),
        name="gated_output",
    )(
        place, low, wide, near, far,
        gate_in.reshape(tokens * heads, WIDTH), norm_gain.reshape(1, WIDTH), out_weight,
    )


def add_kernel(left_ref, right_ref, out_ref):
    out_ref[...] = (left_ref[...].astype(f32) + right_ref[...].astype(f32)).astype(bf16)


def add(left, right):
    inside = pl.BlockSpec(memory_space=pltpu.VMEM)
    return pl.pallas_call(
        add_kernel,
        out_shape=jax.ShapeDtypeStruct(left.shape, bf16),
        in_specs=[inside] * 2,
        out_specs=inside,
        compiler_params=pltpu.CompilerParams(vmem_limit_bytes=2 * 1024 * 1024),
        name="add",
    )(left, right)


def last_kernel(*refs):
    out_ref = refs[-1]
    side = refs[0].shape[1]
    for k in range(2):
        total = refs[k][...].astype(f32)
        for other in (refs[2 + k], refs[4 + k]):
            total = total + other[...].astype(f32)
        out_ref[:, k * side : (k + 1) * side] = total


def last_call(*arrays):
    rows, side = arrays[0].shape
    inside = pl.BlockSpec(memory_space=pltpu.VMEM)
    return pl.pallas_call(
        last_kernel,
        out_shape=jax.ShapeDtypeStruct((rows, 2 * side), f32),
        in_specs=[inside] * 6,
        out_specs=inside,
        compiler_params=pltpu.CompilerParams(vmem_limit_bytes=8 * 1024 * 1024),
        name="last_add",
    )(*arrays)


def shifted(value, axis, steps, around=True):
    count = lax.axis_size(axis)
    pairs = [(i, (i + steps) % count) for i in range(count) if around or 0 <= i + steps < count]
    return lax.ppermute(value, axis, pairs)


def head_sum(parts):
    def right(value):
        return shifted(value, "head", 1)

    def left(value):
        return shifted(value, "head", -1)

    far, up_parts, down_parts, own = parts[0], parts[1:7:2], parts[2:7:2], parts[7]
    up = [right(far[0]), right(up_parts[0][1])]
    down = [left(down_parts[0][0]), left(far[1])]
    up = [right(add(up_parts[0][0], up[0])), up[1]]
    down = [down[0], left(add(down_parts[0][1], down[1]))]
    for step in (1, 2):
        for side in (1, 0):
            up[side] = right(add(up_parts[step][side], up[side]))
            down[1 - side] = left(add(down_parts[step][1 - side], down[1 - side]))
    return last_call(*own, *up, *down)


def on_device(
    query_in, key_in, value_in, gate_in, log_gate, strength,
    query_conv, key_conv, value_conv, norm_gain, out_weight,
):
    z = lax.axis_index("head")
    order = [(z + shift) & 7 for shift in (4, 3, 5, 2, 6, 1, 7, 0)]
    place = jnp.stack(
        [lax.axis_index("ctx_0"), lax.axis_index("ctx_1"), lax.axis_index("ctx_2")] + order
    ).astype(jnp.int32)
    rim = shifted(rim_call(query_in, key_in, value_in), CTX, 1, around=False)
    vheads, tokens = log_gate.shape
    gates = jnp.concatenate(
        [
            log_gate.reshape(vheads, tokens // CHUNK, CHUNK),
            strength.reshape(vheads, tokens // CHUNK, CHUNK),
        ],
        axis=0,
    ).transpose(1, 0, 2)
    low, wide, mine, other = local_call(
        place, query_in, key_in, value_in, query_conv, key_conv, value_conv, rim, gates
    )
    other = shifted(other, "ctx_2", 1)
    half = vheads // 2
    maps = (half, WIDTH, 2 * WIDTH)
    states = (half, WIDTH, WIDTH)
    total, first = small_call(total_kernel, (maps, maps), (), "chip_total", place, mine, other)
    row = [shifted(total, "ctx_1", k) for k in range(1, 4)]
    row_total, before = small_call(
        row_kernel, (maps, maps), ((4,) + maps, (4,) + maps), "row_total", place, total, *row
    )
    rows = [shifted(row_total, "ctx_0", k, around=False) for k in range(1, 4)]
    near, send = small_call(
        prefix_kernel, (states, states), ((4,) + maps, (4,) + states), "prefix",
        place, *rows, before, first,
    )
    far = shifted(send, "ctx_2", 1)
    tail = (low, wide, near, far, gate_in, norm_gain, out_weight)
    parts = []
    for slots in ((0,), (1, 2), (3, 4), (5, 6, 7)):
        pieces = output_call(place, slots, *tail)
        parts += [pieces[2 * i : 2 * i + 2] for i in range(len(slots))]
    return head_sum(parts)


def solution(mesh):
    split = Mesh(
        mesh.devices.reshape(4, 4, 2, mesh.shape["head"]), ("ctx_0", "ctx_1", "ctx_2", "head")
    )
    in_specs = (
        P(CTX, "head", None),
        P(CTX, "head", None),
        P(CTX, "head", None),
        P(CTX, "head", None),
        P("head", CTX),
        P("head", CTX),
        P(None, "head", None),
        P(None, "head", None),
        P(None, "head", None),
        P(),
        P("head", None),
    )
    return jax.shard_map(
        on_device, mesh=split, in_specs=in_specs, out_specs=P(CTX_HEAD, None), check_vma=False
    )
```

```python
import functools
import jax
import jax.numpy as jnp
from jax import lax
from jax.experimental import pallas as pl
from jax.experimental.pallas import tpu as pltpu
from jax.sharding import Mesh
from jax.sharding import PartitionSpec as P

CTX = ("ctx_0", "ctx_1", "ctx_2")
CTX_HEAD = ("ctx_0", "ctx_1", "ctx_2", "head")
CHUNK = 128
WIDTH = 128
PAD = 8
RIM = 4
READ = 4
norm_epsilon = 1e-06
LOG2E = 1.4426950408889634
f32 = jnp.float32
bf16 = jnp.bfloat16


def mm(left, right):
    return jnp.dot(left, right, preferred_element_type=f32)


def silu_of_half(half):
    return half + half * jnp.tanh(half)


def silu(u):
    return silu_of_half(0.5 * u)


def paired(x):
    zero = jnp.zeros((CHUNK, CHUNK), x.dtype)
    top = jnp.concatenate([x[:, :CHUNK], zero], axis=1)
    low = jnp.concatenate([zero, x[:, CHUNK:]], axis=1)
    return jnp.concatenate([top, low], axis=0)


def mix(target, weight_ref, heads, head, start):
    total = None
    for tap in range(4):
        piece = target[pl.ds((start + PAD - 3 + tap) * heads + head, CHUNK, stride=heads), :]
        part = (0.5 * weight_ref[tap, head : head + 1, :]) * piece
        total = part if total is None else total + part
    return silu_of_half(total)


def unit(x):
    return x * lax.rsqrt(jnp.sum(x * x, axis=1, keepdims=True) + norm_epsilon)


def squares():
    row = lax.broadcasted_iota(jnp.int32, (CHUNK, CHUNK), 0)
    col = lax.broadcasted_iota(jnp.int32, (CHUNK, CHUNK), 1)
    return row, col


def running_sums(gates, adder):
    hi = gates.astype(bf16).astype(f32)
    rest = gates - hi
    mid = rest.astype(bf16).astype(f32)
    parts = jnp.concatenate([hi, mid, rest - mid], axis=0).astype(bf16)
    sums = mm(parts, adder)
    return (sums[0:8] + sums[8:16] + sums[16:24]) * LOG2E


def spread(columns, index):
    return jnp.broadcast_to(columns[:, index : index + 1], (CHUNK, CHUNK))


def fill_pads(streams, rim_ref, sems, chunks):
    copies = []
    for chunk in range(chunks):
        row = []
        for which, (source, target, heads, _) in enumerate(streams):
            rows = CHUNK * heads
            row.append(
                pltpu.make_async_copy(
                    source.at[pl.ds(chunk * rows, rows), :],
                    target.at[pl.ds(PAD * heads + chunk * rows, rows), :],
                    sems.at[which, chunk],
                )
            )
        for copy in row:
            copy.start()
        copies.append(row)
    for _, target, heads, first in streams:
        target[pl.ds((PAD - RIM) * heads, RIM * heads), :] = rim_ref[first : first + RIM * heads, :]
    return copies


def together(*steps):
    live = list(steps)
    while live:
        still = []
        for step, weight in live:
            alive = True
            for _ in range(weight):
                if next(step, "end") == "end":
                    alive = False
                    break
            if alive:
                still.append((step, weight))
        live = still


def local_kernel(
    place_ref, k_hbm, v_hbm, kw_hbm, vw_hbm, rim_ref, gate_ref,
    key_ref, pair_ref, near_ref, far_ref,
    k_pad, v_pad, kw_ref, vw_ref,
    mixing_ref, right_ref, solved_ref, fresh_ref, write_ref, end_ref, mask_ref, hold_ref,
    sems, tap_sems,
):
    core = place_ref[2]
    chunks = gate_ref.shape[0]
    qheads = kw_ref.shape[1]
    vheads = vw_ref.shape[1]
    ratio = vheads // qheads
    taps = [
        pltpu.make_async_copy(source, target, tap_sems.at[i])
        for i, (source, target) in enumerate(((kw_hbm, kw_ref), (vw_hbm, vw_ref)))
    ]
    for tap in taps:
        tap.start()
    copies = fill_pads(
        (
            (k_hbm, k_pad, qheads, RIM * qheads),
            (v_hbm, v_pad, vheads, 2 * RIM * qheads),
        ),
        rim_ref, sems, chunks,
    )
    row = lax.broadcasted_iota(jnp.int32, (CHUNK, 2 * CHUNK), 0)
    col = lax.broadcasted_iota(jnp.int32, (CHUNK, 2 * CHUNK), 1) & (CHUNK - 1)

    def same(bits):
        return (row >> bits) == (col >> bits)

    mask_ref[0] = same(4).astype(bf16)
    for level in range(3):
        mask_ref[1 + level] = (same(5 + level) & jnp.logical_not(same(4 + level))).astype(bf16)
    mask_ref[4] = (row == col).astype(bf16)
    row1, col1 = squares()
    strict = row1 > col1
    adder = (row1 <= col1).astype(bf16)
    for h in range(vheads):
        hold_ref[h] = jnp.concatenate(
            [(row1 == col1).astype(f32), jnp.zeros((CHUNK, CHUNK), f32)], axis=1
        )
    for tap in taps:
        tap.wait()

    def prepare(group):
        for chunk in group:
            for copy in copies[chunk]:
                copy.wait()
            start = chunk * CHUNK
            gates = gate_ref[chunk]
            running = running_sums(gates, adder)
            strengths = gates[4:8]
            scaled = running[0:4] + jnp.log2(strengths)
            columns = jnp.concatenate(
                [scaled, strengths, -jnp.exp2(scaled), jnp.zeros_like(scaled)], axis=0
            ).T
            end_row = running[:, CHUNK - 1 : CHUNK]
            tail_row = jnp.exp2(end_row - running)
            end_ref[chunk] = jnp.broadcast_to(jnp.exp2(end_row), (8, CHUNK))
            for g in range(qheads):
                key = unit(mix(k_pad, kw_ref, qheads, g, start))
                key_t = key.T
                packed = key.astype(bf16)
                key_ref[chunk, g] = packed
                kk = mm(packed, key_t.astype(bf16))
                yield
                for side in range(ratio):
                    head = g * ratio + side
                    table = jnp.where(
                        strict, jnp.exp2(spread(columns, head) - running[head : head + 1, :]), 0.0
                    )
                    lanes = slice(side * CHUNK, (side + 1) * CHUNK)
                    mixing_ref[chunk, g, :, lanes] = (kk * table).astype(bf16)
                    right_ref[chunk, head, :, :CHUNK] = (spread(columns, 8 + head) * key).astype(bf16)
                    write_ref[chunk, head] = (key_t * tail_row[head : head + 1, :]).astype(bf16)
                    value = mix(v_pad, vw_ref, vheads, head, start)
                    right_ref[chunk, head, :, CHUNK:] = (spread(columns, 4 + head) * value).astype(bf16)
                    yield

    def invert(group):
        units = [(chunk, g) for chunk in group for g in range(qheads)]

        def mixing(level):
            return [mixing_ref[c, g] * mask_ref[level] for c, g in units]

        eye = mask_ref[4]
        powers = mixing(0)
        inverses = [eye - p for p in powers]
        powers = [mm(p, paired(p)).astype(bf16) for p in powers]
        yield
        for step in range(3):
            inverses = [mm(eye + p, paired(x)).astype(bf16) for p, x in zip(powers, inverses)]
            yield
            if step < 2:
                powers = [mm(p, paired(p)).astype(bf16) for p in powers]
                yield
        for level in range(3):
            crossed = [
                eye - mm(m, paired(x)).astype(bf16) for m, x in zip(mixing(1 + level), inverses)
            ]
            yield
            inverses = [mm(x, paired(y)).astype(bf16) for x, y in zip(inverses, crossed)]
            yield
        for (chunk, g), inverse in zip(units, inverses):
            for side in range(ratio):
                head = g * ratio + side
                answer = mm(inverse[:, side * CHUNK : (side + 1) * CHUNK], right_ref[chunk, head])
                solved_ref[chunk, head] = answer[:, :CHUNK].astype(bf16)
                fresh_ref[chunk, head] = answer[:, CHUNK:]
        yield

    def advance(group):
        for chunk in group:
            states = [hold_ref[h] for h in range(vheads)]
            packed = [s.astype(bf16) for s in states]
            taken = [mm(solved_ref[chunk, h], packed[h]) for h in range(vheads)]
            yield
            updates = [
                jnp.concatenate(
                    [taken[h][:, :WIDTH], fresh_ref[chunk, h] + taken[h][:, WIDTH:]], axis=1
                ).astype(bf16)
                for h in range(vheads)
            ]
            ends = end_ref[chunk]
            for h in range(vheads):
                pair_ref[chunk, h, :CHUNK, :] = packed[h]
                pair_ref[chunk, h, CHUNK:, :] = updates[h]
                end = ends[h : h + 1, :]
                hold_ref[h] = states[h] * jnp.concatenate([end, end], axis=1) + mm(
                    write_ref[chunk, h], updates[h]
                )
            yield

    middle = chunks // 2
    early, late = range(middle), range(middle, chunks)
    together((prepare(early), 1))
    together((invert(early), 1), (prepare(late), 2))
    together((invert(late), 1), (advance(early), 1))
    together((advance(late), 1))
    half = vheads // 2
    for h in range(vheads):
        packed = hold_ref[h].astype(bf16)

        @pl.when(core == h // half)
        def _():
            near_ref[h % half] = packed

        @pl.when(core != h // half)
        def _():
            far_ref[h % half] = packed


def stay(value):
    return pltpu.with_memory_space_constraint(value, pltpu.HBM)


def local_call(place, key, value, key_conv, value_conv, rim, gates, interpret=False):
    chunks = gates.shape[0]
    tokens = chunks * CHUNK
    qheads = key_conv.shape[1]
    vheads = value_conv.shape[1]
    scalar = pl.BlockSpec(memory_space=pltpu.SMEM)
    outside = pl.BlockSpec(memory_space=pltpu.HBM)
    inside = pl.BlockSpec(memory_space=pltpu.VMEM)
    pair = jax.ShapeDtypeStruct((vheads // 2, WIDTH, 2 * WIDTH), bf16)
    return pl.pallas_call(
        local_kernel,
        out_shape=(
            jax.ShapeDtypeStruct((chunks, qheads, CHUNK, WIDTH), bf16),
            jax.ShapeDtypeStruct((chunks, vheads, 2 * CHUNK, 2 * WIDTH), bf16),
            pair,
            pair,
        ),
        in_specs=[scalar] + [outside] * 4 + [inside] * 2,
        out_specs=(inside,) * 4,
        scratch_shapes=[
            pltpu.VMEM(((PAD + tokens) * qheads, WIDTH), f32),
            pltpu.VMEM(((PAD + tokens) * vheads, WIDTH), f32),
            pltpu.VMEM(key_conv.shape, f32),
            pltpu.VMEM(value_conv.shape, f32),
            pltpu.VMEM((chunks, qheads, CHUNK, 2 * CHUNK), bf16),
            pltpu.VMEM((chunks, vheads, CHUNK, 2 * CHUNK), bf16),
            pltpu.VMEM((chunks, vheads, CHUNK, WIDTH), bf16),
            pltpu.VMEM((chunks, vheads, CHUNK, WIDTH), f32),
            pltpu.VMEM((chunks, vheads, CHUNK, CHUNK), bf16),
            pltpu.VMEM((chunks, 8, CHUNK), f32),
            pltpu.VMEM((5, CHUNK, 2 * CHUNK), bf16),
            pltpu.VMEM((vheads, WIDTH, 2 * WIDTH), f32),
            pltpu.SemaphoreType.DMA((2, chunks)),
            pltpu.SemaphoreType.DMA((2,)),
        ],
        compiler_params=pltpu.CompilerParams(vmem_limit_bytes=40 * 1024 * 1024),
        interpret=interpret,
        name="local_map",
    )(
        place,
        stay(key.reshape(tokens * qheads, WIDTH)),
        stay(value.reshape(tokens * vheads, WIDTH)),
        stay(key_conv), stay(value_conv), rim, gates,
    )


def read_kernel(
    q_hbm, qw_ref, rim_ref, gate_ref, key_ref, pair_ref, after_ref, low_ref, wide_ref, mark_ref,
    q_pad, sems,
):
    mark_ref[...] = jnp.zeros_like(mark_ref)
    chunks = gate_ref.shape[0]
    qheads = qw_ref.shape[1]
    vheads = pair_ref.shape[1]
    ratio = vheads // qheads
    copies = fill_pads(((q_hbm, q_pad, qheads, 0),), rim_ref, sems, chunks)
    row1, col1 = squares()
    lower = row1 >= col1
    adder = (row1 <= col1).astype(bf16)
    for row in copies:
        for copy in row:
            copy.wait()

    def one(chunk):
        start = pl.multiple_of(chunk * CHUNK, CHUNK)
        running = running_sums(gate_ref[chunk], adder)
        columns = running.T
        for g in range(qheads):
            query = unit(mix(q_pad, qw_ref, qheads, g, start)) * (WIDTH ** -0.5)
            qk = lax.dot_general(
                query.astype(bf16), key_ref[chunk, g], (((1,), (1,)), ((), ())),
                preferred_element_type=f32,
            )
            for side in range(ratio):
                head = g * ratio + side
                decay_col = spread(columns, head)
                table = jnp.where(lower, jnp.exp2(decay_col - running[head : head + 1, :]), 0.0)
                lift = jnp.exp2(decay_col)
                reading = jnp.concatenate(
                    [(lift * query).astype(bf16), (qk * table).astype(bf16)], axis=1
                )
                result = mm(reading, pair_ref[chunk, head])
                wide_ref[head, pl.ds(start, CHUNK), :] = result[:, :WIDTH].astype(bf16)
                low_ref[head, pl.ds(start, CHUNK), :] = result[:, WIDTH:]

    def some(step, carry):
        for inner in range(READ):
            one(step * READ + inner)
        return carry

    lax.fori_loop(0, chunks // READ, some, 0)


def read_call(query, query_conv, rim, gates, key_rows, pairs, after, interpret=False):
    chunks, vheads = pairs.shape[:2]
    tokens = chunks * CHUNK
    qheads = query_conv.shape[1]
    inside = pl.BlockSpec(memory_space=pltpu.VMEM)
    return pl.pallas_call(
        read_kernel,
        out_shape=(
            jax.ShapeDtypeStruct((vheads, tokens, WIDTH), f32),
            jax.ShapeDtypeStruct((vheads, tokens, WIDTH), bf16),
            jax.ShapeDtypeStruct((8, WIDTH), f32),
        ),
        in_specs=[pl.BlockSpec(memory_space=pltpu.HBM)] + [inside] * 5
        + [pl.BlockSpec(memory_space=pl.ANY)],
        out_specs=(inside,) * 3,
        scratch_shapes=[
            pltpu.VMEM(((PAD + tokens) * qheads, WIDTH), f32),
            pltpu.SemaphoreType.DMA((1, chunks)),
        ],
        compiler_params=pltpu.CompilerParams(vmem_limit_bytes=16 * 1024 * 1024),
        cost_estimate=pl.CostEstimate(flops=1 << 32, transcendentals=0, bytes_accessed=0),
        interpret=interpret,
        name="read_out",
    )(stay(query.reshape(tokens * qheads, WIDTH)), query_conv, rim, gates, key_rows, pairs, after)


def rim_kernel(q_hbm, k_hbm, v_hbm, rim_ref, sems):
    first = 0
    copies = []
    for i, (source, heads) in enumerate(((q_hbm, 2), (k_hbm, 2), (v_hbm, 4))):
        rows = RIM * heads
        copies.append(
            pltpu.make_async_copy(
                source.at[pl.ds(source.shape[0] - rows, rows), :],
                rim_ref.at[pl.ds(first, rows), :],
                sems.at[i],
            )
        )
        first += rows
    for copy in copies:
        copy.start()
    for copy in copies:
        copy.wait()


def rim_call(query, key, value):
    flat = [stay(x.reshape(-1, WIDTH)) for x in (query, key, value)]
    rows = RIM * (query.shape[1] + key.shape[1] + value.shape[1])
    return pl.pallas_call(
        rim_kernel,
        out_shape=jax.ShapeDtypeStruct((rows, WIDTH), f32),
        in_specs=[pl.BlockSpec(memory_space=pltpu.HBM)] * 3,
        out_specs=pl.BlockSpec(memory_space=pltpu.VMEM),
        scratch_shapes=[pltpu.SemaphoreType.DMA((3,))],
        compiler_params=pltpu.CompilerParams(vmem_limit_bytes=1024 * 1024),
        name="rim",
    )(*flat)


def total_kernel(place_ref, mine_ref, other_ref, total_ref, first_ref):
    core = place_ref[2]
    for h in range(mine_ref.shape[0]):
        mine, other = mine_ref[h], other_ref[h]
        first = jnp.where(core == 0, mine, other)
        second = jnp.where(core == 0, other, mine)
        joined = mm(second[:, :WIDTH], first)
        total_ref[h] = jnp.concatenate(
            [joined[:, :WIDTH], joined[:, WIDTH:] + second[:, WIDTH:].astype(f32)], axis=1
        ).astype(bf16)
        first_ref[h] = first


def row_kernel(place_ref, a_ref, b_ref, c_ref, d_ref, mark_ref, total_ref, before_ref, all_ref, sum_ref):
    here = place_ref[1]
    heads = a_ref.shape[0]
    for k, ref in enumerate((a_ref, b_ref, c_ref, d_ref)):
        all_ref[(here + 4 - k) % 4] = ref[...]
    eye = lax.broadcasted_iota(jnp.int32, (WIDTH, 2 * WIDTH), 0) == lax.broadcasted_iota(
        jnp.int32, (WIDTH, 2 * WIDTH), 1
    )
    for h in range(heads):
        sum_ref[0, h] = eye.astype(f32).astype(bf16)
        sum_ref[1, h] = all_ref[0, h]
    for j in range(1, 4):
        for h in range(heads):
            joined = mm(all_ref[j, h, :, :WIDTH], sum_ref[j, h])
            value = jnp.concatenate(
                [joined[:, :WIDTH], joined[:, WIDTH:] + all_ref[j, h, :, WIDTH:].astype(f32)],
                axis=1,
            ).astype(bf16)
            if j < 3:
                sum_ref[j + 1, h] = value
            else:
                total_ref[h] = value
    before_ref[...] = sum_ref[here]


def prefix_kernel(
    place_ref, b_ref, c_ref, d_ref, before_ref, first_ref, mine_ref, send_ref, all_ref, sum_ref
):
    here = place_ref[0]
    core = place_ref[2]
    heads = b_ref.shape[0]
    for k, ref in enumerate((b_ref, c_ref, d_ref)):
        all_ref[(here + 3 - k) % 4] = ref[...]
    for h in range(heads):
        sum_ref[0, h] = jnp.zeros((WIDTH, WIDTH), bf16)
        sum_ref[1, h] = all_ref[0, h, :, WIDTH:]
    for j in range(1, 3):
        for h in range(heads):
            moved = mm(all_ref[j, h, :, :WIDTH], sum_ref[j, h])
            sum_ref[j + 1, h] = (moved + all_ref[j, h, :, WIDTH:].astype(f32)).astype(bf16)
    for h in range(heads):
        row = sum_ref[here, h]
        before = (
            mm(before_ref[h, :, :WIDTH], row) + before_ref[h, :, WIDTH:].astype(f32)
        ).astype(bf16)
        after = mm(first_ref[h, :, :WIDTH], before) + first_ref[h, :, WIDTH:].astype(f32)
        wide = before.astype(f32)
        mine_ref[h] = jnp.where(core == 0, wide, after).astype(bf16)
        send_ref[h] = jnp.where(core == 0, after, wide).astype(bf16)


def small_call(kernel, outs, scratch, name, place, *arrays):
    inside = pl.BlockSpec(memory_space=pltpu.VMEM)
    return pl.pallas_call(
        kernel,
        out_shape=tuple(jax.ShapeDtypeStruct(shape, bf16) for shape in outs),
        in_specs=[pl.BlockSpec(memory_space=pltpu.SMEM)] + [inside] * len(arrays),
        out_specs=(inside,) * len(outs),
        scratch_shapes=[pltpu.VMEM(shape, bf16) for shape in scratch],
        compiler_params=pltpu.CompilerParams(vmem_limit_bytes=8 * 1024 * 1024),
        name=name,
    )(place, *arrays)


def output_kernel(
    place_ref, low_ref, wide_ref, near_ref, far_ref, gate_ref, gain_ref, weight_ref,
    *out_refs, slots
):
    core = place_ref[2]
    heads = low_ref.shape[0]
    half = heads // 2
    rows = out_refs[0].shape[0]
    for index, slot in enumerate(slots):
        start = pl.multiple_of(place_ref[3 + slot] * rows, rows)
        pieces = []
        for h in range(heads):
            entering = jnp.where(core == h // half, near_ref[h % half], far_ref[h % half])
            recurrent = low_ref[h, pl.ds(start, rows), :] + mm(
                wide_ref[h, pl.ds(start, rows), :], entering
            )
            scaled = recurrent * lax.rsqrt(
                jnp.mean(recurrent * recurrent, axis=1, keepdims=True) + norm_epsilon
            )
            gate = gate_ref[pl.ds(start * heads + h, rows, stride=heads), :]
            pieces.append((scaled * gain_ref[...] * silu(gate)).astype(bf16))
        normed = jnp.concatenate(pieces, axis=1)
        side = out_refs[0].shape[1]
        for k in range(2):
            out_refs[2 * index + k][...] = mm(
                normed, weight_ref[:, k * side : (k + 1) * side]
            ).astype(bf16)


def output_call(place, slots, low, wide, near, far, gate_in, norm_gain, out_weight):
    heads, tokens, _ = low.shape
    model = out_weight.shape[1]
    rows = tokens // 8
    inside = pl.BlockSpec(memory_space=pltpu.VMEM)
    piece = jax.ShapeDtypeStruct((rows, model // 2), bf16)
    return pl.pallas_call(
        functools.partial(output_kernel, slots=slots),
        out_shape=(piece,) * (2 * len(slots)),
        in_specs=[pl.BlockSpec(memory_space=pltpu.SMEM)] + [inside] * 7,
        out_specs=(inside,) * (2 * len(slots)),
        compiler_params=pltpu.CompilerParams(vmem_limit_bytes=16 * 1024 * 1024),
        cost_estimate=pl.CostEstimate(
            flops=2 * rows * heads * WIDTH * model * len(slots), transcendentals=0, bytes_accessed=0
        ),
        name="gated_output",
    )(
        place, low, wide, near, far,
        gate_in.reshape(tokens * heads, WIDTH), norm_gain.reshape(1, WIDTH), out_weight,
    )


def add_kernel(left_ref, right_ref, out_ref):
    out_ref[...] = (left_ref[...].astype(f32) + right_ref[...].astype(f32)).astype(bf16)


def add(left, right):
    inside = pl.BlockSpec(memory_space=pltpu.VMEM)
    return pl.pallas_call(
        add_kernel,
        out_shape=jax.ShapeDtypeStruct(left.shape, bf16),
        in_specs=[inside] * 2,
        out_specs=inside,
        compiler_params=pltpu.CompilerParams(vmem_limit_bytes=2 * 1024 * 1024),
        name="add",
    )(left, right)


def last_kernel(*refs):
    out_ref = refs[-1]
    side = refs[0].shape[1]
    for k in range(2):
        total = refs[k][...].astype(f32)
        for other in (refs[2 + k], refs[4 + k]):
            total = total + other[...].astype(f32)
        out_ref[:, k * side : (k + 1) * side] = total


def last_call(*arrays):
    rows, side = arrays[0].shape
    inside = pl.BlockSpec(memory_space=pltpu.VMEM)
    return pl.pallas_call(
        last_kernel,
        out_shape=jax.ShapeDtypeStruct((rows, 2 * side), f32),
        in_specs=[inside] * 6,
        out_specs=inside,
        compiler_params=pltpu.CompilerParams(vmem_limit_bytes=8 * 1024 * 1024),
        name="last_add",
    )(*arrays)


def shifted(value, axis, steps, around=True):
    count = lax.axis_size(axis)
    pairs = [(i, (i + steps) % count) for i in range(count) if around or 0 <= i + steps < count]
    return lax.ppermute(value, axis, pairs)


def head_sum(parts):
    def right(value):
        return shifted(value, "head", 1)

    def left(value):
        return shifted(value, "head", -1)

    far, up_parts, down_parts, own = parts[0], parts[1:7:2], parts[2:7:2], parts[7]
    up = [right(far[0]), right(up_parts[0][1])]
    down = [left(down_parts[0][0]), left(far[1])]
    up = [right(add(up_parts[0][0], up[0])), up[1]]
    down = [down[0], left(add(down_parts[0][1], down[1]))]
    for step in (1, 2):
        for side in (1, 0):
            up[side] = right(add(up_parts[step][side], up[side]))
            down[1 - side] = left(add(down_parts[step][1 - side], down[1 - side]))
    return last_call(*own, *up, *down)


def on_device(
    query_in, key_in, value_in, gate_in, log_gate, strength,
    query_conv, key_conv, value_conv, norm_gain, out_weight,
):
    z = lax.axis_index("head")
    order = [(z + shift) & 7 for shift in (4, 3, 5, 2, 6, 1, 7, 0)]
    place = jnp.stack(
        [lax.axis_index("ctx_0"), lax.axis_index("ctx_1"), lax.axis_index("ctx_2")] + order
    ).astype(jnp.int32)
    rim = shifted(rim_call(query_in, key_in, value_in), CTX, 1, around=False)
    vheads, tokens = log_gate.shape
    gates = jnp.concatenate(
        [
            log_gate.reshape(vheads, tokens // CHUNK, CHUNK),
            strength.reshape(vheads, tokens // CHUNK, CHUNK),
        ],
        axis=0,
    ).transpose(1, 0, 2)
    key_rows, pairs, mine, other = local_call(
        place, key_in, value_in, key_conv, value_conv, rim, gates
    )
    other = shifted(other, "ctx_2", 1)
    half = vheads // 2
    maps = (half, WIDTH, 2 * WIDTH)
    states = (half, WIDTH, WIDTH)
    total, first = small_call(total_kernel, (maps, maps), (), "chip_total", place, mine, other)
    low, wide, mark = read_call(query_in, query_conv, rim, gates, key_rows, pairs, first)
    row = [shifted(total, "ctx_1", k) for k in range(1, 4)]
    row_total, before = small_call(
        row_kernel, (maps, maps), ((4,) + maps, (4,) + maps), "row_total", place, total, *row, mark
    )
    rows = [shifted(row_total, "ctx_0", k, around=False) for k in range(1, 4)]
    near, send = small_call(
        prefix_kernel, (states, states), ((4,) + maps, (4,) + states), "prefix",
        place, *rows, before, first,
    )
    far = shifted(send, "ctx_2", 1)
    tail = (low, wide, near, far, gate_in, norm_gain, out_weight)
    parts = []
    for slots in ((0,), (1, 2), (3, 4), (5, 6, 7)):
        pieces = output_call(place, slots, *tail)
        parts += [pieces[2 * i : 2 * i + 2] for i in range(len(slots))]
    return head_sum(parts)


def solution(mesh):
    split = Mesh(
        mesh.devices.reshape(4, 4, 2, mesh.shape["head"]), ("ctx_0", "ctx_1", "ctx_2", "head")
    )
    in_specs = (
        P(CTX, "head", None),
        P(CTX, "head", None),
        P(CTX, "head", None),
        P(CTX, "head", None),
        P("head", CTX),
        P("head", CTX),
        P(None, "head", None),
        P(None, "head", None),
        P(None, "head", None),
        P(),
        P("head", None),
    )
    return jax.shard_map(
        on_device, mesh=split, in_specs=in_specs, out_specs=P(CTX_HEAD, None), check_vma=False
    )
```

```python
import functools
import jax
import jax.numpy as jnp
from jax import lax
from jax.experimental import pallas as pl
from jax.experimental.pallas import tpu as pltpu
from jax.sharding import Mesh
from jax.sharding import PartitionSpec as P

CTX = ("ctx_0", "ctx_1", "ctx_2")
CTX_HEAD = ("ctx_0", "ctx_1", "ctx_2", "head")
CHUNK = 128
WIDTH = 128
PAD = 8
RIM = 4
READ = 2
norm_epsilon = 1e-06
LOG2E = 1.4426950408889634
f32 = jnp.float32
bf16 = jnp.bfloat16


def mm(left, right):
    return jnp.dot(left, right, preferred_element_type=f32)


def silu_of_half(half):
    return half + half * jnp.tanh(half)


def silu(u):
    return silu_of_half(0.5 * u)


def paired(x):
    zero = jnp.zeros((CHUNK, CHUNK), x.dtype)
    top = jnp.concatenate([x[:, :CHUNK], zero], axis=1)
    low = jnp.concatenate([zero, x[:, CHUNK:]], axis=1)
    return jnp.concatenate([top, low], axis=0)


def mix(target, weight_ref, heads, head, start):
    total = None
    for tap in range(4):
        piece = target[pl.ds((start + PAD - 3 + tap) * heads + head, CHUNK, stride=heads), :]
        part = (0.5 * weight_ref[tap, head : head + 1, :]) * piece
        total = part if total is None else total + part
    return silu_of_half(total)


def unit(x):
    return x * lax.rsqrt(jnp.sum(x * x, axis=1, keepdims=True) + norm_epsilon)


def squares():
    row = lax.broadcasted_iota(jnp.int32, (CHUNK, CHUNK), 0)
    col = lax.broadcasted_iota(jnp.int32, (CHUNK, CHUNK), 1)
    return row, col


def running_sums(gates, adder):
    hi = gates.astype(bf16).astype(f32)
    rest = gates - hi
    mid = rest.astype(bf16).astype(f32)
    parts = jnp.concatenate([hi, mid, rest - mid], axis=0).astype(bf16)
    sums = mm(parts, adder)
    return (sums[0:8] + sums[8:16] + sums[16:24]) * LOG2E


def spread(columns, index):
    return jnp.broadcast_to(columns[:, index : index + 1], (CHUNK, CHUNK))


def fill_pads(streams, sems, first, count):
    copies = []
    for i in range(count):
        row = []
        for which, (source, target, heads) in enumerate(streams):
            lead = PAD * heads if first > 0 and i == 0 else 0
            rows = CHUNK * heads
            row.append(
                pltpu.make_async_copy(
                    source.at[pl.ds((first + i) * rows - lead, rows + lead), :],
                    target.at[pl.ds(PAD * heads + i * rows - lead, rows + lead), :],
                    sems.at[which, i],
                )
            )
        for copy in row:
            copy.start()
        copies.append(row)
    return copies


def fill_rim(target, heads, rim_ref, first):
    target[pl.ds((PAD - RIM) * heads, RIM * heads), :] = rim_ref[first : first + RIM * heads, :]


def together(*steps):
    live = list(steps)
    while live:
        still = []
        for step, weight in live:
            alive = True
            for _ in range(weight):
                if next(step, "end") == "end":
                    alive = False
                    break
            if alive:
                still.append((step, weight))
        live = still


def start_taps(pairs, sems):
    taps = [
        pltpu.make_async_copy(source, target, sems.at[i])
        for i, (source, target) in enumerate(pairs)
    ]
    for tap in taps:
        tap.start()
    return taps


def prepare(group, first, copies, pads, weights, gate_ref, store):
    k_pad, v_pad = pads
    kw_ref, vw_ref = weights
    key_ref, mixing_ref, value_ref, write_ref, rows_ref = store
    qheads = kw_ref.shape[1]
    vheads = vw_ref.shape[1]
    ratio = vheads // qheads
    row1, col1 = squares()
    strict = row1 > col1
    adder = (row1 <= col1).astype(bf16)
    for i in group:
        for copy in copies[i]:
            copy.wait()
        start = i * CHUNK
        gates = gate_ref[first + i]
        running = running_sums(gates, adder)
        strengths = gates[4:8]
        scaled = running[0:4] + jnp.log2(strengths)
        columns = jnp.concatenate([scaled, scaled], axis=0).T
        end_row = running[:, CHUNK - 1 : CHUNK]
        tail_row = jnp.exp2(end_row - running)
        rows_ref[i, 0:4, :] = -jnp.exp2(scaled)
        rows_ref[i, 4:8, :] = strengths
        rows_ref[i, 8:16, :] = jnp.broadcast_to(jnp.exp2(end_row), (8, CHUNK))
        for g in range(qheads):
            key = unit(mix(k_pad, kw_ref, qheads, g, start))
            key_t = key.T
            packed = key.astype(bf16)
            key_ref[i, g] = packed
            kk = mm(packed, key_t.astype(bf16))
            yield
            for side in range(ratio):
                head = g * ratio + side
                table = jnp.where(
                    strict, jnp.exp2(spread(columns, head) - running[head : head + 1, :]), 0.0
                )
                lanes = slice(side * CHUNK, (side + 1) * CHUNK)
                mixing_ref[i, g, :, lanes] = (kk * table).astype(bf16)
                write_ref[i, head] = (key_t * tail_row[head : head + 1, :]).astype(bf16)
                value_ref[i, head] = mix(v_pad, vw_ref, vheads, head, start).astype(bf16)
                yield


def invert(first, store, mask_ref, solved_ref, fresh_ref):
    key_ref, mixing_ref, value_ref, write_ref, rows_ref = store
    count, qheads = mixing_ref.shape[:2]
    ratio = value_ref.shape[1] // qheads
    units = [(i, g) for i in range(count) for g in range(qheads)]

    def mixing(level):
        return [mixing_ref[i, g] * mask_ref[level] for i, g in units]

    eye = mask_ref[4]
    powers = mixing(0)
    inverses = [eye - p for p in powers]
    powers = [mm(p, paired(p)).astype(bf16) for p in powers]
    yield
    for step in range(3):
        inverses = [mm(eye + p, paired(x)).astype(bf16) for p, x in zip(powers, inverses)]
        yield
        if step < 2:
            powers = [mm(p, paired(p)).astype(bf16) for p in powers]
            yield
    for level in range(3):
        crossed = [
            eye - mm(m, paired(x)).astype(bf16) for m, x in zip(mixing(1 + level), inverses)
        ]
        yield
        inverses = [mm(x, paired(y)) for x, y in zip(inverses, crossed)]
        if level < 2:
            inverses = [x.astype(bf16) for x in inverses]
        yield
    for (i, g), inverse in zip(units, inverses):
        for side in range(ratio):
            head = g * ratio + side
            own = inverse[:, side * CHUNK : (side + 1) * CHUNK]
            left = jnp.concatenate(
                [own * rows_ref[i, head : head + 1, :], own * rows_ref[i, 4 + head : 5 + head, :]],
                axis=1,
            ).astype(bf16)
            right = jnp.concatenate([key_ref[i, g], value_ref[i, head]], axis=1)
            answer = mm(left, paired(right))
            solved_ref[first + i, head] = answer[:, :CHUNK].astype(bf16)
            fresh_ref[first + i, head] = answer[:, CHUNK:]
        yield


def join(later, earlier):
    keep1, change1, offset1 = later
    keep0, change0, offset0 = earlier
    moved = mm(change1.astype(bf16), jnp.concatenate([change0, offset0], axis=1).astype(bf16))
    return (
        keep1 * keep0,
        moved[:, :WIDTH] + (keep1 * change0 + keep0 * change1),
        moved[:, WIDTH:] + (keep1 * offset0 + offset1),
    )


def chain_maps(first, store, solved_ref, fresh_ref, vheads, result):
    _, _, _, write_ref, rows_ref = store
    maps = []
    for i in range(write_ref.shape[0]):
        row = []
        for h in range(vheads):
            moved = mm(
                write_ref[i, h],
                jnp.concatenate(
                    [solved_ref[first + i, h], fresh_ref[first + i, h].astype(bf16)], axis=1
                ),
            )
            row.append((rows_ref[i, 8 + h : 9 + h, :], moved[:, :WIDTH], moved[:, WIDTH:]))
        maps.append(row)
        yield
    while len(maps) > 1:
        maps = [
            [join(later, earlier) for later, earlier in zip(maps[k + 1], maps[k])]
            for k in range(0, len(maps), 2)
        ]
        yield
    result.extend(maps[0])


def late_kernel(
    k_hbm, v_hbm, kw_hbm, vw_hbm, gate_ref,
    key_ref, mixing_ref, value_ref, write_ref, rows_ref,
    k_pad, v_pad, kw_ref, vw_ref, sems, tap_sems,
):
    count = key_ref.shape[0]
    taps = start_taps(((kw_hbm, kw_ref), (vw_hbm, vw_ref)), tap_sems)
    copies = fill_pads(
        ((k_hbm, k_pad, kw_ref.shape[1]), (v_hbm, v_pad, vw_ref.shape[1])),
        sems, gate_ref.shape[0] - count, count,
    )
    for tap in taps:
        tap.wait()
    store = (key_ref, mixing_ref, value_ref, write_ref, rows_ref)
    group = prepare(
        range(count), gate_ref.shape[0] - count, copies, (k_pad, v_pad), (kw_ref, vw_ref),
        gate_ref, store,
    )
    together((group, 1))


def local_kernel(
    place_ref, k_hbm, v_hbm, kw_hbm, vw_hbm, rim_ref, gate_ref,
    late_key_ref, late_mixing_ref, late_value_ref, late_write_ref, late_rows_ref,
    key_ref, write_ref, rows_ref, solved_ref, fresh_ref, near_ref, far_ref,
    mixing_ref, value_ref, k_pad, v_pad, kw_ref, vw_ref, mask_ref, sems, tap_sems,
):
    core = place_ref[2]
    chunks = gate_ref.shape[0]
    count = key_ref.shape[0]
    qheads = kw_ref.shape[1]
    vheads = vw_ref.shape[1]
    taps = start_taps(((kw_hbm, kw_ref), (vw_hbm, vw_ref)), tap_sems)
    copies = fill_pads(((k_hbm, k_pad, qheads), (v_hbm, v_pad, vheads)), sems, 0, count)
    fill_rim(k_pad, qheads, rim_ref, RIM * qheads)
    fill_rim(v_pad, vheads, rim_ref, 2 * RIM * qheads)
    row = lax.broadcasted_iota(jnp.int32, (CHUNK, 2 * CHUNK), 0)
    col = lax.broadcasted_iota(jnp.int32, (CHUNK, 2 * CHUNK), 1) & (CHUNK - 1)

    def same(bits):
        return (row >> bits) == (col >> bits)

    mask_ref[0] = same(4).astype(bf16)
    for level in range(3):
        mask_ref[1 + level] = (same(5 + level) & jnp.logical_not(same(4 + level))).astype(bf16)
    mask_ref[4] = (row == col).astype(bf16)
    for tap in taps:
        tap.wait()
    early = (key_ref, mixing_ref, value_ref, write_ref, rows_ref)
    late = (late_key_ref, late_mixing_ref, late_value_ref, late_write_ref, late_rows_ref)
    first_half, second_half = [], []
    together(
        (invert(chunks - count, late, mask_ref, solved_ref, fresh_ref), 1),
        (
            prepare(
                range(count), 0, copies, (k_pad, v_pad), (kw_ref, vw_ref), gate_ref, early
            ),
            2,
        ),
    )
    together(
        (invert(0, early, mask_ref, solved_ref, fresh_ref), 2),
        (chain_maps(chunks - count, late, solved_ref, fresh_ref, vheads, second_half), 1),
    )
    together((chain_maps(0, early, solved_ref, fresh_ref, vheads, first_half), 1))
    half = vheads // 2
    row1, col1 = squares()
    for h in range(vheads):
        keep, change, offset = join(second_half[h], first_half[h])
        packed = jnp.concatenate(
            [change + jnp.where(row1 == col1, keep, 0.0), offset], axis=1
        ).astype(bf16)

        @pl.when(core == h // half)
        def _():
            near_ref[h % half] = packed

        @pl.when(core != h // half)
        def _():
            far_ref[h % half] = packed


def stay(value):
    return pltpu.with_memory_space_constraint(value, pltpu.HBM)


OUTSIDE = pl.BlockSpec(memory_space=pltpu.HBM)
INSIDE = pl.BlockSpec(memory_space=pltpu.VMEM)
SCALAR = pl.BlockSpec(memory_space=pltpu.SMEM)
MIB = 1024 * 1024


def group_shapes(count, qheads, vheads):
    return (
        jax.ShapeDtypeStruct((count, qheads, CHUNK, WIDTH), bf16),
        jax.ShapeDtypeStruct((count, qheads, CHUNK, 2 * CHUNK), bf16),
        jax.ShapeDtypeStruct((count, vheads, CHUNK, WIDTH), bf16),
        jax.ShapeDtypeStruct((count, vheads, CHUNK, CHUNK), bf16),
        jax.ShapeDtypeStruct((count, 16, CHUNK), f32),
    )


def pad_scratch(count, key_conv, value_conv):
    return [
        pltpu.VMEM(((PAD + count * CHUNK) * key_conv.shape[1], WIDTH), f32),
        pltpu.VMEM(((PAD + count * CHUNK) * value_conv.shape[1], WIDTH), f32),
        pltpu.VMEM(key_conv.shape, f32),
        pltpu.VMEM(value_conv.shape, f32),
    ]


def late_call(key, value, key_conv, value_conv, gates, interpret=False):
    count = gates.shape[0] // 2
    return pl.pallas_call(
        late_kernel,
        out_shape=group_shapes(count, key_conv.shape[1], value_conv.shape[1]),
        in_specs=[OUTSIDE] * 4 + [INSIDE],
        out_specs=(INSIDE,) * 5,
        scratch_shapes=pad_scratch(count, key_conv, value_conv)
        + [pltpu.SemaphoreType.DMA((2, count)), pltpu.SemaphoreType.DMA((2,))],
        compiler_params=pltpu.CompilerParams(vmem_limit_bytes=16 * MIB),
        cost_estimate=pl.CostEstimate(flops=1 << 32, transcendentals=0, bytes_accessed=0),
        interpret=interpret,
        name="late_half",
    )(
        stay(key.reshape(-1, WIDTH)), stay(value.reshape(-1, WIDTH)),
        stay(key_conv), stay(value_conv), gates,
    )


def local_call(place, key, value, key_conv, value_conv, rim, gates, late, interpret=False):
    chunks = gates.shape[0]
    count = chunks // 2
    vheads = value_conv.shape[1]
    shapes = group_shapes(count, key_conv.shape[1], vheads)
    pair = jax.ShapeDtypeStruct((vheads // 2, WIDTH, 2 * WIDTH), bf16)
    return pl.pallas_call(
        local_kernel,
        out_shape=(
            shapes[0],
            shapes[3],
            shapes[4],
            jax.ShapeDtypeStruct((chunks, vheads, CHUNK, WIDTH), bf16),
            jax.ShapeDtypeStruct((chunks, vheads, CHUNK, WIDTH), f32),
            pair,
            pair,
        ),
        in_specs=[SCALAR] + [OUTSIDE] * 4 + [INSIDE] * 7,
        out_specs=(INSIDE,) * 7,
        scratch_shapes=[pltpu.VMEM(shapes[1].shape, bf16), pltpu.VMEM(shapes[2].shape, bf16)]
        + pad_scratch(count, key_conv, value_conv)
        + [
            pltpu.VMEM((5, CHUNK, 2 * CHUNK), bf16),
            pltpu.SemaphoreType.DMA((2, count)),
            pltpu.SemaphoreType.DMA((2,)),
        ],
        compiler_params=pltpu.CompilerParams(vmem_limit_bytes=24 * MIB),
        interpret=interpret,
        name="local_map",
    )(
        place, stay(key.reshape(-1, WIDTH)), stay(value.reshape(-1, WIDTH)),
        stay(key_conv), stay(value_conv), rim, gates, *late,
    )


def chain_kernel(
    solved_ref, fresh_ref, write_ref, rows_ref, late_write_ref, late_rows_ref, after_ref,
    pair_ref, mark_ref, hold_ref,
):
    chunks, vheads = solved_ref.shape[:2]
    count = write_ref.shape[0]
    mark_ref[...] = jnp.zeros_like(mark_ref)
    row1, col1 = squares()
    for h in range(vheads):
        hold_ref[h] = jnp.concatenate(
            [(row1 == col1).astype(f32), jnp.zeros((CHUNK, CHUNK), f32)], axis=1
        )
    for first, writes, rows in ((0, write_ref, rows_ref), (count, late_write_ref, late_rows_ref)):

        def step(i, carry):
            chunk = first + i
            states = [hold_ref[h] for h in range(vheads)]
            packed = [s.astype(bf16) for s in states]
            taken = [mm(solved_ref[chunk, h], packed[h]) for h in range(vheads)]
            updates = [
                jnp.concatenate(
                    [taken[h][:, :WIDTH], fresh_ref[chunk, h] + taken[h][:, WIDTH:]], axis=1
                ).astype(bf16)
                for h in range(vheads)
            ]
            ends = rows[i]
            for h in range(vheads):
                pair_ref[chunk, h, :CHUNK, :] = packed[h]
                pair_ref[chunk, h, CHUNK:, :] = updates[h]
                end = ends[8 + h : 9 + h, :]
                hold_ref[h] = states[h] * jnp.concatenate([end, end], axis=1) + mm(
                    writes[i, h], updates[h]
                )
            return carry

        lax.fori_loop(0, count, step, 0)


def chain_call(solved, fresh, write, rows, late_write, late_rows, after, interpret=False):
    chunks, vheads = solved.shape[:2]
    return pl.pallas_call(
        chain_kernel,
        out_shape=(
            jax.ShapeDtypeStruct((chunks, vheads, 2 * CHUNK, 2 * WIDTH), bf16),
            jax.ShapeDtypeStruct((8, WIDTH), f32),
        ),
        in_specs=[INSIDE] * 6 + [pl.BlockSpec(memory_space=pl.ANY)],
        out_specs=(INSIDE,) * 2,
        scratch_shapes=[pltpu.VMEM((vheads, WIDTH, 2 * WIDTH), f32)],
        compiler_params=pltpu.CompilerParams(vmem_limit_bytes=16 * MIB),
        cost_estimate=pl.CostEstimate(flops=1 << 32, transcendentals=0, bytes_accessed=0),
        interpret=interpret,
        name="chain",
    )(solved, fresh, write, rows, late_write, late_rows, after)


def read_kernel(
    q_hbm, qw_ref, rim_ref, gate_ref, key_ref, late_key_ref, pair_ref, after_ref,
    low_ref, wide_ref, mark_ref, q_pad, sems,
):
    mark_ref[...] = jnp.zeros_like(mark_ref)
    chunks = gate_ref.shape[0]
    count = key_ref.shape[0]
    qheads = qw_ref.shape[1]
    vheads = pair_ref.shape[1]
    ratio = vheads // qheads
    copies = fill_pads(((q_hbm, q_pad, qheads),), sems, 0, chunks)
    fill_rim(q_pad, qheads, rim_ref, 0)
    row1, col1 = squares()
    lower = row1 >= col1
    adder = (row1 <= col1).astype(bf16)
    for first, keys in ((0, key_ref), (count, late_key_ref)):
        for row in copies[first : first + count]:
            for copy in row:
                copy.wait()

        def some(step, carry):
            for inner in range(READ):
                i = step * READ + inner
                chunk = first + i
                start = pl.multiple_of(chunk * CHUNK, CHUNK)
                running = running_sums(gate_ref[chunk], adder)
                columns = running.T
                for g in range(qheads):
                    query = unit(mix(q_pad, qw_ref, qheads, g, start)) * (WIDTH ** -0.5)
                    qk = lax.dot_general(
                        query.astype(bf16), keys[i, g], (((1,), (1,)), ((), ())),
                        preferred_element_type=f32,
                    )
                    for side in range(ratio):
                        head = g * ratio + side
                        decay_col = spread(columns, head)
                        table = jnp.where(
                            lower, jnp.exp2(decay_col - running[head : head + 1, :]), 0.0
                        )
                        lift = jnp.exp2(decay_col)
                        reading = jnp.concatenate(
                            [(lift * query).astype(bf16), (qk * table).astype(bf16)], axis=1
                        )
                        result = mm(reading, pair_ref[chunk, head])
                        wide_ref[head, pl.ds(start, CHUNK), :] = result[:, :WIDTH].astype(bf16)
                        low_ref[head, pl.ds(start, CHUNK), :] = result[:, WIDTH:]
            return carry

        lax.fori_loop(0, count // READ, some, 0)


def read_call(query, query_conv, rim, gates, keys, late_keys, pairs, after, interpret=False):
    chunks, vheads = pairs.shape[:2]
    tokens = chunks * CHUNK
    qheads = query_conv.shape[1]
    return pl.pallas_call(
        read_kernel,
        out_shape=(
            jax.ShapeDtypeStruct((vheads, tokens, WIDTH), f32),
            jax.ShapeDtypeStruct((vheads, tokens, WIDTH), bf16),
            jax.ShapeDtypeStruct((8, WIDTH), f32),
        ),
        in_specs=[OUTSIDE] + [INSIDE] * 6 + [pl.BlockSpec(memory_space=pl.ANY)],
        out_specs=(INSIDE,) * 3,
        scratch_shapes=[
            pltpu.VMEM(((PAD + tokens) * qheads, WIDTH), f32),
            pltpu.SemaphoreType.DMA((1, chunks)),
        ],
        compiler_params=pltpu.CompilerParams(vmem_limit_bytes=16 * MIB),
        cost_estimate=pl.CostEstimate(flops=1 << 32, transcendentals=0, bytes_accessed=0),
        interpret=interpret,
        name="read_out",
    )(
        stay(query.reshape(tokens * qheads, WIDTH)), query_conv, rim, gates, keys, late_keys,
        pairs, after,
    )


def rim_kernel(q_hbm, k_hbm, v_hbm, rim_ref, sems):
    first = 0
    copies = []
    for i, (source, heads) in enumerate(((q_hbm, 2), (k_hbm, 2), (v_hbm, 4))):
        rows = RIM * heads
        copies.append(
            pltpu.make_async_copy(
                source.at[pl.ds(source.shape[0] - rows, rows), :],
                rim_ref.at[pl.ds(first, rows), :],
                sems.at[i],
            )
        )
        first += rows
    for copy in copies:
        copy.start()
    for copy in copies:
        copy.wait()


def rim_call(query, key, value):
    flat = [stay(x.reshape(-1, WIDTH)) for x in (query, key, value)]
    rows = RIM * (query.shape[1] + key.shape[1] + value.shape[1])
    return pl.pallas_call(
        rim_kernel,
        out_shape=jax.ShapeDtypeStruct((rows, WIDTH), f32),
        in_specs=[pl.BlockSpec(memory_space=pltpu.HBM)] * 3,
        out_specs=pl.BlockSpec(memory_space=pltpu.VMEM),
        scratch_shapes=[pltpu.SemaphoreType.DMA((3,))],
        compiler_params=pltpu.CompilerParams(vmem_limit_bytes=1024 * 1024),
        name="rim",
    )(*flat)


def total_kernel(place_ref, mine_ref, other_ref, total_ref, first_ref):
    core = place_ref[2]
    for h in range(mine_ref.shape[0]):
        mine, other = mine_ref[h], other_ref[h]
        first = jnp.where(core == 0, mine, other)
        second = jnp.where(core == 0, other, mine)
        joined = mm(second[:, :WIDTH], first)
        total_ref[h] = jnp.concatenate(
            [joined[:, :WIDTH], joined[:, WIDTH:] + second[:, WIDTH:].astype(f32)], axis=1
        ).astype(bf16)
        first_ref[h] = first


def row_kernel(place_ref, a_ref, b_ref, c_ref, d_ref, mark_ref, total_ref, before_ref, all_ref, sum_ref):
    here = place_ref[1]
    heads = a_ref.shape[0]
    for k, ref in enumerate((a_ref, b_ref, c_ref, d_ref)):
        all_ref[(here + 4 - k) % 4] = ref[...]
    eye = lax.broadcasted_iota(jnp.int32, (WIDTH, 2 * WIDTH), 0) == lax.broadcasted_iota(
        jnp.int32, (WIDTH, 2 * WIDTH), 1
    )
    for h in range(heads):
        sum_ref[0, h] = eye.astype(f32).astype(bf16)
        sum_ref[1, h] = all_ref[0, h]
    for j in range(1, 4):
        for h in range(heads):
            joined = mm(all_ref[j, h, :, :WIDTH], sum_ref[j, h])
            value = jnp.concatenate(
                [joined[:, :WIDTH], joined[:, WIDTH:] + all_ref[j, h, :, WIDTH:].astype(f32)],
                axis=1,
            ).astype(bf16)
            if j < 3:
                sum_ref[j + 1, h] = value
            else:
                total_ref[h] = value
    before_ref[...] = sum_ref[here]


def prefix_kernel(
    place_ref, b_ref, c_ref, d_ref, before_ref, first_ref, mark_ref,
    mine_ref, send_ref, all_ref, sum_ref,
):
    here = place_ref[0]
    core = place_ref[2]
    heads = b_ref.shape[0]
    for k, ref in enumerate((b_ref, c_ref, d_ref)):
        all_ref[(here + 3 - k) % 4] = ref[...]
    for h in range(heads):
        sum_ref[0, h] = jnp.zeros((WIDTH, WIDTH), bf16)
        sum_ref[1, h] = all_ref[0, h, :, WIDTH:]
    for j in range(1, 3):
        for h in range(heads):
            moved = mm(all_ref[j, h, :, :WIDTH], sum_ref[j, h])
            sum_ref[j + 1, h] = (moved + all_ref[j, h, :, WIDTH:].astype(f32)).astype(bf16)
    for h in range(heads):
        row = sum_ref[here, h]
        before = (
            mm(before_ref[h, :, :WIDTH], row) + before_ref[h, :, WIDTH:].astype(f32)
        ).astype(bf16)
        after = mm(first_ref[h, :, :WIDTH], before) + first_ref[h, :, WIDTH:].astype(f32)
        wide = before.astype(f32)
        mine_ref[h] = jnp.where(core == 0, wide, after).astype(bf16)
        send_ref[h] = jnp.where(core == 0, after, wide).astype(bf16)


def small_call(kernel, outs, scratch, name, place, *arrays):
    inside = pl.BlockSpec(memory_space=pltpu.VMEM)
    return pl.pallas_call(
        kernel,
        out_shape=tuple(jax.ShapeDtypeStruct(shape, bf16) for shape in outs),
        in_specs=[pl.BlockSpec(memory_space=pltpu.SMEM)] + [inside] * len(arrays),
        out_specs=(inside,) * len(outs),
        scratch_shapes=[pltpu.VMEM(shape, bf16) for shape in scratch],
        compiler_params=pltpu.CompilerParams(vmem_limit_bytes=8 * 1024 * 1024),
        name=name,
    )(place, *arrays)


def output_kernel(
    place_ref, low_ref, wide_ref, near_ref, far_ref, gate_ref, gain_ref, weight_ref,
    *out_refs, slots
):
    core = place_ref[2]
    heads = low_ref.shape[0]
    half = heads // 2
    rows = out_refs[0].shape[0]
    for index, slot in enumerate(slots):
        start = pl.multiple_of(place_ref[3 + slot] * rows, rows)
        pieces = []
        for h in range(heads):
            entering = jnp.where(core == h // half, near_ref[h % half], far_ref[h % half])
            recurrent = low_ref[h, pl.ds(start, rows), :] + mm(
                wide_ref[h, pl.ds(start, rows), :], entering
            )
            scaled = recurrent * lax.rsqrt(
                jnp.mean(recurrent * recurrent, axis=1, keepdims=True) + norm_epsilon
            )
            gate = gate_ref[pl.ds(start * heads + h, rows, stride=heads), :]
            pieces.append((scaled * gain_ref[...] * silu(gate)).astype(bf16))
        normed = jnp.concatenate(pieces, axis=1)
        side = out_refs[0].shape[1]
        for k in range(2):
            out_refs[2 * index + k][...] = mm(
                normed, weight_ref[:, k * side : (k + 1) * side]
            ).astype(bf16)


def output_call(place, slots, low, wide, near, far, gate_in, norm_gain, out_weight):
    heads, tokens, _ = low.shape
    model = out_weight.shape[1]
    rows = tokens // 8
    inside = pl.BlockSpec(memory_space=pltpu.VMEM)
    piece = jax.ShapeDtypeStruct((rows, model // 2), bf16)
    return pl.pallas_call(
        functools.partial(output_kernel, slots=slots),
        out_shape=(piece,) * (2 * len(slots)),
        in_specs=[pl.BlockSpec(memory_space=pltpu.SMEM)] + [inside] * 7,
        out_specs=(inside,) * (2 * len(slots)),
        compiler_params=pltpu.CompilerParams(vmem_limit_bytes=16 * 1024 * 1024),
        cost_estimate=pl.CostEstimate(
            flops=2 * rows * heads * WIDTH * model * len(slots), transcendentals=0, bytes_accessed=0
        ),
        name="gated_output",
    )(
        place, low, wide, near, far,
        gate_in.reshape(tokens * heads, WIDTH), norm_gain.reshape(1, WIDTH), out_weight,
    )


def add_kernel(left_ref, right_ref, out_ref):
    out_ref[...] = (left_ref[...].astype(f32) + right_ref[...].astype(f32)).astype(bf16)


def add(left, right):
    inside = pl.BlockSpec(memory_space=pltpu.VMEM)
    return pl.pallas_call(
        add_kernel,
        out_shape=jax.ShapeDtypeStruct(left.shape, bf16),
        in_specs=[inside] * 2,
        out_specs=inside,
        compiler_params=pltpu.CompilerParams(vmem_limit_bytes=2 * 1024 * 1024),
        name="add",
    )(left, right)


def last_kernel(*refs):
    out_ref = refs[-1]
    side = refs[0].shape[1]
    for k in range(2):
        total = refs[k][...].astype(f32)
        for other in (refs[2 + k], refs[4 + k]):
            total = total + other[...].astype(f32)
        out_ref[:, k * side : (k + 1) * side] = total


def last_call(*arrays):
    rows, side = arrays[0].shape
    inside = pl.BlockSpec(memory_space=pltpu.VMEM)
    return pl.pallas_call(
        last_kernel,
        out_shape=jax.ShapeDtypeStruct((rows, 2 * side), f32),
        in_specs=[inside] * 6,
        out_specs=inside,
        compiler_params=pltpu.CompilerParams(vmem_limit_bytes=8 * 1024 * 1024),
        name="last_add",
    )(*arrays)


def shifted(value, axis, steps, around=True):
    count = lax.axis_size(axis)
    pairs = [(i, (i + steps) % count) for i in range(count) if around or 0 <= i + steps < count]
    return lax.ppermute(value, axis, pairs)


def head_sum(parts):
    def right(value):
        return shifted(value, "head", 1)

    def left(value):
        return shifted(value, "head", -1)

    far, up_parts, down_parts, own = parts[0], parts[1:7:2], parts[2:7:2], parts[7]
    up = [right(far[0]), right(up_parts[0][1])]
    down = [left(down_parts[0][0]), left(far[1])]
    up = [right(add(up_parts[0][0], up[0])), up[1]]
    down = [down[0], left(add(down_parts[0][1], down[1]))]
    for step in (1, 2):
        for side in (1, 0):
            up[side] = right(add(up_parts[step][side], up[side]))
            down[1 - side] = left(add(down_parts[step][1 - side], down[1 - side]))
    return last_call(*own, *up, *down)


def on_device(
    query_in, key_in, value_in, gate_in, log_gate, strength,
    query_conv, key_conv, value_conv, norm_gain, out_weight,
):
    z = lax.axis_index("head")
    order = [(z + shift) & 7 for shift in (4, 3, 5, 2, 6, 1, 7, 0)]
    place = jnp.stack(
        [lax.axis_index("ctx_0"), lax.axis_index("ctx_1"), lax.axis_index("ctx_2")] + order
    ).astype(jnp.int32)
    rim = shifted(rim_call(query_in, key_in, value_in), CTX, 1, around=False)
    vheads, tokens = log_gate.shape
    gates = jnp.concatenate(
        [
            log_gate.reshape(vheads, tokens // CHUNK, CHUNK),
            strength.reshape(vheads, tokens // CHUNK, CHUNK),
        ],
        axis=0,
    ).transpose(1, 0, 2)
    late = late_call(key_in, value_in, key_conv, value_conv, gates)
    keys, write, ends, solved, fresh, mine, other = local_call(
        place, key_in, value_in, key_conv, value_conv, rim, gates, late
    )
    other = shifted(other, "ctx_2", 1)
    half = vheads // 2
    maps = (half, WIDTH, 2 * WIDTH)
    states = (half, WIDTH, WIDTH)
    total, first = small_call(total_kernel, (maps, maps), (), "chip_total", place, mine, other)
    pairs, mark = chain_call(solved, fresh, write, ends, late[3], late[4], first)
    row = [shifted(total, "ctx_1", k) for k in range(1, 4)]
    row_total, before = small_call(
        row_kernel, (maps, maps), ((4,) + maps, (4,) + maps), "row_total", place, total, *row, mark
    )
    rows = [shifted(row_total, "ctx_0", k, around=False) for k in range(1, 4)]
    low, wide, mark = read_call(
        query_in, query_conv, rim, gates, keys, late[0], pairs, before
    )
    near, send = small_call(
        prefix_kernel, (states, states), ((4,) + maps, (4,) + states), "prefix",
        place, *rows, before, first, mark,
    )
    far = shifted(send, "ctx_2", 1)
    tail = (low, wide, near, far, gate_in, norm_gain, out_weight)
    parts = []
    for slots in ((0, 1, 2), (3, 4), (5, 6, 7)):
        pieces = output_call(place, slots, *tail)
        parts += [pieces[2 * i : 2 * i + 2] for i in range(len(slots))]
    return head_sum(parts)


def solution(mesh):
    split = Mesh(
        mesh.devices.reshape(4, 4, 2, mesh.shape["head"]), ("ctx_0", "ctx_1", "ctx_2", "head")
    )
    in_specs = (
        P(CTX, "head", None),
        P(CTX, "head", None),
        P(CTX, "head", None),
        P(CTX, "head", None),
        P("head", CTX),
        P("head", CTX),
        P(None, "head", None),
        P(None, "head", None),
        P(None, "head", None),
        P(),
        P("head", None),
    )
    return jax.shard_map(
        on_device, mesh=split, in_specs=in_specs, out_specs=P(CTX_HEAD, None), check_vma=False
    )
```

```python
import functools
import jax
import jax.numpy as jnp
from jax import lax
from jax.experimental import pallas as pl
from jax.experimental.pallas import tpu as pltpu
from jax.sharding import Mesh
from jax.sharding import PartitionSpec as P

CTX = ("ctx_0", "ctx_1", "ctx_2")
CTX_HEAD = ("ctx_0", "ctx_1", "ctx_2", "head")
CHUNK = 128
WIDTH = 128
PAD = 8
RIM = 4
READ = 2
norm_epsilon = 1e-06
LOG2E = 1.4426950408889634
f32 = jnp.float32
bf16 = jnp.bfloat16


def mm(left, right):
    return jnp.dot(left, right, preferred_element_type=f32)


def silu_of_half(half):
    return half + half * jnp.tanh(half)


def silu(u):
    return silu_of_half(0.5 * u)


def paired(x):
    zero = jnp.zeros((CHUNK, CHUNK), x.dtype)
    top = jnp.concatenate([x[:, :CHUNK], zero], axis=1)
    low = jnp.concatenate([zero, x[:, CHUNK:]], axis=1)
    return jnp.concatenate([top, low], axis=0)


def mix(target, weight_ref, heads, head, start):
    total = None
    for tap in range(4):
        piece = target[pl.ds((start + PAD - 3 + tap) * heads + head, CHUNK, stride=heads), :]
        part = (0.5 * weight_ref[tap, head : head + 1, :]) * piece
        total = part if total is None else total + part
    return silu_of_half(total)


def unit(x):
    return x * lax.rsqrt(jnp.sum(x * x, axis=1, keepdims=True) + norm_epsilon)


def squares():
    row = lax.broadcasted_iota(jnp.int32, (CHUNK, CHUNK), 0)
    col = lax.broadcasted_iota(jnp.int32, (CHUNK, CHUNK), 1)
    return row, col


def running_sums(gates, adder):
    hi = gates.astype(bf16).astype(f32)
    rest = gates - hi
    mid = rest.astype(bf16).astype(f32)
    parts = jnp.concatenate([hi, mid, rest - mid], axis=0).astype(bf16)
    sums = mm(parts, adder)
    return (sums[0:8] + sums[8:16] + sums[16:24]) * LOG2E


def spread(columns, index):
    return jnp.broadcast_to(columns[:, index : index + 1], (CHUNK, CHUNK))


def fill_pad(pad, source, heads, rim_ref, first):
    pad[pl.ds((PAD - RIM) * heads, RIM * heads), :] = rim_ref[first : first + RIM * heads, :]
    pad[pl.ds(PAD * heads, CHUNK * heads), :] = source[pl.ds(0, CHUNK * heads), :]


def rows_of(source, pad, chunk):
    if isinstance(chunk, int) and chunk == 0:
        return pad, 0
    return source, chunk * CHUNK - PAD


def together(*steps):
    live = list(steps)
    while live:
        still = []
        for step, weight in live:
            alive = True
            for _ in range(weight):
                if next(step, "end") == "end":
                    alive = False
                    break
            if alive:
                still.append((step, weight))
        live = still


def prepare(group, first, sources, pads, weights, gate_ref, store):
    kw_ref, vw_ref = weights
    key_ref, mixing_ref, value_ref, write_ref, rows_ref = store
    qheads = kw_ref.shape[1]
    vheads = vw_ref.shape[1]
    ratio = vheads // qheads
    row1, col1 = squares()
    strict = row1 > col1
    adder = (row1 <= col1).astype(bf16)
    for i in group:
        (k_rows, start), (v_rows, _) = [
            rows_of(source, pad, first + i) for source, pad in zip(sources, pads)
        ]
        gates = gate_ref[first + i]
        running = running_sums(gates, adder)
        strengths = gates[4:8]
        scaled = running[0:4] + jnp.log2(strengths)
        columns = jnp.concatenate([scaled, scaled], axis=0).T
        end_row = running[:, CHUNK - 1 : CHUNK]
        tail_row = jnp.exp2(end_row - running)
        rows_ref[i, 0:4, :] = -jnp.exp2(scaled)
        rows_ref[i, 4:8, :] = strengths
        rows_ref[i, 8:16, :] = jnp.broadcast_to(jnp.exp2(end_row), (8, CHUNK))
        for g in range(qheads):
            key = unit(mix(k_rows, kw_ref, qheads, g, start))
            key_t = key.T
            packed = key.astype(bf16)
            key_ref[i, g] = packed
            kk = mm(packed, key_t.astype(bf16))
            yield
            for side in range(ratio):
                head = g * ratio + side
                table = jnp.where(
                    strict, jnp.exp2(spread(columns, head) - running[head : head + 1, :]), 0.0
                )
                lanes = slice(side * CHUNK, (side + 1) * CHUNK)
                mixing_ref[i, g, :, lanes] = (kk * table).astype(bf16)
                write_ref[i, head] = (key_t * tail_row[head : head + 1, :]).astype(bf16)
                value_ref[i, head] = mix(v_rows, vw_ref, vheads, head, start).astype(bf16)
                yield


def invert(first, store, mask_ref, solved_ref, fresh_ref):
    key_ref, mixing_ref, value_ref, write_ref, rows_ref = store
    count, qheads = mixing_ref.shape[:2]
    ratio = value_ref.shape[1] // qheads
    units = [(i, g) for i in range(count) for g in range(qheads)]

    def mixing(level):
        return [mixing_ref[i, g] * mask_ref[level] for i, g in units]

    eye = mask_ref[4]
    powers = mixing(0)
    inverses = [eye - p for p in powers]
    powers = [mm(p, paired(p)).astype(bf16) for p in powers]
    yield
    for step in range(3):
        inverses = [mm(eye + p, paired(x)).astype(bf16) for p, x in zip(powers, inverses)]
        yield
        if step < 2:
            powers = [mm(p, paired(p)).astype(bf16) for p in powers]
            yield
    for level in range(3):
        crossed = [
            eye - mm(m, paired(x)).astype(bf16) for m, x in zip(mixing(1 + level), inverses)
        ]
        yield
        inverses = [mm(x, paired(y)) for x, y in zip(inverses, crossed)]
        if level < 2:
            inverses = [x.astype(bf16) for x in inverses]
        yield
    for (i, g), inverse in zip(units, inverses):
        for side in range(ratio):
            head = g * ratio + side
            own = inverse[:, side * CHUNK : (side + 1) * CHUNK]
            left = jnp.concatenate(
                [own * rows_ref[i, head : head + 1, :], own * rows_ref[i, 4 + head : 5 + head, :]],
                axis=1,
            ).astype(bf16)
            right = jnp.concatenate([key_ref[i, g], value_ref[i, head]], axis=1)
            answer = mm(left, paired(right))
            solved_ref[first + i, head] = answer[:, :CHUNK].astype(bf16)
            fresh_ref[first + i, head] = answer[:, CHUNK:]
        yield


def join(later, earlier):
    keep1, change1, offset1 = later
    keep0, change0, offset0 = earlier
    moved = mm(change1.astype(bf16), jnp.concatenate([change0, offset0], axis=1).astype(bf16))
    return (
        keep1 * keep0,
        moved[:, :WIDTH] + (keep1 * change0 + keep0 * change1),
        moved[:, WIDTH:] + (keep1 * offset0 + offset1),
    )


def chain_maps(first, store, solved_ref, fresh_ref, vheads, result):
    _, _, _, write_ref, rows_ref = store
    maps = []
    for i in range(write_ref.shape[0]):
        row = []
        for h in range(vheads):
            moved = mm(
                write_ref[i, h],
                jnp.concatenate(
                    [solved_ref[first + i, h], fresh_ref[first + i, h].astype(bf16)], axis=1
                ),
            )
            row.append((rows_ref[i, 8 + h : 9 + h, :], moved[:, :WIDTH], moved[:, WIDTH:]))
        maps.append(row)
        yield
    while len(maps) > 1:
        maps = [
            [join(later, earlier) for later, earlier in zip(maps[k + 1], maps[k])]
            for k in range(0, len(maps), 2)
        ]
        yield
    result.extend(maps[0])


def late_kernel(
    place_ref, k_ref, v_ref, kw_ref, vw_ref, gate_ref,
    key_ref, mixing_ref, value_ref, write_ref, rows_ref,
):
    count = key_ref.shape[0]
    store = (key_ref, mixing_ref, value_ref, write_ref, rows_ref)
    group = prepare(
        range(count), gate_ref.shape[0] - count, (k_ref, v_ref), (None, None), (kw_ref, vw_ref),
        gate_ref, store,
    )
    together((group, 1))


def local_kernel(
    place_ref, k_ref, v_ref, kw_ref, vw_ref, rim_ref, gate_ref,
    late_key_ref, late_mixing_ref, late_value_ref, late_write_ref, late_rows_ref,
    key_ref, write_ref, rows_ref, solved_ref, fresh_ref, near_ref, far_ref,
    mixing_ref, value_ref, k_pad, v_pad, mask_ref,
):
    core = place_ref[2]
    chunks = gate_ref.shape[0]
    count = key_ref.shape[0]
    qheads = kw_ref.shape[1]
    vheads = vw_ref.shape[1]
    fill_pad(k_pad, k_ref, qheads, rim_ref, RIM * qheads)
    fill_pad(v_pad, v_ref, vheads, rim_ref, 2 * RIM * qheads)
    row = lax.broadcasted_iota(jnp.int32, (CHUNK, 2 * CHUNK), 0)
    col = lax.broadcasted_iota(jnp.int32, (CHUNK, 2 * CHUNK), 1) & (CHUNK - 1)

    def same(bits):
        return (row >> bits) == (col >> bits)

    mask_ref[0] = same(4).astype(bf16)
    for level in range(3):
        mask_ref[1 + level] = (same(5 + level) & jnp.logical_not(same(4 + level))).astype(bf16)
    mask_ref[4] = (row == col).astype(bf16)
    early = (key_ref, mixing_ref, value_ref, write_ref, rows_ref)
    late = (late_key_ref, late_mixing_ref, late_value_ref, late_write_ref, late_rows_ref)
    first_half, second_half = [], []
    together(
        (invert(chunks - count, late, mask_ref, solved_ref, fresh_ref), 1),
        (
            prepare(
                range(count), 0, (k_ref, v_ref), (k_pad, v_pad), (kw_ref, vw_ref), gate_ref, early
            ),
            2,
        ),
    )
    together(
        (invert(0, early, mask_ref, solved_ref, fresh_ref), 2),
        (chain_maps(chunks - count, late, solved_ref, fresh_ref, vheads, second_half), 1),
    )
    together((chain_maps(0, early, solved_ref, fresh_ref, vheads, first_half), 1))
    half = vheads // 2
    row1, col1 = squares()
    for h in range(vheads):
        keep, change, offset = join(second_half[h], first_half[h])
        packed = jnp.concatenate(
            [change + jnp.where(row1 == col1, keep, 0.0), offset], axis=1
        ).astype(bf16)

        @pl.when(core == h // half)
        def _():
            near_ref[h % half] = packed

        @pl.when(core != h // half)
        def _():
            far_ref[h % half] = packed


def stay(value):
    return pltpu.with_memory_space_constraint(value, pltpu.HBM)


INSIDE = pl.BlockSpec(memory_space=pltpu.VMEM)
SCALAR = pl.BlockSpec(memory_space=pltpu.SMEM)
MIB = 1024 * 1024


def group_shapes(count, qheads, vheads):
    return (
        jax.ShapeDtypeStruct((count, qheads, CHUNK, WIDTH), bf16),
        jax.ShapeDtypeStruct((count, qheads, CHUNK, 2 * CHUNK), bf16),
        jax.ShapeDtypeStruct((count, vheads, CHUNK, WIDTH), bf16),
        jax.ShapeDtypeStruct((count, vheads, CHUNK, CHUNK), bf16),
        jax.ShapeDtypeStruct((count, 16, CHUNK), f32),
    )


def pad_scratch(heads):
    return pltpu.VMEM(((PAD + CHUNK) * heads, WIDTH), f32)


def late_call(place, key, value, key_conv, value_conv, gates, interpret=False):
    count = gates.shape[0] // 2
    return pl.pallas_call(
        late_kernel,
        out_shape=group_shapes(count, key_conv.shape[1], value_conv.shape[1]),
        in_specs=[SCALAR] + [INSIDE] * 5,
        out_specs=(INSIDE,) * 5,
        compiler_params=pltpu.CompilerParams(vmem_limit_bytes=12 * MIB),
        cost_estimate=pl.CostEstimate(flops=1 << 32, transcendentals=0, bytes_accessed=0),
        interpret=interpret,
        name="late_half",
    )(place, key.reshape(-1, WIDTH), value.reshape(-1, WIDTH), key_conv, value_conv, gates)


def local_call(place, key, value, key_conv, value_conv, rim, gates, late, interpret=False):
    chunks = gates.shape[0]
    count = chunks // 2
    qheads = key_conv.shape[1]
    vheads = value_conv.shape[1]
    shapes = group_shapes(count, qheads, vheads)
    pair = jax.ShapeDtypeStruct((vheads // 2, WIDTH, 2 * WIDTH), bf16)
    return pl.pallas_call(
        local_kernel,
        out_shape=(
            shapes[0],
            shapes[3],
            shapes[4],
            jax.ShapeDtypeStruct((chunks, vheads, CHUNK, WIDTH), bf16),
            jax.ShapeDtypeStruct((chunks, vheads, CHUNK, WIDTH), f32),
            pair,
            pair,
        ),
        in_specs=[SCALAR] + [INSIDE] * 11,
        out_specs=(INSIDE,) * 7,
        scratch_shapes=[
            pltpu.VMEM(shapes[1].shape, bf16),
            pltpu.VMEM(shapes[2].shape, bf16),
            pad_scratch(qheads),
            pad_scratch(vheads),
            pltpu.VMEM((5, CHUNK, 2 * CHUNK), bf16),
        ],
        compiler_params=pltpu.CompilerParams(vmem_limit_bytes=20 * MIB),
        interpret=interpret,
        name="local_map",
    )(
        place, key.reshape(-1, WIDTH), value.reshape(-1, WIDTH), key_conv, value_conv, rim,
        gates, *late,
    )


def read_chunk(chunk, i, rows, start, qw_ref, gate_ref, key_ref, pair_ref, low_ref, wide_ref):
    qheads = qw_ref.shape[1]
    ratio = pair_ref.shape[1] // qheads
    row1, col1 = squares()
    running = running_sums(gate_ref[chunk], (row1 <= col1).astype(bf16))
    columns = running.T
    target = pl.ds(pl.multiple_of(chunk * CHUNK, CHUNK), CHUNK)
    for g in range(qheads):
        query = unit(mix(rows, qw_ref, qheads, g, start)) * (WIDTH ** -0.5)
        qk = lax.dot_general(
            query.astype(bf16), key_ref[i, g], (((1,), (1,)), ((), ())),
            preferred_element_type=f32,
        )
        for side in range(ratio):
            head = g * ratio + side
            decay_col = spread(columns, head)
            table = jnp.where(
                row1 >= col1, jnp.exp2(decay_col - running[head : head + 1, :]), 0.0
            )
            lift = jnp.exp2(decay_col)
            reading = jnp.concatenate(
                [(lift * query).astype(bf16), (qk * table).astype(bf16)], axis=1
            )
            result = mm(reading, pair_ref[chunk, head])
            wide_ref[head, target, :] = result[:, :WIDTH].astype(bf16)
            low_ref[head, target, :] = result[:, WIDTH:]


def chain_kernel(
    solved_ref, fresh_ref, write_ref, rows_ref, late_write_ref, late_rows_ref,
    q_ref, qw_ref, rim_ref, gate_ref, key_ref, after_ref,
    pair_ref, low_ref, wide_ref, mark_ref, hold_ref, q_pad,
):
    chunks, vheads = solved_ref.shape[:2]
    count = write_ref.shape[0]
    mark_ref[...] = jnp.zeros_like(mark_ref)
    fill_pad(q_pad, q_ref, qw_ref.shape[1], rim_ref, 0)
    row1, col1 = squares()
    for h in range(vheads):
        hold_ref[h] = jnp.concatenate(
            [(row1 == col1).astype(f32), jnp.zeros((CHUNK, CHUNK), f32)], axis=1
        )

    def advance(chunk, writes, ends, i):
        states = [hold_ref[h] for h in range(vheads)]
        packed = [s.astype(bf16) for s in states]
        taken = [mm(solved_ref[chunk, h], packed[h]) for h in range(vheads)]
        updates = [
            jnp.concatenate(
                [taken[h][:, :WIDTH], fresh_ref[chunk, h] + taken[h][:, WIDTH:]], axis=1
            ).astype(bf16)
            for h in range(vheads)
        ]
        for h in range(vheads):
            pair_ref[chunk, h, :CHUNK, :] = packed[h]
            pair_ref[chunk, h, CHUNK:, :] = updates[h]
            end = ends[i, 8 + h : 9 + h, :]
            hold_ref[h] = states[h] * jnp.concatenate([end, end], axis=1) + mm(
                writes[i, h], updates[h]
            )

    def read(chunk):
        rows, start = rows_of(q_ref, q_pad, chunk)
        read_chunk(
            chunk, chunk, rows, start, qw_ref, gate_ref, key_ref, pair_ref, low_ref, wide_ref
        )

    def early_step(i, carry):
        advance(i, write_ref, rows_ref, i)
        read(i)
        return carry

    def late_step(i, carry):
        advance(count + i, late_write_ref, late_rows_ref, i)
        return carry

    advance(0, write_ref, rows_ref, 0)
    read(0)
    lax.fori_loop(1, count, early_step, 0)
    lax.fori_loop(0, count, late_step, 0)


def chain_call(
    solved, fresh, write, rows, late_write, late_rows, query, query_conv, rim, gates, keys, after,
    interpret=False,
):
    chunks, vheads = solved.shape[:2]
    tokens = chunks * CHUNK
    return pl.pallas_call(
        chain_kernel,
        out_shape=(
            jax.ShapeDtypeStruct((chunks, vheads, 2 * CHUNK, 2 * WIDTH), bf16),
            jax.ShapeDtypeStruct((vheads, tokens, WIDTH), f32),
            jax.ShapeDtypeStruct((vheads, tokens, WIDTH), bf16),
            jax.ShapeDtypeStruct((8, WIDTH), f32),
        ),
        in_specs=[INSIDE] * 11 + [pl.BlockSpec(memory_space=pl.ANY)],
        out_specs=(INSIDE,) * 4,
        scratch_shapes=[
            pltpu.VMEM((vheads, WIDTH, 2 * WIDTH), f32), pad_scratch(query_conv.shape[1])
        ],
        compiler_params=pltpu.CompilerParams(vmem_limit_bytes=20 * MIB),
        cost_estimate=pl.CostEstimate(flops=1 << 32, transcendentals=0, bytes_accessed=0),
        interpret=interpret,
        name="chain",
    )(
        solved, fresh, write, rows, late_write, late_rows, query.reshape(-1, WIDTH), query_conv,
        rim, gates, keys, after,
    )


def read_kernel(
    q_ref, qw_ref, gate_ref, late_key_ref, pair_ref, old_low_ref, old_wide_ref, after_ref,
    low_ref, wide_ref, mark_ref,
):
    mark_ref[...] = jnp.zeros_like(mark_ref)
    count = late_key_ref.shape[0]
    chunks = gate_ref.shape[0]
    done = (chunks - count) * CHUNK
    low_ref[:, :done, :] = old_low_ref[:, :done, :]
    wide_ref[:, :done, :] = old_wide_ref[:, :done, :]

    def some(step, carry):
        for inner in range(READ):
            i = step * READ + inner
            chunk = chunks - count + i
            read_chunk(
                chunk, i, q_ref, chunk * CHUNK - PAD, qw_ref, gate_ref, late_key_ref, pair_ref,
                low_ref, wide_ref,
            )
        return carry

    lax.fori_loop(0, count // READ, some, 0)


def read_call(query, query_conv, gates, late_keys, pairs, low, wide, after, interpret=False):
    return pl.pallas_call(
        read_kernel,
        out_shape=(
            jax.ShapeDtypeStruct(low.shape, f32),
            jax.ShapeDtypeStruct(wide.shape, bf16),
            jax.ShapeDtypeStruct((8, WIDTH), f32),
        ),
        in_specs=[INSIDE] * 7 + [pl.BlockSpec(memory_space=pl.ANY)],
        out_specs=(INSIDE,) * 3,
        compiler_params=pltpu.CompilerParams(vmem_limit_bytes=20 * MIB),
        cost_estimate=pl.CostEstimate(flops=1 << 32, transcendentals=0, bytes_accessed=0),
        interpret=interpret,
        name="read_out",
    )(query.reshape(-1, WIDTH), query_conv, gates, late_keys, pairs, low, wide, after)


def rim_kernel(q_hbm, k_hbm, v_hbm, rim_ref, sems):
    first = 0
    copies = []
    for i, (source, heads) in enumerate(((q_hbm, 2), (k_hbm, 2), (v_hbm, 4))):
        rows = RIM * heads
        copies.append(
            pltpu.make_async_copy(
                source.at[pl.ds(source.shape[0] - rows, rows), :],
                rim_ref.at[pl.ds(first, rows), :],
                sems.at[i],
            )
        )
        first += rows
    for copy in copies:
        copy.start()
    for copy in copies:
        copy.wait()


def rim_call(query, key, value):
    flat = [stay(x.reshape(-1, WIDTH)) for x in (query, key, value)]
    rows = RIM * (query.shape[1] + key.shape[1] + value.shape[1])
    return pl.pallas_call(
        rim_kernel,
        out_shape=jax.ShapeDtypeStruct((rows, WIDTH), f32),
        in_specs=[pl.BlockSpec(memory_space=pltpu.HBM)] * 3,
        out_specs=pl.BlockSpec(memory_space=pltpu.VMEM),
        scratch_shapes=[pltpu.SemaphoreType.DMA((3,))],
        compiler_params=pltpu.CompilerParams(vmem_limit_bytes=1024 * 1024),
        name="rim",
    )(*flat)


def total_kernel(place_ref, mine_ref, other_ref, total_ref, first_ref):
    core = place_ref[2]
    for h in range(mine_ref.shape[0]):
        mine, other = mine_ref[h], other_ref[h]
        first = jnp.where(core == 0, mine, other)
        second = jnp.where(core == 0, other, mine)
        joined = mm(second[:, :WIDTH], first)
        total_ref[h] = jnp.concatenate(
            [joined[:, :WIDTH], joined[:, WIDTH:] + second[:, WIDTH:].astype(f32)], axis=1
        ).astype(bf16)
        first_ref[h] = first


def row_kernel(place_ref, a_ref, b_ref, c_ref, d_ref, mark_ref, total_ref, before_ref, all_ref, sum_ref):
    here = place_ref[1]
    heads = a_ref.shape[0]
    for k, ref in enumerate((a_ref, b_ref, c_ref, d_ref)):
        all_ref[(here + 4 - k) % 4] = ref[...]
    eye = lax.broadcasted_iota(jnp.int32, (WIDTH, 2 * WIDTH), 0) == lax.broadcasted_iota(
        jnp.int32, (WIDTH, 2 * WIDTH), 1
    )
    for h in range(heads):
        sum_ref[0, h] = eye.astype(f32).astype(bf16)
        sum_ref[1, h] = all_ref[0, h]
    for j in range(1, 4):
        for h in range(heads):
            joined = mm(all_ref[j, h, :, :WIDTH], sum_ref[j, h])
            value = jnp.concatenate(
                [joined[:, :WIDTH], joined[:, WIDTH:] + all_ref[j, h, :, WIDTH:].astype(f32)],
                axis=1,
            ).astype(bf16)
            if j < 3:
                sum_ref[j + 1, h] = value
            else:
                total_ref[h] = value
    before_ref[...] = sum_ref[here]


def prefix_kernel(
    place_ref, b_ref, c_ref, d_ref, before_ref, first_ref, mark_ref,
    mine_ref, send_ref, all_ref, sum_ref,
):
    here = place_ref[0]
    core = place_ref[2]
    heads = b_ref.shape[0]
    for k, ref in enumerate((b_ref, c_ref, d_ref)):
        all_ref[(here + 3 - k) % 4] = ref[...]
    for h in range(heads):
        sum_ref[0, h] = jnp.zeros((WIDTH, WIDTH), bf16)
        sum_ref[1, h] = all_ref[0, h, :, WIDTH:]
    for j in range(1, 3):
        for h in range(heads):
            moved = mm(all_ref[j, h, :, :WIDTH], sum_ref[j, h])
            sum_ref[j + 1, h] = (moved + all_ref[j, h, :, WIDTH:].astype(f32)).astype(bf16)
    for h in range(heads):
        row = sum_ref[here, h]
        before = (
            mm(before_ref[h, :, :WIDTH], row) + before_ref[h, :, WIDTH:].astype(f32)
        ).astype(bf16)
        after = mm(first_ref[h, :, :WIDTH], before) + first_ref[h, :, WIDTH:].astype(f32)
        wide = before.astype(f32)
        mine_ref[h] = jnp.where(core == 0, wide, after).astype(bf16)
        send_ref[h] = jnp.where(core == 0, after, wide).astype(bf16)


def small_call(kernel, outs, scratch, name, place, *arrays):
    inside = pl.BlockSpec(memory_space=pltpu.VMEM)
    return pl.pallas_call(
        kernel,
        out_shape=tuple(jax.ShapeDtypeStruct(shape, bf16) for shape in outs),
        in_specs=[pl.BlockSpec(memory_space=pltpu.SMEM)] + [inside] * len(arrays),
        out_specs=(inside,) * len(outs),
        scratch_shapes=[pltpu.VMEM(shape, bf16) for shape in scratch],
        compiler_params=pltpu.CompilerParams(vmem_limit_bytes=8 * 1024 * 1024),
        name=name,
    )(place, *arrays)


def output_kernel(
    place_ref, low_ref, wide_ref, near_ref, far_ref, gate_ref, gain_ref, weight_ref,
    *out_refs, slots
):
    core = place_ref[2]
    heads = low_ref.shape[0]
    half = heads // 2
    rows = out_refs[0].shape[0]
    for index, slot in enumerate(slots):
        start = pl.multiple_of(place_ref[3 + slot] * rows, rows)
        pieces = []
        for h in range(heads):
            entering = jnp.where(core == h // half, near_ref[h % half], far_ref[h % half])
            recurrent = low_ref[h, pl.ds(start, rows), :] + mm(
                wide_ref[h, pl.ds(start, rows), :], entering
            )
            scaled = recurrent * lax.rsqrt(
                jnp.mean(recurrent * recurrent, axis=1, keepdims=True) + norm_epsilon
            )
            gate = gate_ref[pl.ds(start * heads + h, rows, stride=heads), :]
            pieces.append((scaled * gain_ref[...] * silu(gate)).astype(bf16))
        normed = jnp.concatenate(pieces, axis=1)
        side = out_refs[0].shape[1]
        for k in range(2):
            out_refs[2 * index + k][...] = mm(
                normed, weight_ref[:, k * side : (k + 1) * side]
            ).astype(bf16)


def output_call(place, slots, low, wide, near, far, gate_in, norm_gain, out_weight):
    heads, tokens, _ = low.shape
    model = out_weight.shape[1]
    rows = tokens // 8
    inside = pl.BlockSpec(memory_space=pltpu.VMEM)
    piece = jax.ShapeDtypeStruct((rows, model // 2), bf16)
    return pl.pallas_call(
        functools.partial(output_kernel, slots=slots),
        out_shape=(piece,) * (2 * len(slots)),
        in_specs=[pl.BlockSpec(memory_space=pltpu.SMEM)] + [inside] * 7,
        out_specs=(inside,) * (2 * len(slots)),
        compiler_params=pltpu.CompilerParams(vmem_limit_bytes=16 * 1024 * 1024),
        cost_estimate=pl.CostEstimate(
            flops=2 * rows * heads * WIDTH * model * len(slots), transcendentals=0, bytes_accessed=0
        ),
        name="gated_output",
    )(
        place, low, wide, near, far,
        gate_in.reshape(tokens * heads, WIDTH), norm_gain.reshape(1, WIDTH), out_weight,
    )


def add_kernel(left_ref, right_ref, out_ref):
    out_ref[...] = (left_ref[...].astype(f32) + right_ref[...].astype(f32)).astype(bf16)


def add(left, right):
    inside = pl.BlockSpec(memory_space=pltpu.VMEM)
    return pl.pallas_call(
        add_kernel,
        out_shape=jax.ShapeDtypeStruct(left.shape, bf16),
        in_specs=[inside] * 2,
        out_specs=inside,
        compiler_params=pltpu.CompilerParams(vmem_limit_bytes=2 * 1024 * 1024),
        name="add",
    )(left, right)


def last_kernel(*refs):
    out_ref = refs[-1]
    side = refs[0].shape[1]
    for k in range(2):
        total = refs[k][...].astype(f32)
        for other in (refs[2 + k], refs[4 + k]):
            total = total + other[...].astype(f32)
        out_ref[:, k * side : (k + 1) * side] = total


def last_call(*arrays):
    rows, side = arrays[0].shape
    inside = pl.BlockSpec(memory_space=pltpu.VMEM)
    return pl.pallas_call(
        last_kernel,
        out_shape=jax.ShapeDtypeStruct((rows, 2 * side), f32),
        in_specs=[inside] * 6,
        out_specs=inside,
        compiler_params=pltpu.CompilerParams(vmem_limit_bytes=8 * 1024 * 1024),
        name="last_add",
    )(*arrays)


def shifted(value, axis, steps, around=True):
    count = lax.axis_size(axis)
    pairs = [(i, (i + steps) % count) for i in range(count) if around or 0 <= i + steps < count]
    return lax.ppermute(value, axis, pairs)


def head_sum(parts):
    def right(value):
        return shifted(value, "head", 1)

    def left(value):
        return shifted(value, "head", -1)

    far, up_parts, down_parts, own = parts[0], parts[1:7:2], parts[2:7:2], parts[7]
    up = [right(far[0]), right(up_parts[0][1])]
    down = [left(down_parts[0][0]), left(far[1])]
    up = [right(add(up_parts[0][0], up[0])), up[1]]
    down = [down[0], left(add(down_parts[0][1], down[1]))]
    for step in (1, 2):
        for side in (1, 0):
            up[side] = right(add(up_parts[step][side], up[side]))
            down[1 - side] = left(add(down_parts[step][1 - side], down[1 - side]))
    return last_call(*own, *up, *down)


def on_device(
    query_in, key_in, value_in, gate_in, log_gate, strength,
    query_conv, key_conv, value_conv, norm_gain, out_weight,
):
    z = lax.axis_index("head")
    order = [(z + shift) & 7 for shift in (4, 3, 5, 2, 6, 1, 7, 0)]
    place = jnp.stack(
        [lax.axis_index("ctx_0"), lax.axis_index("ctx_1"), lax.axis_index("ctx_2")] + order
    ).astype(jnp.int32)
    rim = shifted(rim_call(query_in, key_in, value_in), CTX, 1, around=False)
    vheads, tokens = log_gate.shape
    gates = jnp.concatenate(
        [
            log_gate.reshape(vheads, tokens // CHUNK, CHUNK),
            strength.reshape(vheads, tokens // CHUNK, CHUNK),
        ],
        axis=0,
    ).transpose(1, 0, 2)
    late = late_call(place, key_in, value_in, key_conv, value_conv, gates)
    keys, write, ends, solved, fresh, mine, other = local_call(
        place, key_in, value_in, key_conv, value_conv, rim, gates, late
    )
    other = shifted(other, "ctx_2", 1)
    half = vheads // 2
    maps = (half, WIDTH, 2 * WIDTH)
    states = (half, WIDTH, WIDTH)
    total, first = small_call(total_kernel, (maps, maps), (), "chip_total", place, mine, other)
    pairs, low, wide, mark = chain_call(
        solved, fresh, write, ends, late[3], late[4], query_in, query_conv, rim, gates, keys, first
    )
    row = [shifted(total, "ctx_1", k) for k in range(1, 4)]
    row_total, before = small_call(
        row_kernel, (maps, maps), ((4,) + maps, (4,) + maps), "row_total", place, total, *row, mark
    )
    rows = [shifted(row_total, "ctx_0", k, around=False) for k in range(1, 4)]
    low, wide, mark = read_call(
        query_in, query_conv, gates, late[0], pairs, low, wide, before
    )
    near, send = small_call(
        prefix_kernel, (states, states), ((4,) + maps, (4,) + states), "prefix",
        place, *rows, before, first, mark,
    )
    far = shifted(send, "ctx_2", 1)
    tail = (low, wide, near, far, gate_in, norm_gain, out_weight)
    parts = []
    for slots in ((0,), (1, 2), (3, 4), (5, 6, 7)):
        pieces = output_call(place, slots, *tail)
        parts += [pieces[2 * i : 2 * i + 2] for i in range(len(slots))]
    return head_sum(parts)


def solution(mesh):
    split = Mesh(
        mesh.devices.reshape(4, 4, 2, mesh.shape["head"]), ("ctx_0", "ctx_1", "ctx_2", "head")
    )
    in_specs = (
        P(CTX, "head", None),
        P(CTX, "head", None),
        P(CTX, "head", None),
        P(CTX, "head", None),
        P("head", CTX),
        P("head", CTX),
        P(None, "head", None),
        P(None, "head", None),
        P(None, "head", None),
        P(),
        P("head", None),
    )
    return jax.shard_map(
        on_device, mesh=split, in_specs=in_specs, out_specs=P(CTX_HEAD, None), check_vma=False
    )
```

```python
import functools
import jax
import jax.numpy as jnp
from jax import lax
from jax.experimental import pallas as pl
from jax.experimental.pallas import tpu as pltpu
from jax.sharding import Mesh
from jax.sharding import PartitionSpec as P

CTX = ("ctx_0", "ctx_1", "ctx_2")
CTX_HEAD = ("ctx_0", "ctx_1", "ctx_2", "head")
CHUNK = 128
WIDTH = 128
PAD = 8
RIM = 4
READ = 2
norm_epsilon = 1e-06
LOG2E = 1.4426950408889634
f32 = jnp.float32
bf16 = jnp.bfloat16


def mm(left, right):
    return jnp.dot(left, right, preferred_element_type=f32)


def silu_of_half(half):
    return half + half * jnp.tanh(half)


def silu(u):
    return silu_of_half(0.5 * u)


def paired(x):
    zero = jnp.zeros((CHUNK, CHUNK), x.dtype)
    top = jnp.concatenate([x[:, :CHUNK], zero], axis=1)
    low = jnp.concatenate([zero, x[:, CHUNK:]], axis=1)
    return jnp.concatenate([top, low], axis=0)


def mix(target, weight_ref, heads, head, start):
    total = None
    for tap in range(4):
        piece = target[pl.ds((start + PAD - 3 + tap) * heads + head, CHUNK, stride=heads), :]
        part = (0.5 * weight_ref[tap, head : head + 1, :]) * piece
        total = part if total is None else total + part
    return silu_of_half(total)


def unit(x):
    return x * lax.rsqrt(jnp.sum(x * x, axis=1, keepdims=True) + norm_epsilon)


def squares():
    row = lax.broadcasted_iota(jnp.int32, (CHUNK, CHUNK), 0)
    col = lax.broadcasted_iota(jnp.int32, (CHUNK, CHUNK), 1)
    return row, col


def running_sums(gates, adder):
    hi = gates.astype(bf16).astype(f32)
    rest = gates - hi
    mid = rest.astype(bf16).astype(f32)
    parts = jnp.concatenate([hi, mid, rest - mid], axis=0).astype(bf16)
    sums = mm(parts, adder)
    return (sums[0:8] + sums[8:16] + sums[16:24]) * LOG2E


def spread(columns, index):
    return jnp.broadcast_to(columns[:, index : index + 1], (CHUNK, CHUNK))


def fill_pad(pad, source, heads, rim_ref, first):
    pad[pl.ds((PAD - RIM) * heads, RIM * heads), :] = rim_ref[first : first + RIM * heads, :]
    pad[pl.ds(PAD * heads, CHUNK * heads), :] = source[pl.ds(0, CHUNK * heads), :]


def rows_of(source, pad, chunk):
    if isinstance(chunk, int) and chunk == 0:
        return pad, 0
    return source, chunk * CHUNK - PAD


def together(*steps):
    live = list(steps)
    while live:
        still = []
        for step, weight in live:
            alive = True
            for _ in range(weight):
                if next(step, "end") == "end":
                    alive = False
                    break
            if alive:
                still.append((step, weight))
        live = still


def fill_masks(mask_ref):
    row = lax.broadcasted_iota(jnp.int32, (CHUNK, 2 * CHUNK), 0)
    col = lax.broadcasted_iota(jnp.int32, (CHUNK, 2 * CHUNK), 1) & (CHUNK - 1)

    def same(bits):
        return (row >> bits) == (col >> bits)

    mask_ref[0] = same(4).astype(bf16)
    for level in range(3):
        mask_ref[1 + level] = (same(5 + level) & jnp.logical_not(same(4 + level))).astype(bf16)
    mask_ref[4] = (row == col).astype(bf16)


class View:
    def __init__(self, ref, base):
        self.ref, self.base = ref, base

    def __getitem__(self, key):
        return self.ref[(key[0] + self.base,) + key[1:]]

    def __setitem__(self, key, value):
        self.ref[(key[0] + self.base,) + key[1:]] = value


def prepare(group, first, sources, pads, weights, gate_ref, store):
    kw_ref, vw_ref = weights
    key_ref, mixing_ref, value_ref, write_ref, rows_ref = store
    qheads = kw_ref.shape[1]
    vheads = vw_ref.shape[1]
    ratio = vheads // qheads
    row1, col1 = squares()
    strict = row1 > col1
    adder = (row1 <= col1).astype(bf16)
    for i in group:
        (k_rows, start), (v_rows, _) = [
            rows_of(source, pad, first + i) for source, pad in zip(sources, pads)
        ]
        gates = gate_ref[first + i]
        running = running_sums(gates, adder)
        strengths = gates[4:8]
        scaled = running[0:4] + jnp.log2(strengths)
        columns = jnp.concatenate([scaled, scaled], axis=0).T
        end_row = running[:, CHUNK - 1 : CHUNK]
        tail_row = jnp.exp2(end_row - running)
        rows_ref[i, 0:4, :] = -jnp.exp2(scaled)
        rows_ref[i, 4:8, :] = strengths
        rows_ref[i, 8:16, :] = jnp.broadcast_to(jnp.exp2(end_row), (8, CHUNK))
        for g in range(qheads):
            key = unit(mix(k_rows, kw_ref, qheads, g, start))
            key_t = key.T
            packed = key.astype(bf16)
            key_ref[i, g] = packed
            kk = mm(packed, key_t.astype(bf16))
            yield
            for side in range(ratio):
                head = g * ratio + side
                table = jnp.where(
                    strict, jnp.exp2(spread(columns, head) - running[head : head + 1, :]), 0.0
                )
                lanes = slice(side * CHUNK, (side + 1) * CHUNK)
                mixing_ref[i, g, :, lanes] = (kk * table).astype(bf16)
                write_ref[i, head] = (key_t * tail_row[head : head + 1, :]).astype(bf16)
                value_ref[i, head] = mix(v_rows, vw_ref, vheads, head, start).astype(bf16)
                yield


def invert(count, store, qheads, vheads, mask_ref, solved_ref, fresh_ref):
    key_ref, mixing_ref, value_ref, write_ref, rows_ref = store
    ratio = vheads // qheads
    units = [(i, g) for i in range(count) for g in range(qheads)]

    def mixing(level):
        return [mixing_ref[i, g] * mask_ref[level] for i, g in units]

    eye = mask_ref[4]
    powers = mixing(0)
    inverses = [eye - p for p in powers]
    powers = [mm(p, paired(p)).astype(bf16) for p in powers]
    yield
    for step in range(3):
        inverses = [mm(eye + p, paired(x)).astype(bf16) for p, x in zip(powers, inverses)]
        yield
        if step < 2:
            powers = [mm(p, paired(p)).astype(bf16) for p in powers]
            yield
    for level in range(3):
        crossed = [
            eye - mm(m, paired(x)).astype(bf16) for m, x in zip(mixing(1 + level), inverses)
        ]
        yield
        inverses = [mm(x, paired(y)) for x, y in zip(inverses, crossed)]
        if level < 2:
            inverses = [x.astype(bf16) for x in inverses]
        yield
    for (i, g), inverse in zip(units, inverses):
        for side in range(ratio):
            head = g * ratio + side
            own = inverse[:, side * CHUNK : (side + 1) * CHUNK]
            left = jnp.concatenate(
                [own * rows_ref[i, head : head + 1, :], own * rows_ref[i, 4 + head : 5 + head, :]],
                axis=1,
            ).astype(bf16)
            right = jnp.concatenate([key_ref[i, g], value_ref[i, head]], axis=1)
            answer = mm(left, paired(right))
            solved_ref[i, head] = answer[:, :CHUNK].astype(bf16)
            fresh_ref[i, head] = answer[:, CHUNK:]
        yield


def join(later, earlier):
    keep1, change1, offset1 = later
    keep0, change0, offset0 = earlier
    moved = mm(change1.astype(bf16), jnp.concatenate([change0, offset0], axis=1).astype(bf16))
    return (
        keep1 * keep0,
        moved[:, :WIDTH] + (keep1 * change0 + keep0 * change1),
        moved[:, WIDTH:] + (keep1 * offset0 + offset1),
    )


def chain_maps(count, store, solved_ref, fresh_ref, vheads, result):
    _, _, _, write_ref, rows_ref = store
    maps = []
    for i in range(count):
        row = []
        for h in range(vheads):
            moved = mm(
                write_ref[i, h],
                jnp.concatenate(
                    [solved_ref[i, h], fresh_ref[i, h].astype(bf16)], axis=1
                ),
            )
            row.append((rows_ref[i, 8 + h : 9 + h, :], moved[:, :WIDTH], moved[:, WIDTH:]))
        maps.append(row)
        yield
    while len(maps) > 1:
        maps = [
            [join(later, earlier) for later, earlier in zip(maps[k + 1], maps[k])]
            for k in range(0, len(maps), 2)
        ]
        yield
    result.extend(maps[0])


def split_store(refs, base):
    return tuple(View(ref, base) for ref in refs)


def first_kernel(
    place_ref, k_ref, v_ref, kw_ref, vw_ref, gate_ref,
    key_ref, mixing_ref, value_ref, write_ref, rows_ref, solved_ref, fresh_ref, mask_ref,
):
    chunks = gate_ref.shape[0]
    count = chunks // 2
    fill_masks(mask_ref)
    whole = (key_ref, mixing_ref, value_ref, write_ref, rows_ref)
    late = split_store(whole, count)
    sources = ((k_ref, v_ref), (None, None), (kw_ref, vw_ref), gate_ref)
    together((prepare(range(count), count, *sources, late), 1))
    together(
        (
            invert(
                count, late, key_ref.shape[1], value_ref.shape[1], mask_ref,
                solved_ref, fresh_ref,
            ),
            1,
        ),
        (prepare(range(1, count), 0, *sources, whole), 2),
    )


def local_kernel(
    place_ref, k_ref, v_ref, kw_ref, vw_ref, rim_ref, gate_ref,
    later_key_ref, later_mixing_ref, later_value_ref, later_write_ref, later_rows_ref,
    late_solved_ref, late_fresh_ref, mask_ref,
    key_ref, write_ref, rows_ref, solved_ref, fresh_ref, near_ref, far_ref,
    mixing_ref, value_ref, k_pad, v_pad,
):
    core = place_ref[2]
    chunks = gate_ref.shape[0]
    count = chunks // 2
    qheads = kw_ref.shape[1]
    vheads = vw_ref.shape[1]
    fill_pad(k_pad, k_ref, qheads, rim_ref, RIM * qheads)
    fill_pad(v_pad, v_ref, vheads, rim_ref, 2 * RIM * qheads)
    opening = (key_ref, mixing_ref, value_ref, write_ref, rows_ref)
    rest = (later_key_ref, later_mixing_ref, later_value_ref, later_write_ref, later_rows_ref)
    early = tuple(Joined(head, tail) for head, tail in zip(opening, rest))
    late = split_store(rest, count)
    first_half, second_half = [], []
    together(
        (
            prepare(
                range(1), 0, (k_ref, v_ref), (k_pad, v_pad), (kw_ref, vw_ref), gate_ref, opening
            ),
            1,
        ),
        (
            chain_maps(
                count, late, late_solved_ref, late_fresh_ref, vheads, second_half
            ),
            1,
        ),
    )
    together(
        (invert(count, early, qheads, vheads, mask_ref, solved_ref, fresh_ref), 1),
    )
    together((chain_maps(count, early, solved_ref, fresh_ref, vheads, first_half), 1))
    half = vheads // 2
    row1, col1 = squares()
    for h in range(vheads):
        keep, change, offset = join(second_half[h], first_half[h])
        packed = jnp.concatenate(
            [change + jnp.where(row1 == col1, keep, 0.0), offset], axis=1
        ).astype(bf16)

        @pl.when(core == h // half)
        def _():
            near_ref[h % half] = packed

        @pl.when(core != h // half)
        def _():
            far_ref[h % half] = packed


class Joined:
    def __init__(self, head, tail):
        self.head, self.tail = head, tail

    def __getitem__(self, key):
        return self.head[key] if key[0] == 0 else self.tail[key]


def stay(value):
    return pltpu.with_memory_space_constraint(value, pltpu.HBM)


INSIDE = pl.BlockSpec(memory_space=pltpu.VMEM)
SCALAR = pl.BlockSpec(memory_space=pltpu.SMEM)
MIB = 1024 * 1024


def group_shapes(count, qheads, vheads):
    return (
        jax.ShapeDtypeStruct((count, qheads, CHUNK, WIDTH), bf16),
        jax.ShapeDtypeStruct((count, qheads, CHUNK, 2 * CHUNK), bf16),
        jax.ShapeDtypeStruct((count, vheads, CHUNK, WIDTH), bf16),
        jax.ShapeDtypeStruct((count, vheads, CHUNK, CHUNK), bf16),
        jax.ShapeDtypeStruct((count, 16, CHUNK), f32),
    )


def pad_scratch(heads):
    return pltpu.VMEM(((PAD + CHUNK) * heads, WIDTH), f32)


def first_call(place, key, value, key_conv, value_conv, gates, interpret=False):
    chunks = gates.shape[0]
    count = chunks // 2
    vheads = value_conv.shape[1]
    return pl.pallas_call(
        first_kernel,
        out_shape=group_shapes(chunks, key_conv.shape[1], vheads)
        + (
            jax.ShapeDtypeStruct((count, vheads, CHUNK, WIDTH), bf16),
            jax.ShapeDtypeStruct((count, vheads, CHUNK, WIDTH), f32),
            jax.ShapeDtypeStruct((5, CHUNK, 2 * CHUNK), bf16),
        ),
        in_specs=[SCALAR] + [INSIDE] * 5,
        out_specs=(INSIDE,) * 8,
        compiler_params=pltpu.CompilerParams(vmem_limit_bytes=16 * MIB),
        cost_estimate=pl.CostEstimate(flops=1 << 32, transcendentals=0, bytes_accessed=0),
        interpret=interpret,
        name="first_map",
    )(place, key.reshape(-1, WIDTH), value.reshape(-1, WIDTH), key_conv, value_conv, gates)


def local_call(place, key, value, key_conv, value_conv, rim, gates, later, interpret=False):
    chunks = gates.shape[0]
    count = chunks // 2
    qheads = key_conv.shape[1]
    vheads = value_conv.shape[1]
    shapes = group_shapes(1, qheads, vheads)
    pair = jax.ShapeDtypeStruct((vheads // 2, WIDTH, 2 * WIDTH), bf16)
    return pl.pallas_call(
        local_kernel,
        out_shape=(
            shapes[0],
            shapes[3],
            shapes[4],
            jax.ShapeDtypeStruct((count, vheads, CHUNK, WIDTH), bf16),
            jax.ShapeDtypeStruct((count, vheads, CHUNK, WIDTH), f32),
            pair,
            pair,
        ),
        in_specs=[SCALAR] + [INSIDE] * 14,
        out_specs=(INSIDE,) * 7,
        scratch_shapes=[
            pltpu.VMEM(shapes[1].shape, bf16),
            pltpu.VMEM(shapes[2].shape, bf16),
            pad_scratch(qheads),
            pad_scratch(vheads),
        ],
        compiler_params=pltpu.CompilerParams(vmem_limit_bytes=20 * MIB),
        interpret=interpret,
        name="local_map",
    )(
        place, key.reshape(-1, WIDTH), value.reshape(-1, WIDTH), key_conv, value_conv, rim,
        gates, *later,
    )


def read_chunk(chunk, i, rows, start, qw_ref, gate_ref, key_ref, pair_ref, low_ref, wide_ref):
    qheads = qw_ref.shape[1]
    ratio = pair_ref.shape[1] // qheads
    row1, col1 = squares()
    running = running_sums(gate_ref[chunk], (row1 <= col1).astype(bf16))
    columns = running.T
    target = pl.ds(pl.multiple_of(chunk * CHUNK, CHUNK), CHUNK)
    for g in range(qheads):
        query = unit(mix(rows, qw_ref, qheads, g, start)) * (WIDTH ** -0.5)
        qk = lax.dot_general(
            query.astype(bf16), key_ref[i, g], (((1,), (1,)), ((), ())),
            preferred_element_type=f32,
        )
        for side in range(ratio):
            head = g * ratio + side
            decay_col = spread(columns, head)
            table = jnp.where(
                row1 >= col1, jnp.exp2(decay_col - running[head : head + 1, :]), 0.0
            )
            lift = jnp.exp2(decay_col)
            reading = jnp.concatenate(
                [(lift * query).astype(bf16), (qk * table).astype(bf16)], axis=1
            )
            result = mm(reading, pair_ref[chunk, head])
            wide_ref[head, target, :] = result[:, :WIDTH].astype(bf16)
            low_ref[head, target, :] = result[:, WIDTH:]


def chain_kernel(
    solved_ref, fresh_ref, late_solved_ref, late_fresh_ref,
    write_ref, rows_ref, later_write_ref, later_rows_ref,
    q_ref, qw_ref, rim_ref, gate_ref, key_ref, later_key_ref, after_ref,
    pair_ref, low_ref, wide_ref, mark_ref, hold_ref, q_pad,
):
    count, vheads = solved_ref.shape[:2]
    mark_ref[...] = jnp.zeros_like(mark_ref)
    fill_pad(q_pad, q_ref, qw_ref.shape[1], rim_ref, 0)
    row1, col1 = squares()
    for h in range(vheads):
        hold_ref[h] = jnp.concatenate(
            [(row1 == col1).astype(f32), jnp.zeros((CHUNK, CHUNK), f32)], axis=1
        )

    def advance(chunk, i, solved, fresh, writes, ends):
        states = [hold_ref[h] for h in range(vheads)]
        packed = [s.astype(bf16) for s in states]
        taken = [mm(solved[i, h], packed[h]) for h in range(vheads)]
        updates = [
            jnp.concatenate(
                [taken[h][:, :WIDTH], fresh[i, h] + taken[h][:, WIDTH:]], axis=1
            ).astype(bf16)
            for h in range(vheads)
        ]
        for h in range(vheads):
            pair_ref[chunk, h, :CHUNK, :] = packed[h]
            pair_ref[chunk, h, CHUNK:, :] = updates[h]
            end = ends[chunk, 8 + h : 9 + h, :]
            hold_ref[h] = states[h] * jnp.concatenate([end, end], axis=1) + mm(
                writes[chunk, h], updates[h]
            )

    def read(chunk, keys):
        rows, start = rows_of(q_ref, q_pad, chunk)
        read_chunk(
            chunk, chunk, rows, start, qw_ref, gate_ref, keys, pair_ref, low_ref, wide_ref
        )

    def early_step(i, carry):
        advance(i, i, solved_ref, fresh_ref, later_write_ref, later_rows_ref)
        read(i, later_key_ref)
        return carry

    def late_step(i, carry):
        advance(
            count + i, i, late_solved_ref, late_fresh_ref, later_write_ref, later_rows_ref
        )
        return carry

    advance(0, 0, solved_ref, fresh_ref, write_ref, rows_ref)
    read(0, key_ref)
    lax.fori_loop(1, count, early_step, 0)
    lax.fori_loop(0, count, late_step, 0)


def chain_call(
    solved, fresh, write, rows, later, query, query_conv, rim, gates, keys, after, interpret=False
):
    later_keys, _, _, later_write, later_rows, late_solved, late_fresh, _ = later
    chunks, vheads = later_write.shape[:2]
    tokens = chunks * CHUNK
    return pl.pallas_call(
        chain_kernel,
        out_shape=(
            jax.ShapeDtypeStruct((chunks, vheads, 2 * CHUNK, 2 * WIDTH), bf16),
            jax.ShapeDtypeStruct((vheads, tokens, WIDTH), f32),
            jax.ShapeDtypeStruct((vheads, tokens, WIDTH), bf16),
            jax.ShapeDtypeStruct((8, WIDTH), f32),
        ),
        in_specs=[INSIDE] * 14 + [pl.BlockSpec(memory_space=pl.ANY)],
        out_specs=(INSIDE,) * 4,
        scratch_shapes=[
            pltpu.VMEM((vheads, WIDTH, 2 * WIDTH), f32), pad_scratch(query_conv.shape[1])
        ],
        compiler_params=pltpu.CompilerParams(vmem_limit_bytes=20 * MIB),
        cost_estimate=pl.CostEstimate(flops=1 << 32, transcendentals=0, bytes_accessed=0),
        interpret=interpret,
        name="chain",
    )(
        solved, fresh, late_solved, late_fresh, write, rows, later_write, later_rows,
        query.reshape(-1, WIDTH), query_conv, rim, gates, keys, later_keys, after,
    )


def read_kernel(
    q_ref, qw_ref, gate_ref, late_key_ref, pair_ref, old_low_ref, old_wide_ref, after_ref,
    low_ref, wide_ref, mark_ref,
):
    mark_ref[...] = jnp.zeros_like(mark_ref)
    chunks = gate_ref.shape[0]
    count = chunks // 2
    done = (chunks - count) * CHUNK
    low_ref[:, :done, :] = old_low_ref[:, :done, :]
    wide_ref[:, :done, :] = old_wide_ref[:, :done, :]

    def some(step, carry):
        for inner in range(READ):
            i = step * READ + inner
            chunk = chunks - count + i
            read_chunk(
                chunk, chunk, q_ref, chunk * CHUNK - PAD, qw_ref, gate_ref, late_key_ref, pair_ref,
                low_ref, wide_ref,
            )
        return carry

    lax.fori_loop(0, count // READ, some, 0)


def read_call(query, query_conv, gates, late_keys, pairs, low, wide, after, interpret=False):
    return pl.pallas_call(
        read_kernel,
        out_shape=(
            jax.ShapeDtypeStruct(low.shape, f32),
            jax.ShapeDtypeStruct(wide.shape, bf16),
            jax.ShapeDtypeStruct((8, WIDTH), f32),
        ),
        in_specs=[INSIDE] * 7 + [pl.BlockSpec(memory_space=pl.ANY)],
        out_specs=(INSIDE,) * 3,
        compiler_params=pltpu.CompilerParams(vmem_limit_bytes=20 * MIB),
        cost_estimate=pl.CostEstimate(flops=1 << 32, transcendentals=0, bytes_accessed=0),
        interpret=interpret,
        name="read_out",
    )(query.reshape(-1, WIDTH), query_conv, gates, late_keys, pairs, low, wide, after)


def rim_kernel(q_hbm, k_hbm, v_hbm, rim_ref, sems):
    first = 0
    copies = []
    for i, (source, heads) in enumerate(((q_hbm, 2), (k_hbm, 2), (v_hbm, 4))):
        rows = RIM * heads
        copies.append(
            pltpu.make_async_copy(
                source.at[pl.ds(source.shape[0] - rows, rows), :],
                rim_ref.at[pl.ds(first, rows), :],
                sems.at[i],
            )
        )
        first += rows
    for copy in copies:
        copy.start()
    for copy in copies:
        copy.wait()


def rim_call(query, key, value):
    flat = [stay(x.reshape(-1, WIDTH)) for x in (query, key, value)]
    rows = RIM * (query.shape[1] + key.shape[1] + value.shape[1])
    return pl.pallas_call(
        rim_kernel,
        out_shape=jax.ShapeDtypeStruct((rows, WIDTH), f32),
        in_specs=[pl.BlockSpec(memory_space=pltpu.HBM)] * 3,
        out_specs=pl.BlockSpec(memory_space=pltpu.VMEM),
        scratch_shapes=[pltpu.SemaphoreType.DMA((3,))],
        compiler_params=pltpu.CompilerParams(vmem_limit_bytes=1024 * 1024),
        name="rim",
    )(*flat)


def total_kernel(place_ref, mine_ref, other_ref, total_ref, first_ref):
    core = place_ref[2]
    for h in range(mine_ref.shape[0]):
        mine, other = mine_ref[h], other_ref[h]
        first = jnp.where(core == 0, mine, other)
        second = jnp.where(core == 0, other, mine)
        joined = mm(second[:, :WIDTH], first)
        total_ref[h] = jnp.concatenate(
            [joined[:, :WIDTH], joined[:, WIDTH:] + second[:, WIDTH:].astype(f32)], axis=1
        ).astype(bf16)
        first_ref[h] = first


def row_kernel(place_ref, a_ref, b_ref, c_ref, d_ref, mark_ref, total_ref, before_ref, all_ref, sum_ref):
    here = place_ref[1]
    heads = a_ref.shape[0]
    for k, ref in enumerate((a_ref, b_ref, c_ref, d_ref)):
        all_ref[(here + 4 - k) % 4] = ref[...]
    eye = lax.broadcasted_iota(jnp.int32, (WIDTH, 2 * WIDTH), 0) == lax.broadcasted_iota(
        jnp.int32, (WIDTH, 2 * WIDTH), 1
    )
    for h in range(heads):
        sum_ref[0, h] = eye.astype(f32).astype(bf16)
        sum_ref[1, h] = all_ref[0, h]
    for j in range(1, 4):
        for h in range(heads):
            joined = mm(all_ref[j, h, :, :WIDTH], sum_ref[j, h])
            value = jnp.concatenate(
                [joined[:, :WIDTH], joined[:, WIDTH:] + all_ref[j, h, :, WIDTH:].astype(f32)],
                axis=1,
            ).astype(bf16)
            if j < 3:
                sum_ref[j + 1, h] = value
            else:
                total_ref[h] = value
    before_ref[...] = sum_ref[here]


def prefix_kernel(
    place_ref, b_ref, c_ref, d_ref, before_ref, first_ref, mark_ref,
    mine_ref, send_ref, all_ref, sum_ref,
):
    here = place_ref[0]
    core = place_ref[2]
    heads = b_ref.shape[0]
    for k, ref in enumerate((b_ref, c_ref, d_ref)):
        all_ref[(here + 3 - k) % 4] = ref[...]
    for h in range(heads):
        sum_ref[0, h] = jnp.zeros((WIDTH, WIDTH), bf16)
        sum_ref[1, h] = all_ref[0, h, :, WIDTH:]
    for j in range(1, 3):
        for h in range(heads):
            moved = mm(all_ref[j, h, :, :WIDTH], sum_ref[j, h])
            sum_ref[j + 1, h] = (moved + all_ref[j, h, :, WIDTH:].astype(f32)).astype(bf16)
    for h in range(heads):
        row = sum_ref[here, h]
        before = (
            mm(before_ref[h, :, :WIDTH], row) + before_ref[h, :, WIDTH:].astype(f32)
        ).astype(bf16)
        after = mm(first_ref[h, :, :WIDTH], before) + first_ref[h, :, WIDTH:].astype(f32)
        wide = before.astype(f32)
        mine_ref[h] = jnp.where(core == 0, wide, after).astype(bf16)
        send_ref[h] = jnp.where(core == 0, after, wide).astype(bf16)


def small_call(kernel, outs, scratch, name, place, *arrays):
    inside = pl.BlockSpec(memory_space=pltpu.VMEM)
    return pl.pallas_call(
        kernel,
        out_shape=tuple(jax.ShapeDtypeStruct(shape, bf16) for shape in outs),
        in_specs=[pl.BlockSpec(memory_space=pltpu.SMEM)] + [inside] * len(arrays),
        out_specs=(inside,) * len(outs),
        scratch_shapes=[pltpu.VMEM(shape, bf16) for shape in scratch],
        compiler_params=pltpu.CompilerParams(vmem_limit_bytes=8 * 1024 * 1024),
        name=name,
    )(place, *arrays)


def output_kernel(
    place_ref, low_ref, wide_ref, near_ref, far_ref, gate_ref, gain_ref, weight_ref,
    *out_refs, slots
):
    core = place_ref[2]
    heads = low_ref.shape[0]
    half = heads // 2
    rows = out_refs[0].shape[0]
    for index, slot in enumerate(slots):
        start = pl.multiple_of(place_ref[3 + slot] * rows, rows)
        pieces = []
        for h in range(heads):
            entering = jnp.where(core == h // half, near_ref[h % half], far_ref[h % half])
            recurrent = low_ref[h, pl.ds(start, rows), :] + mm(
                wide_ref[h, pl.ds(start, rows), :], entering
            )
            scaled = recurrent * lax.rsqrt(
                jnp.mean(recurrent * recurrent, axis=1, keepdims=True) + norm_epsilon
            )
            gate = gate_ref[pl.ds(start * heads + h, rows, stride=heads), :]
            pieces.append((scaled * gain_ref[...] * silu(gate)).astype(bf16))
        normed = jnp.concatenate(pieces, axis=1)
        side = out_refs[0].shape[1]
        for k in range(2):
            out_refs[2 * index + k][...] = mm(
                normed, weight_ref[:, k * side : (k + 1) * side]
            ).astype(bf16)


def output_call(place, slots, low, wide, near, far, gate_in, norm_gain, out_weight):
    heads, tokens, _ = low.shape
    model = out_weight.shape[1]
    rows = tokens // 8
    inside = pl.BlockSpec(memory_space=pltpu.VMEM)
    piece = jax.ShapeDtypeStruct((rows, model // 2), bf16)
    return pl.pallas_call(
        functools.partial(output_kernel, slots=slots),
        out_shape=(piece,) * (2 * len(slots)),
        in_specs=[pl.BlockSpec(memory_space=pltpu.SMEM)] + [inside] * 7,
        out_specs=(inside,) * (2 * len(slots)),
        compiler_params=pltpu.CompilerParams(vmem_limit_bytes=16 * 1024 * 1024),
        cost_estimate=pl.CostEstimate(
            flops=2 * rows * heads * WIDTH * model * len(slots), transcendentals=0, bytes_accessed=0
        ),
        name="gated_output",
    )(
        place, low, wide, near, far,
        gate_in.reshape(tokens * heads, WIDTH), norm_gain.reshape(1, WIDTH), out_weight,
    )


def add_kernel(left_ref, right_ref, out_ref):
    out_ref[...] = (left_ref[...].astype(f32) + right_ref[...].astype(f32)).astype(bf16)


def add(left, right):
    inside = pl.BlockSpec(memory_space=pltpu.VMEM)
    return pl.pallas_call(
        add_kernel,
        out_shape=jax.ShapeDtypeStruct(left.shape, bf16),
        in_specs=[inside] * 2,
        out_specs=inside,
        compiler_params=pltpu.CompilerParams(vmem_limit_bytes=2 * 1024 * 1024),
        name="add",
    )(left, right)


def last_kernel(*refs):
    out_ref = refs[-1]
    side = refs[0].shape[1]
    for k in range(2):
        total = refs[k][...].astype(f32)
        for other in (refs[2 + k], refs[4 + k]):
            total = total + other[...].astype(f32)
        out_ref[:, k * side : (k + 1) * side] = total


def last_call(*arrays):
    rows, side = arrays[0].shape
    inside = pl.BlockSpec(memory_space=pltpu.VMEM)
    return pl.pallas_call(
        last_kernel,
        out_shape=jax.ShapeDtypeStruct((rows, 2 * side), f32),
        in_specs=[inside] * 6,
        out_specs=inside,
        compiler_params=pltpu.CompilerParams(vmem_limit_bytes=8 * 1024 * 1024),
        name="last_add",
    )(*arrays)


def shifted(value, axis, steps, around=True):
    count = lax.axis_size(axis)
    pairs = [(i, (i + steps) % count) for i in range(count) if around or 0 <= i + steps < count]
    return lax.ppermute(value, axis, pairs)


def head_sum(parts):
    def right(value):
        return shifted(value, "head", 1)

    def left(value):
        return shifted(value, "head", -1)

    far, up_parts, down_parts, own = parts[0], parts[1:7:2], parts[2:7:2], parts[7]
    up = [right(far[0]), right(up_parts[0][1])]
    down = [left(down_parts[0][0]), left(far[1])]
    up = [right(add(up_parts[0][0], up[0])), up[1]]
    down = [down[0], left(add(down_parts[0][1], down[1]))]
    for step in (1, 2):
        for side in (1, 0):
            up[side] = right(add(up_parts[step][side], up[side]))
            down[1 - side] = left(add(down_parts[step][1 - side], down[1 - side]))
    return last_call(*own, *up, *down)


def on_device(
    query_in, key_in, value_in, gate_in, log_gate, strength,
    query_conv, key_conv, value_conv, norm_gain, out_weight,
):
    z = lax.axis_index("head")
    order = [(z + shift) & 7 for shift in (4, 3, 5, 2, 6, 1, 7, 0)]
    place = jnp.stack(
        [lax.axis_index("ctx_0"), lax.axis_index("ctx_1"), lax.axis_index("ctx_2")] + order
    ).astype(jnp.int32)
    rim = shifted(rim_call(query_in, key_in, value_in), CTX, 1, around=False)
    vheads, tokens = log_gate.shape
    gates = jnp.concatenate(
        [
            log_gate.reshape(vheads, tokens // CHUNK, CHUNK),
            strength.reshape(vheads, tokens // CHUNK, CHUNK),
        ],
        axis=0,
    ).transpose(1, 0, 2)
    later = first_call(place, key_in, value_in, key_conv, value_conv, gates)
    keys, write, ends, solved, fresh, mine, other = local_call(
        place, key_in, value_in, key_conv, value_conv, rim, gates, later
    )
    other = shifted(other, "ctx_2", 1)
    half = vheads // 2
    maps = (half, WIDTH, 2 * WIDTH)
    states = (half, WIDTH, WIDTH)
    total, first = small_call(total_kernel, (maps, maps), (), "chip_total", place, mine, other)
    pairs, low, wide, mark = chain_call(
        solved, fresh, write, ends, later, query_in, query_conv, rim, gates, keys, first
    )
    row = [shifted(total, "ctx_1", k) for k in range(1, 4)]
    row_total, before = small_call(
        row_kernel, (maps, maps), ((4,) + maps, (4,) + maps), "row_total", place, total, *row, mark
    )
    rows = [shifted(row_total, "ctx_0", k, around=False) for k in range(1, 4)]
    low, wide, mark = read_call(
        query_in, query_conv, gates, later[0], pairs, low, wide, before
    )
    near, send = small_call(
        prefix_kernel, (states, states), ((4,) + maps, (4,) + states), "prefix",
        place, *rows, before, first, mark,
    )
    far = shifted(send, "ctx_2", 1)
    tail = (low, wide, near, far, gate_in, norm_gain, out_weight)
    parts = []
    for slots in ((0,), (1, 2), (3, 4), (5, 6, 7)):
        pieces = output_call(place, slots, *tail)
        parts += [pieces[2 * i : 2 * i + 2] for i in range(len(slots))]
    return head_sum(parts)


def solution(mesh):
    split = Mesh(
        mesh.devices.reshape(4, 4, 2, mesh.shape["head"]), ("ctx_0", "ctx_1", "ctx_2", "head")
    )
    in_specs = (
        P(CTX, "head", None),
        P(CTX, "head", None),
        P(CTX, "head", None),
        P(CTX, "head", None),
        P("head", CTX),
        P("head", CTX),
        P(None, "head", None),
        P(None, "head", None),
        P(None, "head", None),
        P(),
        P("head", None),
    )
    return jax.shard_map(
        on_device, mesh=split, in_specs=in_specs, out_specs=P(CTX_HEAD, None), check_vma=False
    )
```

```python
import functools
import jax
import jax.numpy as jnp
from jax import lax
from jax.experimental import pallas as pl
from jax.experimental.pallas import tpu as pltpu
from jax.sharding import Mesh
from jax.sharding import PartitionSpec as P

CTX = ("ctx_0", "ctx_1", "ctx_2")
CTX_HEAD = ("ctx_0", "ctx_1", "ctx_2", "head")
CHUNK = 128
WIDTH = 128
PAD = 8
RIM = 4
READ = 2
norm_epsilon = 1e-06
LOG2E = 1.4426950408889634
f32 = jnp.float32
bf16 = jnp.bfloat16


def mm(left, right):
    return jnp.dot(left, right, preferred_element_type=f32)


def silu_of_half(half):
    return half + half * jnp.tanh(half)


def silu(u):
    return silu_of_half(0.5 * u)


def paired(x):
    zero = jnp.zeros((CHUNK, CHUNK), x.dtype)
    top = jnp.concatenate([x[:, :CHUNK], zero], axis=1)
    low = jnp.concatenate([zero, x[:, CHUNK:]], axis=1)
    return jnp.concatenate([top, low], axis=0)


def mix(target, weight_ref, heads, head, start):
    total = None
    for tap in range(4):
        piece = target[pl.ds((start + PAD - 3 + tap) * heads + head, CHUNK, stride=heads), :]
        part = (0.5 * weight_ref[tap, head : head + 1, :]) * piece
        total = part if total is None else total + part
    return silu_of_half(total)


def unit(x):
    return x * lax.rsqrt(jnp.sum(x * x, axis=1, keepdims=True) + norm_epsilon)


def squares():
    row = lax.broadcasted_iota(jnp.int32, (CHUNK, CHUNK), 0)
    col = lax.broadcasted_iota(jnp.int32, (CHUNK, CHUNK), 1)
    return row, col


def running_sums(gates, adder):
    hi = gates.astype(bf16).astype(f32)
    rest = gates - hi
    mid = rest.astype(bf16).astype(f32)
    parts = jnp.concatenate([hi, mid, rest - mid], axis=0).astype(bf16)
    sums = mm(parts, adder)
    return (sums[0:8] + sums[8:16] + sums[16:24]) * LOG2E


def spread(columns, index):
    return jnp.broadcast_to(columns[:, index : index + 1], (CHUNK, CHUNK))


def fill_pad(pad, source, heads, rim_ref, first):
    pad[pl.ds((PAD - RIM) * heads, RIM * heads), :] = rim_ref[first : first + RIM * heads, :]
    pad[pl.ds(PAD * heads, CHUNK * heads), :] = source[pl.ds(0, CHUNK * heads), :]


def rows_of(source, pad, chunk):
    if isinstance(chunk, int) and chunk == 0:
        return pad, 0
    return source, chunk * CHUNK - PAD


def together(*steps):
    live = list(steps)
    while live:
        still = []
        for step, weight in live:
            alive = True
            for _ in range(weight):
                if next(step, "end") == "end":
                    alive = False
                    break
            if alive:
                still.append((step, weight))
        live = still


def fill_masks(mask_ref):
    row = lax.broadcasted_iota(jnp.int32, (CHUNK, 2 * CHUNK), 0)
    col = lax.broadcasted_iota(jnp.int32, (CHUNK, 2 * CHUNK), 1) & (CHUNK - 1)

    def same(bits):
        return (row >> bits) == (col >> bits)

    mask_ref[0] = same(4).astype(bf16)
    for level in range(3):
        mask_ref[1 + level] = (same(5 + level) & jnp.logical_not(same(4 + level))).astype(bf16)
    mask_ref[4] = (row == col).astype(bf16)


class View:
    def __init__(self, ref, base):
        self.ref, self.base = ref, base

    def __getitem__(self, key):
        return self.ref[(key[0] + self.base,) + key[1:]]

    def __setitem__(self, key, value):
        self.ref[(key[0] + self.base,) + key[1:]] = value


def prepare(group, first, sources, pads, weights, gate_ref, store):
    kw_ref, vw_ref = weights
    key_ref, mixing_ref, value_ref, write_ref, rows_ref = store
    qheads = kw_ref.shape[1]
    vheads = vw_ref.shape[1]
    ratio = vheads // qheads
    row1, col1 = squares()
    strict = row1 > col1
    adder = (row1 <= col1).astype(bf16)
    for i in group:
        (k_rows, start), (v_rows, _) = [
            rows_of(source, pad, first + i) for source, pad in zip(sources, pads)
        ]
        gates = gate_ref[first + i]
        running = running_sums(gates, adder)
        strengths = gates[4:8]
        scaled = running[0:4] + jnp.log2(strengths)
        columns = jnp.concatenate([scaled, scaled], axis=0).T
        end_row = running[:, CHUNK - 1 : CHUNK]
        tail_row = jnp.exp2(end_row - running)
        rows_ref[i, 0:4, :] = -jnp.exp2(scaled)
        rows_ref[i, 4:8, :] = strengths
        rows_ref[i, 8:16, :] = jnp.broadcast_to(jnp.exp2(end_row), (8, CHUNK))
        for g in range(qheads):
            key = unit(mix(k_rows, kw_ref, qheads, g, start))
            key_t = key.T
            packed = key.astype(bf16)
            key_ref[i, g] = packed
            kk = mm(packed, key_t.astype(bf16))
            yield
            for side in range(ratio):
                head = g * ratio + side
                table = jnp.where(
                    strict, jnp.exp2(spread(columns, head) - running[head : head + 1, :]), 0.0
                )
                lanes = slice(side * CHUNK, (side + 1) * CHUNK)
                mixing_ref[i, g, :, lanes] = (kk * table).astype(bf16)
                write_ref[i, head] = (key_t * tail_row[head : head + 1, :]).astype(bf16)
                value_ref[i, head] = mix(v_rows, vw_ref, vheads, head, start).astype(bf16)
                yield


def invert(count, store, qheads, vheads, mask_ref, solved_ref, fresh_ref):
    key_ref, mixing_ref, value_ref, write_ref, rows_ref = store
    ratio = vheads // qheads
    units = [(i, g) for i in range(count) for g in range(qheads)]

    def mixing(level):
        return [mixing_ref[i, g] * mask_ref[level] for i, g in units]

    eye = mask_ref[4]
    powers = mixing(0)
    inverses = [eye - p for p in powers]
    powers = [mm(p, paired(p)).astype(bf16) for p in powers]
    yield
    for step in range(3):
        inverses = [mm(eye + p, paired(x)).astype(bf16) for p, x in zip(powers, inverses)]
        yield
        if step < 2:
            powers = [mm(p, paired(p)).astype(bf16) for p in powers]
            yield
    for level in range(3):
        crossed = [
            eye - mm(m, paired(x)).astype(bf16) for m, x in zip(mixing(1 + level), inverses)
        ]
        yield
        inverses = [mm(x, paired(y)) for x, y in zip(inverses, crossed)]
        if level < 2:
            inverses = [x.astype(bf16) for x in inverses]
        yield
    for (i, g), inverse in zip(units, inverses):
        for side in range(ratio):
            head = g * ratio + side
            own = inverse[:, side * CHUNK : (side + 1) * CHUNK]
            left = jnp.concatenate(
                [own * rows_ref[i, head : head + 1, :], own * rows_ref[i, 4 + head : 5 + head, :]],
                axis=1,
            ).astype(bf16)
            right = jnp.concatenate([key_ref[i, g], value_ref[i, head]], axis=1)
            answer = mm(left, paired(right))
            solved_ref[i, head] = answer[:, :CHUNK].astype(bf16)
            fresh_ref[i, head] = answer[:, CHUNK:]
        yield


def join(later, earlier):
    keep1, change1, offset1 = later
    keep0, change0, offset0 = earlier
    moved = mm(change1.astype(bf16), jnp.concatenate([change0, offset0], axis=1).astype(bf16))
    return (
        keep1 * keep0,
        moved[:, :WIDTH] + (keep1 * change0 + keep0 * change1),
        moved[:, WIDTH:] + (keep1 * offset0 + offset1),
    )


def chain_maps(count, store, solved_ref, fresh_ref, vheads, result):
    _, _, _, write_ref, rows_ref = store
    maps = []
    for i in range(count):
        row = []
        for h in range(vheads):
            moved = mm(
                write_ref[i, h],
                jnp.concatenate(
                    [solved_ref[i, h], fresh_ref[i, h].astype(bf16)], axis=1
                ),
            )
            row.append((rows_ref[i, 8 + h : 9 + h, :], moved[:, :WIDTH], moved[:, WIDTH:]))
        maps.append(row)
        yield
    while len(maps) > 1:
        maps = [
            [join(later, earlier) for later, earlier in zip(maps[k + 1], maps[k])]
            for k in range(0, len(maps), 2)
        ]
        yield
    result.extend(maps[0])


def split_store(refs, base):
    return tuple(View(ref, base) for ref in refs)


def first_kernel(
    place_ref, k_ref, v_ref, kw_ref, vw_ref, gate_ref,
    key_ref, mixing_ref, value_ref, write_ref, rows_ref, solved_ref, fresh_ref, mask_ref,
):
    chunks = gate_ref.shape[0]
    count = chunks // 2
    fill_masks(mask_ref)
    whole = (key_ref, mixing_ref, value_ref, write_ref, rows_ref)
    late = split_store(whole, count)
    sources = ((k_ref, v_ref), (None, None), (kw_ref, vw_ref), gate_ref)
    together(
        *[(prepare(range(i, i + 1), count, *sources, late), 1) for i in range(count)]
    )
    together(
        (
            invert(
                count, late, key_ref.shape[1], value_ref.shape[1], mask_ref,
                solved_ref, fresh_ref,
            ),
            1,
        ),
        (prepare(range(1, count), 0, *sources, whole), 2),
    )


def local_kernel(
    place_ref, k_ref, v_ref, kw_ref, vw_ref, rim_ref, gate_ref,
    later_key_ref, later_mixing_ref, later_value_ref, later_write_ref, later_rows_ref,
    late_solved_ref, late_fresh_ref, mask_ref,
    key_ref, write_ref, rows_ref, solved_ref, fresh_ref, near_ref, far_ref,
    mixing_ref, value_ref, k_pad, v_pad,
):
    core = place_ref[2]
    chunks = gate_ref.shape[0]
    count = chunks // 2
    qheads = kw_ref.shape[1]
    vheads = vw_ref.shape[1]
    fill_pad(k_pad, k_ref, qheads, rim_ref, RIM * qheads)
    fill_pad(v_pad, v_ref, vheads, rim_ref, 2 * RIM * qheads)
    opening = (key_ref, mixing_ref, value_ref, write_ref, rows_ref)
    rest = (later_key_ref, later_mixing_ref, later_value_ref, later_write_ref, later_rows_ref)
    early = tuple(Joined(head, tail) for head, tail in zip(opening, rest))
    late = split_store(rest, count)
    first_half, second_half = [], []
    together(
        (
            prepare(
                range(1), 0, (k_ref, v_ref), (k_pad, v_pad), (kw_ref, vw_ref), gate_ref, opening
            ),
            1,
        ),
        (
            chain_maps(
                count, late, late_solved_ref, late_fresh_ref, vheads, second_half
            ),
            1,
        ),
    )
    together(
        (invert(count, early, qheads, vheads, mask_ref, solved_ref, fresh_ref), 1),
    )
    together((chain_maps(count, early, solved_ref, fresh_ref, vheads, first_half), 1))
    half = vheads // 2
    row1, col1 = squares()
    for h in range(vheads):
        keep, change, offset = join(second_half[h], first_half[h])
        packed = jnp.concatenate(
            [change + jnp.where(row1 == col1, keep, 0.0), offset], axis=1
        ).astype(bf16)

        @pl.when(core == h // half)
        def _():
            near_ref[h % half] = packed

        @pl.when(core != h // half)
        def _():
            far_ref[h % half] = packed


class Joined:
    def __init__(self, head, tail):
        self.head, self.tail = head, tail

    def __getitem__(self, key):
        return self.head[key] if key[0] == 0 else self.tail[key]


def stay(value):
    return pltpu.with_memory_space_constraint(value, pltpu.HBM)


INSIDE = pl.BlockSpec(memory_space=pltpu.VMEM)
SCALAR = pl.BlockSpec(memory_space=pltpu.SMEM)
MIB = 1024 * 1024


def group_shapes(count, qheads, vheads):
    return (
        jax.ShapeDtypeStruct((count, qheads, CHUNK, WIDTH), bf16),
        jax.ShapeDtypeStruct((count, qheads, CHUNK, 2 * CHUNK), bf16),
        jax.ShapeDtypeStruct((count, vheads, CHUNK, WIDTH), bf16),
        jax.ShapeDtypeStruct((count, vheads, CHUNK, CHUNK), bf16),
        jax.ShapeDtypeStruct((count, 16, CHUNK), f32),
    )


def pad_scratch(heads):
    return pltpu.VMEM(((PAD + CHUNK) * heads, WIDTH), f32)


def first_call(place, key, value, key_conv, value_conv, gates, interpret=False):
    chunks = gates.shape[0]
    count = chunks // 2
    vheads = value_conv.shape[1]
    return pl.pallas_call(
        first_kernel,
        out_shape=group_shapes(chunks, key_conv.shape[1], vheads)
        + (
            jax.ShapeDtypeStruct((count, vheads, CHUNK, WIDTH), bf16),
            jax.ShapeDtypeStruct((count, vheads, CHUNK, WIDTH), f32),
            jax.ShapeDtypeStruct((5, CHUNK, 2 * CHUNK), bf16),
        ),
        in_specs=[SCALAR] + [INSIDE] * 5,
        out_specs=(INSIDE,) * 8,
        compiler_params=pltpu.CompilerParams(vmem_limit_bytes=16 * MIB),
        cost_estimate=pl.CostEstimate(flops=1 << 32, transcendentals=0, bytes_accessed=0),
        interpret=interpret,
        name="first_map",
    )(place, key.reshape(-1, WIDTH), value.reshape(-1, WIDTH), key_conv, value_conv, gates)


def local_call(place, key, value, key_conv, value_conv, rim, gates, later, interpret=False):
    chunks = gates.shape[0]
    count = chunks // 2
    qheads = key_conv.shape[1]
    vheads = value_conv.shape[1]
    shapes = group_shapes(1, qheads, vheads)
    pair = jax.ShapeDtypeStruct((vheads // 2, WIDTH, 2 * WIDTH), bf16)
    return pl.pallas_call(
        local_kernel,
        out_shape=(
            shapes[0],
            shapes[3],
            shapes[4],
            jax.ShapeDtypeStruct((count, vheads, CHUNK, WIDTH), bf16),
            jax.ShapeDtypeStruct((count, vheads, CHUNK, WIDTH), f32),
            pair,
            pair,
        ),
        in_specs=[SCALAR] + [INSIDE] * 14,
        out_specs=(INSIDE,) * 7,
        scratch_shapes=[
            pltpu.VMEM(shapes[1].shape, bf16),
            pltpu.VMEM(shapes[2].shape, bf16),
            pad_scratch(qheads),
            pad_scratch(vheads),
        ],
        compiler_params=pltpu.CompilerParams(vmem_limit_bytes=20 * MIB),
        interpret=interpret,
        name="local_map",
    )(
        place, key.reshape(-1, WIDTH), value.reshape(-1, WIDTH), key_conv, value_conv, rim,
        gates, *later,
    )


def read_chunk(chunk, i, rows, start, qw_ref, gate_ref, key_ref, pair_ref, low_ref, wide_ref):
    qheads = qw_ref.shape[1]
    ratio = pair_ref.shape[1] // qheads
    row1, col1 = squares()
    running = running_sums(gate_ref[chunk], (row1 <= col1).astype(bf16))
    columns = running.T
    target = pl.ds(pl.multiple_of(chunk * CHUNK, CHUNK), CHUNK)
    for g in range(qheads):
        query = unit(mix(rows, qw_ref, qheads, g, start)) * (WIDTH ** -0.5)
        qk = lax.dot_general(
            query.astype(bf16), key_ref[i, g], (((1,), (1,)), ((), ())),
            preferred_element_type=f32,
        )
        for side in range(ratio):
            head = g * ratio + side
            decay_col = spread(columns, head)
            table = jnp.where(
                row1 >= col1, jnp.exp2(decay_col - running[head : head + 1, :]), 0.0
            )
            lift = jnp.exp2(decay_col)
            reading = jnp.concatenate(
                [(lift * query).astype(bf16), (qk * table).astype(bf16)], axis=1
            )
            result = mm(reading, pair_ref[chunk, head])
            wide_ref[head, target, :] = result[:, :WIDTH].astype(bf16)
            low_ref[head, target, :] = result[:, WIDTH:]


def chain_kernel(
    solved_ref, fresh_ref, late_solved_ref, late_fresh_ref,
    write_ref, rows_ref, later_write_ref, later_rows_ref,
    q_ref, qw_ref, rim_ref, gate_ref, key_ref, later_key_ref, after_ref,
    pair_ref, low_ref, wide_ref, mark_ref, hold_ref, q_pad,
):
    count, vheads = solved_ref.shape[:2]
    mark_ref[...] = jnp.zeros_like(mark_ref)
    fill_pad(q_pad, q_ref, qw_ref.shape[1], rim_ref, 0)
    row1, col1 = squares()
    for h in range(vheads):
        hold_ref[h] = jnp.concatenate(
            [(row1 == col1).astype(f32), jnp.zeros((CHUNK, CHUNK), f32)], axis=1
        )

    def advance(chunk, i, solved, fresh, writes, ends):
        states = [hold_ref[h] for h in range(vheads)]
        packed = [s.astype(bf16) for s in states]
        taken = [mm(solved[i, h], packed[h]) for h in range(vheads)]
        updates = [
            jnp.concatenate(
                [taken[h][:, :WIDTH], fresh[i, h] + taken[h][:, WIDTH:]], axis=1
            ).astype(bf16)
            for h in range(vheads)
        ]
        for h in range(vheads):
            pair_ref[chunk, h, :CHUNK, :] = packed[h]
            pair_ref[chunk, h, CHUNK:, :] = updates[h]
            end = ends[chunk, 8 + h : 9 + h, :]
            hold_ref[h] = states[h] * jnp.concatenate([end, end], axis=1) + mm(
                writes[chunk, h], updates[h]
            )

    def read(chunk, keys):
        rows, start = rows_of(q_ref, q_pad, chunk)
        read_chunk(
            chunk, chunk, rows, start, qw_ref, gate_ref, keys, pair_ref, low_ref, wide_ref
        )

    def early_step(i, carry):
        advance(i, i, solved_ref, fresh_ref, later_write_ref, later_rows_ref)
        read(i, later_key_ref)
        return carry

    def late_step(i, carry):
        advance(
            count + i, i, late_solved_ref, late_fresh_ref, later_write_ref, later_rows_ref
        )
        return carry

    advance(0, 0, solved_ref, fresh_ref, write_ref, rows_ref)
    read(0, key_ref)
    lax.fori_loop(1, count, early_step, 0)
    lax.fori_loop(0, count, late_step, 0)


def chain_call(
    solved, fresh, write, rows, later, query, query_conv, rim, gates, keys, after, interpret=False
):
    later_keys, _, _, later_write, later_rows, late_solved, late_fresh, _ = later
    chunks, vheads = later_write.shape[:2]
    tokens = chunks * CHUNK
    return pl.pallas_call(
        chain_kernel,
        out_shape=(
            jax.ShapeDtypeStruct((chunks, vheads, 2 * CHUNK, 2 * WIDTH), bf16),
            jax.ShapeDtypeStruct((vheads, tokens, WIDTH), f32),
            jax.ShapeDtypeStruct((vheads, tokens, WIDTH), bf16),
            jax.ShapeDtypeStruct((8, WIDTH), f32),
        ),
        in_specs=[INSIDE] * 14 + [pl.BlockSpec(memory_space=pl.ANY)],
        out_specs=(INSIDE,) * 4,
        scratch_shapes=[
            pltpu.VMEM((vheads, WIDTH, 2 * WIDTH), f32), pad_scratch(query_conv.shape[1])
        ],
        compiler_params=pltpu.CompilerParams(vmem_limit_bytes=20 * MIB),
        cost_estimate=pl.CostEstimate(flops=1 << 32, transcendentals=0, bytes_accessed=0),
        interpret=interpret,
        name="chain",
    )(
        solved, fresh, late_solved, late_fresh, write, rows, later_write, later_rows,
        query.reshape(-1, WIDTH), query_conv, rim, gates, keys, later_keys, after,
    )


def read_kernel(
    q_ref, qw_ref, gate_ref, late_key_ref, pair_ref, old_low_ref, old_wide_ref, after_ref,
    low_ref, wide_ref, mark_ref,
):
    mark_ref[...] = jnp.zeros_like(mark_ref)
    chunks = gate_ref.shape[0]
    count = chunks // 2
    done = (chunks - count) * CHUNK
    low_ref[:, :done, :] = old_low_ref[:, :done, :]
    wide_ref[:, :done, :] = old_wide_ref[:, :done, :]

    def some(step, carry):
        for inner in range(READ):
            i = step * READ + inner
            chunk = chunks - count + i
            read_chunk(
                chunk, chunk, q_ref, chunk * CHUNK - PAD, qw_ref, gate_ref, late_key_ref, pair_ref,
                low_ref, wide_ref,
            )
        return carry

    lax.fori_loop(0, count // READ, some, 0)


def read_call(query, query_conv, gates, late_keys, pairs, low, wide, after, interpret=False):
    return pl.pallas_call(
        read_kernel,
        out_shape=(
            jax.ShapeDtypeStruct(low.shape, f32),
            jax.ShapeDtypeStruct(wide.shape, bf16),
            jax.ShapeDtypeStruct((8, WIDTH), f32),
        ),
        in_specs=[INSIDE] * 7 + [pl.BlockSpec(memory_space=pl.ANY)],
        out_specs=(INSIDE,) * 3,
        compiler_params=pltpu.CompilerParams(vmem_limit_bytes=20 * MIB),
        cost_estimate=pl.CostEstimate(flops=1 << 32, transcendentals=0, bytes_accessed=0),
        interpret=interpret,
        name="read_out",
    )(query.reshape(-1, WIDTH), query_conv, gates, late_keys, pairs, low, wide, after)


def rim_kernel(q_hbm, k_hbm, v_hbm, rim_ref, sems):
    first = 0
    copies = []
    for i, (source, heads) in enumerate(((q_hbm, 2), (k_hbm, 2), (v_hbm, 4))):
        rows = RIM * heads
        copies.append(
            pltpu.make_async_copy(
                source.at[pl.ds(source.shape[0] - rows, rows), :],
                rim_ref.at[pl.ds(first, rows), :],
                sems.at[i],
            )
        )
        first += rows
    for copy in copies:
        copy.start()
    for copy in copies:
        copy.wait()


def rim_call(query, key, value):
    flat = [stay(x.reshape(-1, WIDTH)) for x in (query, key, value)]
    rows = RIM * (query.shape[1] + key.shape[1] + value.shape[1])
    return pl.pallas_call(
        rim_kernel,
        out_shape=jax.ShapeDtypeStruct((rows, WIDTH), f32),
        in_specs=[pl.BlockSpec(memory_space=pltpu.HBM)] * 3,
        out_specs=pl.BlockSpec(memory_space=pltpu.VMEM),
        scratch_shapes=[pltpu.SemaphoreType.DMA((3,))],
        compiler_params=pltpu.CompilerParams(vmem_limit_bytes=1024 * 1024),
        name="rim",
    )(*flat)


def total_kernel(place_ref, mine_ref, other_ref, total_ref, first_ref):
    core = place_ref[2]
    for h in range(mine_ref.shape[0]):
        mine, other = mine_ref[h], other_ref[h]
        first = jnp.where(core == 0, mine, other)
        second = jnp.where(core == 0, other, mine)
        joined = mm(second[:, :WIDTH], first)
        total_ref[h] = jnp.concatenate(
            [joined[:, :WIDTH], joined[:, WIDTH:] + second[:, WIDTH:].astype(f32)], axis=1
        ).astype(bf16)
        first_ref[h] = first


def row_kernel(place_ref, a_ref, c_ref, b_ref, d_ref, mark_ref, total_ref, before_ref, all_ref, sum_ref):
    here = place_ref[1]
    heads = a_ref.shape[0]
    for k, ref in enumerate((a_ref, b_ref, c_ref, d_ref)):
        all_ref[(here + 4 - k) % 4] = ref[...]
    eye = lax.broadcasted_iota(jnp.int32, (WIDTH, 2 * WIDTH), 0) == lax.broadcasted_iota(
        jnp.int32, (WIDTH, 2 * WIDTH), 1
    )
    for h in range(heads):
        sum_ref[0, h] = eye.astype(f32).astype(bf16)
        sum_ref[1, h] = all_ref[0, h]
    for j in range(1, 4):
        for h in range(heads):
            joined = mm(all_ref[j, h, :, :WIDTH], sum_ref[j, h])
            value = jnp.concatenate(
                [joined[:, :WIDTH], joined[:, WIDTH:] + all_ref[j, h, :, WIDTH:].astype(f32)],
                axis=1,
            ).astype(bf16)
            if j < 3:
                sum_ref[j + 1, h] = value
            else:
                total_ref[h] = value
    before_ref[...] = sum_ref[here]


def prefix_kernel(
    place_ref, c_ref, b_ref, d_ref, before_ref, first_ref, mark_ref,
    mine_ref, send_ref, all_ref, sum_ref,
):
    here = place_ref[0]
    core = place_ref[2]
    heads = b_ref.shape[0]
    for k, ref in enumerate((b_ref, c_ref, d_ref)):
        all_ref[(here + 3 - k) % 4] = ref[...]
    for h in range(heads):
        sum_ref[0, h] = jnp.zeros((WIDTH, WIDTH), bf16)
        sum_ref[1, h] = all_ref[0, h, :, WIDTH:]
    for j in range(1, 3):
        for h in range(heads):
            moved = mm(all_ref[j, h, :, :WIDTH], sum_ref[j, h])
            sum_ref[j + 1, h] = (moved + all_ref[j, h, :, WIDTH:].astype(f32)).astype(bf16)
    for h in range(heads):
        row = sum_ref[here, h]
        before = (
            mm(before_ref[h, :, :WIDTH], row) + before_ref[h, :, WIDTH:].astype(f32)
        ).astype(bf16)
        after = mm(first_ref[h, :, :WIDTH], before) + first_ref[h, :, WIDTH:].astype(f32)
        wide = before.astype(f32)
        mine_ref[h] = jnp.where(core == 0, wide, after).astype(bf16)
        send_ref[h] = jnp.where(core == 0, after, wide).astype(bf16)


def small_call(kernel, outs, scratch, name, place, *arrays):
    inside = pl.BlockSpec(memory_space=pltpu.VMEM)
    return pl.pallas_call(
        kernel,
        out_shape=tuple(jax.ShapeDtypeStruct(shape, bf16) for shape in outs),
        in_specs=[pl.BlockSpec(memory_space=pltpu.SMEM)] + [inside] * len(arrays),
        out_specs=(inside,) * len(outs),
        scratch_shapes=[pltpu.VMEM(shape, bf16) for shape in scratch],
        compiler_params=pltpu.CompilerParams(vmem_limit_bytes=8 * 1024 * 1024),
        name=name,
    )(place, *arrays)


def output_kernel(
    place_ref, low_ref, wide_ref, near_ref, far_ref, gate_ref, gain_ref, weight_ref,
    *out_refs, slots
):
    core = place_ref[2]
    heads = low_ref.shape[0]
    half = heads // 2
    rows = out_refs[0].shape[0]
    for index, slot in enumerate(slots):
        start = pl.multiple_of(place_ref[3 + slot] * rows, rows)
        pieces = []
        for h in range(heads):
            entering = jnp.where(core == h // half, near_ref[h % half], far_ref[h % half])
            recurrent = low_ref[h, pl.ds(start, rows), :] + mm(
                wide_ref[h, pl.ds(start, rows), :], entering
            )
            scaled = recurrent * lax.rsqrt(
                jnp.mean(recurrent * recurrent, axis=1, keepdims=True) + norm_epsilon
            )
            gate = gate_ref[pl.ds(start * heads + h, rows, stride=heads), :]
            pieces.append((scaled * gain_ref[...] * silu(gate)).astype(bf16))
        normed = jnp.concatenate(pieces, axis=1)
        side = out_refs[0].shape[1]
        for k in range(2):
            out_refs[2 * index + k][...] = mm(
                normed, weight_ref[:, k * side : (k + 1) * side]
            ).astype(bf16)


def output_call(place, slots, low, wide, near, far, gate_in, norm_gain, out_weight):
    heads, tokens, _ = low.shape
    model = out_weight.shape[1]
    rows = tokens // 8
    inside = pl.BlockSpec(memory_space=pltpu.VMEM)
    piece = jax.ShapeDtypeStruct((rows, model // 2), bf16)
    return pl.pallas_call(
        functools.partial(output_kernel, slots=slots),
        out_shape=(piece,) * (2 * len(slots)),
        in_specs=[pl.BlockSpec(memory_space=pltpu.SMEM)] + [inside] * 7,
        out_specs=(inside,) * (2 * len(slots)),
        compiler_params=pltpu.CompilerParams(vmem_limit_bytes=16 * 1024 * 1024),
        cost_estimate=pl.CostEstimate(
            flops=2 * rows * heads * WIDTH * model * len(slots), transcendentals=0, bytes_accessed=0
        ),
        name="gated_output",
    )(
        place, low, wide, near, far,
        gate_in.reshape(tokens * heads, WIDTH), norm_gain.reshape(1, WIDTH), out_weight,
    )


def add_kernel(left_ref, right_ref, out_ref):
    out_ref[...] = (left_ref[...].astype(f32) + right_ref[...].astype(f32)).astype(bf16)


def add(left, right):
    inside = pl.BlockSpec(memory_space=pltpu.VMEM)
    return pl.pallas_call(
        add_kernel,
        out_shape=jax.ShapeDtypeStruct(left.shape, bf16),
        in_specs=[inside] * 2,
        out_specs=inside,
        compiler_params=pltpu.CompilerParams(vmem_limit_bytes=2 * 1024 * 1024),
        name="add",
    )(left, right)


def last_kernel(*refs):
    out_ref = refs[-1]
    side = refs[0].shape[1]
    for k in range(2):
        total = refs[k][...].astype(f32)
        for other in (refs[2 + k], refs[4 + k]):
            total = total + other[...].astype(f32)
        out_ref[:, k * side : (k + 1) * side] = total


def last_call(*arrays):
    rows, side = arrays[0].shape
    inside = pl.BlockSpec(memory_space=pltpu.VMEM)
    return pl.pallas_call(
        last_kernel,
        out_shape=jax.ShapeDtypeStruct((rows, 2 * side), f32),
        in_specs=[inside] * 6,
        out_specs=inside,
        compiler_params=pltpu.CompilerParams(vmem_limit_bytes=8 * 1024 * 1024),
        name="last_add",
    )(*arrays)


def shifted(value, axis, steps, around=True):
    count = lax.axis_size(axis)
    pairs = [(i, (i + steps) % count) for i in range(count) if around or 0 <= i + steps < count]
    return lax.ppermute(value, axis, pairs)


def head_sum(parts):
    def right(value):
        return shifted(value, "head", 1)

    def left(value):
        return shifted(value, "head", -1)

    far, up_parts, down_parts, own = parts[0], parts[1:7:2], parts[2:7:2], parts[7]
    up = [right(far[0]), right(up_parts[0][1])]
    down = [left(down_parts[0][0]), left(far[1])]
    up = [right(add(up_parts[0][0], up[0])), up[1]]
    down = [down[0], left(add(down_parts[0][1], down[1]))]
    for step in (1, 2):
        for side in (1, 0):
            up[side] = right(add(up_parts[step][side], up[side]))
            down[1 - side] = left(add(down_parts[step][1 - side], down[1 - side]))
    return last_call(*own, *up, *down)


def on_device(
    query_in, key_in, value_in, gate_in, log_gate, strength,
    query_conv, key_conv, value_conv, norm_gain, out_weight,
):
    z = lax.axis_index("head")
    order = [(z + shift) & 7 for shift in (4, 3, 5, 2, 6, 1, 7, 0)]
    place = jnp.stack(
        [lax.axis_index("ctx_0"), lax.axis_index("ctx_1"), lax.axis_index("ctx_2")] + order
    ).astype(jnp.int32)
    rim = shifted(rim_call(query_in, key_in, value_in), CTX, 1, around=False)
    vheads, tokens = log_gate.shape
    gates = jnp.concatenate(
        [
            log_gate.reshape(vheads, tokens // CHUNK, CHUNK),
            strength.reshape(vheads, tokens // CHUNK, CHUNK),
        ],
        axis=0,
    ).transpose(1, 0, 2)
    later = first_call(place, key_in, value_in, key_conv, value_conv, gates)
    keys, write, ends, solved, fresh, mine, other = local_call(
        place, key_in, value_in, key_conv, value_conv, rim, gates, later
    )
    other = shifted(other, "ctx_2", 1)
    half = vheads // 2
    maps = (half, WIDTH, 2 * WIDTH)
    states = (half, WIDTH, WIDTH)
    total, first = small_call(total_kernel, (maps, maps), (), "chip_total", place, mine, other)
    pairs, low, wide, mark = chain_call(
        solved, fresh, write, ends, later, query_in, query_conv, rim, gates, keys, first
    )
    row = {k: shifted(total, "ctx_1", k) for k in (2, 1, 3)}
    row_total, before = small_call(
        row_kernel, (maps, maps), ((4,) + maps, (4,) + maps), "row_total", place, total, row[2], row[1], row[3], mark
    )
    rows = {k: shifted(row_total, "ctx_0", k, around=False) for k in (2, 1, 3)}
    low, wide, mark = read_call(
        query_in, query_conv, gates, later[0], pairs, low, wide, before
    )
    near, send = small_call(
        prefix_kernel, (states, states), ((4,) + maps, (4,) + states), "prefix",
        place, rows[2], rows[1], rows[3], before, first, mark,
    )
    far = shifted(send, "ctx_2", 1)
    tail = (low, wide, near, far, gate_in, norm_gain, out_weight)
    parts = []
    for slots in ((0,), (1, 2), (3, 4), (5, 6, 7)):
        pieces = output_call(place, slots, *tail)
        parts += [pieces[2 * i : 2 * i + 2] for i in range(len(slots))]
    return head_sum(parts)


def solution(mesh):
    split = Mesh(
        mesh.devices.reshape(4, 4, 2, mesh.shape["head"]), ("ctx_0", "ctx_1", "ctx_2", "head")
    )
    in_specs = (
        P(CTX, "head", None),
        P(CTX, "head", None),
        P(CTX, "head", None),
        P(CTX, "head", None),
        P("head", CTX),
        P("head", CTX),
        P(None, "head", None),
        P(None, "head", None),
        P(None, "head", None),
        P(),
        P("head", None),
    )
    return jax.shard_map(
        on_device, mesh=split, in_specs=in_specs, out_specs=P(CTX_HEAD, None), check_vma=False
    )
```

```python
import functools
import jax
import jax.numpy as jnp
from jax import lax
from jax.experimental import pallas as pl
from jax.experimental.pallas import tpu as pltpu
from jax.sharding import Mesh
from jax.sharding import PartitionSpec as P

CTX = ("ctx_0", "ctx_1", "ctx_2")
CTX_HEAD = ("ctx_0", "ctx_1", "ctx_2", "head")
CHUNK = 128
WIDTH = 128
PAD = 8
RIM = 4
READ = 2
norm_epsilon = 1e-06
LOG2E = 1.4426950408889634
f32 = jnp.float32
bf16 = jnp.bfloat16


def mm(left, right):
    return jnp.dot(left, right, preferred_element_type=f32)


def silu_of_half(half):
    return half + half * jnp.tanh(half)


def silu(u):
    return silu_of_half(0.5 * u)


def paired(x):
    zero = jnp.zeros((CHUNK, CHUNK), x.dtype)
    top = jnp.concatenate([x[:, :CHUNK], zero], axis=1)
    low = jnp.concatenate([zero, x[:, CHUNK:]], axis=1)
    return jnp.concatenate([top, low], axis=0)


def mix(target, weight_ref, heads, head, start):
    total = None
    for tap in range(4):
        piece = target[pl.ds((start + PAD - 3 + tap) * heads + head, CHUNK, stride=heads), :]
        part = (0.5 * weight_ref[tap, head : head + 1, :]) * piece
        total = part if total is None else total + part
    return silu_of_half(total)


def unit(x):
    return x * lax.rsqrt(jnp.sum(x * x, axis=1, keepdims=True) + norm_epsilon)


def squares():
    row = lax.broadcasted_iota(jnp.int32, (CHUNK, CHUNK), 0)
    col = lax.broadcasted_iota(jnp.int32, (CHUNK, CHUNK), 1)
    return row, col


def running_sums(gates, adder):
    hi = gates.astype(bf16).astype(f32)
    rest = gates - hi
    mid = rest.astype(bf16).astype(f32)
    parts = jnp.concatenate([hi, mid, rest - mid], axis=0).astype(bf16)
    sums = mm(parts, adder)
    return (sums[0:8] + sums[8:16] + sums[16:24]) * LOG2E


def spread(columns, index):
    return jnp.broadcast_to(columns[:, index : index + 1], (CHUNK, CHUNK))


def fill_pad(pad, source, heads, rim_ref, first):
    pad[pl.ds((PAD - RIM) * heads, RIM * heads), :] = rim_ref[first : first + RIM * heads, :]
    pad[pl.ds(PAD * heads, CHUNK * heads), :] = source[pl.ds(0, CHUNK * heads), :]


def rows_of(source, pad, chunk):
    if isinstance(chunk, int) and chunk == 0:
        return pad, 0
    return source, chunk * CHUNK - PAD


def together(*steps):
    live = list(steps)
    while live:
        still = []
        for step, weight in live:
            alive = True
            for _ in range(weight):
                if next(step, "end") == "end":
                    alive = False
                    break
            if alive:
                still.append((step, weight))
        live = still


def fill_masks(mask_ref):
    row = lax.broadcasted_iota(jnp.int32, (CHUNK, 2 * CHUNK), 0)
    col = lax.broadcasted_iota(jnp.int32, (CHUNK, 2 * CHUNK), 1) & (CHUNK - 1)

    def same(bits):
        return (row >> bits) == (col >> bits)

    mask_ref[0] = same(4).astype(bf16)
    for level in range(3):
        mask_ref[1 + level] = (same(5 + level) & jnp.logical_not(same(4 + level))).astype(bf16)
    mask_ref[4] = (row == col).astype(bf16)


class View:
    def __init__(self, ref, base):
        self.ref, self.base = ref, base

    def __getitem__(self, key):
        return self.ref[(key[0] + self.base,) + key[1:]]

    def __setitem__(self, key, value):
        self.ref[(key[0] + self.base,) + key[1:]] = value


def prepare(group, first, sources, pads, weights, gate_ref, store):
    kw_ref, vw_ref = weights
    key_ref, mixing_ref, value_ref, write_ref, rows_ref = store
    qheads = kw_ref.shape[1]
    vheads = vw_ref.shape[1]
    ratio = vheads // qheads
    row1, col1 = squares()
    strict = row1 > col1
    adder = (row1 <= col1).astype(bf16)
    for i in group:
        (k_rows, start), (v_rows, _) = [
            rows_of(source, pad, first + i) for source, pad in zip(sources, pads)
        ]
        gates = gate_ref[first + i]
        running = running_sums(gates, adder)
        strengths = gates[4:8]
        scaled = running[0:4] + jnp.log2(strengths)
        columns = jnp.concatenate([scaled, scaled], axis=0).T
        end_row = running[:, CHUNK - 1 : CHUNK]
        tail_row = jnp.exp2(end_row - running)
        rows_ref[i, 0:4, :] = -jnp.exp2(scaled)
        rows_ref[i, 4:8, :] = strengths
        rows_ref[i, 8:16, :] = jnp.broadcast_to(jnp.exp2(end_row), (8, CHUNK))
        for g in range(qheads):
            key = unit(mix(k_rows, kw_ref, qheads, g, start))
            key_t = key.T
            packed = key.astype(bf16)
            key_ref[i, g] = packed
            kk = mm(packed, key_t.astype(bf16))
            yield
            for side in range(ratio):
                head = g * ratio + side
                table = jnp.where(
                    strict, jnp.exp2(spread(columns, head) - running[head : head + 1, :]), 0.0
                )
                lanes = slice(side * CHUNK, (side + 1) * CHUNK)
                mixing_ref[i, g, :, lanes] = (kk * table).astype(bf16)
                write_ref[i, head] = (key_t * tail_row[head : head + 1, :]).astype(bf16)
                value_ref[i, head] = mix(v_rows, vw_ref, vheads, head, start).astype(bf16)
                yield


def invert(count, store, qheads, vheads, mask_ref, solved_ref, fresh_ref):
    key_ref, mixing_ref, value_ref, write_ref, rows_ref = store
    ratio = vheads // qheads
    units = [(i, g) for i in range(count) for g in range(qheads)]

    def mixing(level):
        return [mixing_ref[i, g] * mask_ref[level] for i, g in units]

    eye = mask_ref[4]
    powers = mixing(0)
    inverses = [eye - p for p in powers]
    powers = [mm(p, paired(p)).astype(bf16) for p in powers]
    yield
    for step in range(3):
        inverses = [mm(eye + p, paired(x)).astype(bf16) for p, x in zip(powers, inverses)]
        yield
        if step < 2:
            powers = [mm(p, paired(p)).astype(bf16) for p in powers]
            yield
    for level in range(3):
        crossed = [
            eye - mm(m, paired(x)).astype(bf16) for m, x in zip(mixing(1 + level), inverses)
        ]
        yield
        inverses = [mm(x, paired(y)) for x, y in zip(inverses, crossed)]
        if level < 2:
            inverses = [x.astype(bf16) for x in inverses]
        yield
    for (i, g), inverse in zip(units, inverses):
        for side in range(ratio):
            head = g * ratio + side
            own = inverse[:, side * CHUNK : (side + 1) * CHUNK]
            left = jnp.concatenate(
                [own * rows_ref[i, head : head + 1, :], own * rows_ref[i, 4 + head : 5 + head, :]],
                axis=1,
            ).astype(bf16)
            right = jnp.concatenate([key_ref[i, g], value_ref[i, head]], axis=1)
            answer = mm(left, paired(right))
            solved_ref[i, head] = answer[:, :CHUNK].astype(bf16)
            fresh_ref[i, head] = answer[:, CHUNK:]
        yield


def join(later, earlier):
    keep1, change1, offset1 = later
    keep0, change0, offset0 = earlier
    moved = mm(change1.astype(bf16), jnp.concatenate([change0, offset0], axis=1).astype(bf16))
    return (
        keep1 * keep0,
        moved[:, :WIDTH] + (keep1 * change0 + keep0 * change1),
        moved[:, WIDTH:] + (keep1 * offset0 + offset1),
    )


def chain_maps(count, store, solved_ref, fresh_ref, vheads, result):
    _, _, _, write_ref, rows_ref = store
    maps = []
    for i in range(count):
        row = []
        for h in range(vheads):
            moved = mm(
                write_ref[i, h],
                jnp.concatenate(
                    [solved_ref[i, h], fresh_ref[i, h].astype(bf16)], axis=1
                ),
            )
            row.append((rows_ref[i, 8 + h : 9 + h, :], moved[:, :WIDTH], moved[:, WIDTH:]))
        maps.append(row)
        yield
    while len(maps) > 1:
        maps = [
            [join(later, earlier) for later, earlier in zip(maps[k + 1], maps[k])]
            for k in range(0, len(maps), 2)
        ]
        yield
    result.extend(maps[0])


def split_store(refs, base):
    return tuple(View(ref, base) for ref in refs)


def first_kernel(
    place_ref, k_ref, v_ref, kw_ref, vw_ref, gate_ref,
    key_ref, mixing_ref, value_ref, write_ref, rows_ref, solved_ref, fresh_ref, mask_ref,
):
    chunks = gate_ref.shape[0]
    count = chunks // 2
    fill_masks(mask_ref)
    whole = (key_ref, mixing_ref, value_ref, write_ref, rows_ref)
    late = split_store(whole, count)
    sources = ((k_ref, v_ref), (None, None), (kw_ref, vw_ref), gate_ref)
    together((prepare(range(count), count, *sources, late), 1))
    together(
        (
            invert(
                count, late, key_ref.shape[1], value_ref.shape[1], mask_ref,
                solved_ref, fresh_ref,
            ),
            1,
        ),
        (prepare(range(1, count), 0, *sources, whole), 2),
    )


def local_kernel(
    place_ref, k_ref, v_ref, kw_ref, vw_ref, rim_ref, gate_ref,
    later_key_ref, later_mixing_ref, later_value_ref, later_write_ref, later_rows_ref,
    late_solved_ref, late_fresh_ref, mask_ref,
    key_ref, write_ref, rows_ref, solved_ref, fresh_ref, near_ref, far_ref,
    mixing_ref, value_ref, k_pad, v_pad,
):
    core = place_ref[2]
    chunks = gate_ref.shape[0]
    count = chunks // 2
    qheads = kw_ref.shape[1]
    vheads = vw_ref.shape[1]
    fill_pad(k_pad, k_ref, qheads, rim_ref, RIM * qheads)
    fill_pad(v_pad, v_ref, vheads, rim_ref, 2 * RIM * qheads)
    opening = (key_ref, mixing_ref, value_ref, write_ref, rows_ref)
    rest = (later_key_ref, later_mixing_ref, later_value_ref, later_write_ref, later_rows_ref)
    early = tuple(Joined(head, tail) for head, tail in zip(opening, rest))
    late = split_store(rest, count)
    first_half, second_half = [], []
    together(
        (
            prepare(
                range(1), 0, (k_ref, v_ref), (k_pad, v_pad), (kw_ref, vw_ref), gate_ref, opening
            ),
            1,
        ),
        (
            chain_maps(
                count, late, late_solved_ref, late_fresh_ref, vheads, second_half
            ),
            1,
        ),
    )
    together(
        (invert(count, early, qheads, vheads, mask_ref, solved_ref, fresh_ref), 1),
    )
    together((chain_maps(count, early, solved_ref, fresh_ref, vheads, first_half), 1))
    half = vheads // 2
    row1, col1 = squares()
    for h in range(vheads):
        keep, change, offset = join(second_half[h], first_half[h])
        packed = jnp.concatenate(
            [change + jnp.where(row1 == col1, keep, 0.0), offset], axis=1
        ).astype(bf16)

        @pl.when(core == h // half)
        def _():
            near_ref[h % half] = packed

        @pl.when(core != h // half)
        def _():
            far_ref[h % half] = packed


class Joined:
    def __init__(self, head, tail):
        self.head, self.tail = head, tail

    def __getitem__(self, key):
        return self.head[key] if key[0] == 0 else self.tail[key]


def stay(value):
    return pltpu.with_memory_space_constraint(value, pltpu.HBM)


INSIDE = pl.BlockSpec(memory_space=pltpu.VMEM)
SCALAR = pl.BlockSpec(memory_space=pltpu.SMEM)
MIB = 1024 * 1024


def group_shapes(count, qheads, vheads):
    return (
        jax.ShapeDtypeStruct((count, qheads, CHUNK, WIDTH), bf16),
        jax.ShapeDtypeStruct((count, qheads, CHUNK, 2 * CHUNK), bf16),
        jax.ShapeDtypeStruct((count, vheads, CHUNK, WIDTH), bf16),
        jax.ShapeDtypeStruct((count, vheads, CHUNK, CHUNK), bf16),
        jax.ShapeDtypeStruct((count, 16, CHUNK), f32),
    )


def pad_scratch(heads):
    return pltpu.VMEM(((PAD + CHUNK) * heads, WIDTH), f32)


def first_call(place, key, value, key_conv, value_conv, gates, interpret=False):
    chunks = gates.shape[0]
    count = chunks // 2
    vheads = value_conv.shape[1]
    return pl.pallas_call(
        first_kernel,
        out_shape=group_shapes(chunks, key_conv.shape[1], vheads)
        + (
            jax.ShapeDtypeStruct((count, vheads, CHUNK, WIDTH), bf16),
            jax.ShapeDtypeStruct((count, vheads, CHUNK, WIDTH), f32),
            jax.ShapeDtypeStruct((5, CHUNK, 2 * CHUNK), bf16),
        ),
        in_specs=[SCALAR] + [INSIDE] * 5,
        out_specs=(INSIDE,) * 8,
        compiler_params=pltpu.CompilerParams(vmem_limit_bytes=16 * MIB),
        cost_estimate=pl.CostEstimate(flops=1 << 32, transcendentals=0, bytes_accessed=0),
        interpret=interpret,
        name="first_map",
    )(place, key.reshape(-1, WIDTH), value.reshape(-1, WIDTH), key_conv, value_conv, gates)


def local_call(place, key, value, key_conv, value_conv, rim, gates, later, interpret=False):
    chunks = gates.shape[0]
    count = chunks // 2
    qheads = key_conv.shape[1]
    vheads = value_conv.shape[1]
    shapes = group_shapes(1, qheads, vheads)
    pair = jax.ShapeDtypeStruct((vheads // 2, WIDTH, 2 * WIDTH), bf16)
    return pl.pallas_call(
        local_kernel,
        out_shape=(
            shapes[0],
            shapes[3],
            shapes[4],
            jax.ShapeDtypeStruct((count, vheads, CHUNK, WIDTH), bf16),
            jax.ShapeDtypeStruct((count, vheads, CHUNK, WIDTH), f32),
            pair,
            pair,
        ),
        in_specs=[SCALAR] + [INSIDE] * 14,
        out_specs=(INSIDE,) * 7,
        scratch_shapes=[
            pltpu.VMEM(shapes[1].shape, bf16),
            pltpu.VMEM(shapes[2].shape, bf16),
            pad_scratch(qheads),
            pad_scratch(vheads),
        ],
        compiler_params=pltpu.CompilerParams(vmem_limit_bytes=20 * MIB),
        interpret=interpret,
        name="local_map",
    )(
        place, key.reshape(-1, WIDTH), value.reshape(-1, WIDTH), key_conv, value_conv, rim,
        gates, *later,
    )


def read_chunk(chunk, i, rows, start, qw_ref, gate_ref, key_ref, pair_ref, low_ref, wide_ref):
    qheads = qw_ref.shape[1]
    ratio = pair_ref.shape[1] // qheads
    row1, col1 = squares()
    running = running_sums(gate_ref[chunk], (row1 <= col1).astype(bf16))
    columns = running.T
    target = pl.ds(pl.multiple_of(chunk * CHUNK, CHUNK), CHUNK)
    for g in range(qheads):
        query = unit(mix(rows, qw_ref, qheads, g, start)) * (WIDTH ** -0.5)
        qk = lax.dot_general(
            query.astype(bf16), key_ref[i, g], (((1,), (1,)), ((), ())),
            preferred_element_type=f32,
        )
        for side in range(ratio):
            head = g * ratio + side
            decay_col = spread(columns, head)
            table = jnp.where(
                row1 >= col1, jnp.exp2(decay_col - running[head : head + 1, :]), 0.0
            )
            lift = jnp.exp2(decay_col)
            reading = jnp.concatenate(
                [(lift * query).astype(bf16), (qk * table).astype(bf16)], axis=1
            )
            result = mm(reading, pair_ref[chunk, head])
            wide_ref[head, target, :] = result[:, :WIDTH].astype(bf16)
            low_ref[head, target, :] = result[:, WIDTH:]


def chain_kernel(
    solved_ref, fresh_ref, late_solved_ref, late_fresh_ref,
    write_ref, rows_ref, later_write_ref, later_rows_ref,
    q_ref, qw_ref, rim_ref, gate_ref, key_ref, later_key_ref, after_ref,
    pair_ref, low_ref, wide_ref, mark_ref, hold_ref, q_pad,
):
    count, vheads = solved_ref.shape[:2]
    mark_ref[...] = jnp.zeros_like(mark_ref)
    fill_pad(q_pad, q_ref, qw_ref.shape[1], rim_ref, 0)
    row1, col1 = squares()
    for h in range(vheads):
        hold_ref[h] = jnp.concatenate(
            [(row1 == col1).astype(f32), jnp.zeros((CHUNK, CHUNK), f32)], axis=1
        )

    def advance(chunk, i, solved, fresh, writes, ends):
        states = [hold_ref[h] for h in range(vheads)]
        packed = [s.astype(bf16) for s in states]
        taken = [mm(solved[i, h], packed[h]) for h in range(vheads)]
        updates = [
            jnp.concatenate(
                [taken[h][:, :WIDTH], fresh[i, h] + taken[h][:, WIDTH:]], axis=1
            ).astype(bf16)
            for h in range(vheads)
        ]
        for h in range(vheads):
            pair_ref[chunk, h, :CHUNK, :] = packed[h]
            pair_ref[chunk, h, CHUNK:, :] = updates[h]
            end = ends[chunk, 8 + h : 9 + h, :]
            hold_ref[h] = states[h] * jnp.concatenate([end, end], axis=1) + mm(
                writes[chunk, h], updates[h]
            )

    def read(chunk, keys):
        rows, start = rows_of(q_ref, q_pad, chunk)
        read_chunk(
            chunk, chunk, rows, start, qw_ref, gate_ref, keys, pair_ref, low_ref, wide_ref
        )

    def early_step(i, carry):
        advance(i, i, solved_ref, fresh_ref, later_write_ref, later_rows_ref)
        read(i, later_key_ref)
        return carry

    def late_step(i, carry):
        advance(
            count + i, i, late_solved_ref, late_fresh_ref, later_write_ref, later_rows_ref
        )
        return carry

    advance(0, 0, solved_ref, fresh_ref, write_ref, rows_ref)
    read(0, key_ref)
    lax.fori_loop(1, count, early_step, 0)
    lax.fori_loop(0, count, late_step, 0)


def chain_call(
    solved, fresh, write, rows, later, query, query_conv, rim, gates, keys, after, interpret=False
):
    later_keys, _, _, later_write, later_rows, late_solved, late_fresh, _ = later
    chunks, vheads = later_write.shape[:2]
    tokens = chunks * CHUNK
    return pl.pallas_call(
        chain_kernel,
        out_shape=(
            jax.ShapeDtypeStruct((chunks, vheads, 2 * CHUNK, 2 * WIDTH), bf16),
            jax.ShapeDtypeStruct((vheads, tokens, WIDTH), f32),
            jax.ShapeDtypeStruct((vheads, tokens, WIDTH), bf16),
            jax.ShapeDtypeStruct((8, WIDTH), f32),
        ),
        in_specs=[INSIDE] * 14 + [pl.BlockSpec(memory_space=pl.ANY)],
        out_specs=(INSIDE,) * 4,
        scratch_shapes=[
            pltpu.VMEM((vheads, WIDTH, 2 * WIDTH), f32), pad_scratch(query_conv.shape[1])
        ],
        compiler_params=pltpu.CompilerParams(vmem_limit_bytes=20 * MIB),
        cost_estimate=pl.CostEstimate(flops=1 << 32, transcendentals=0, bytes_accessed=0),
        interpret=interpret,
        name="chain",
    )(
        solved, fresh, late_solved, late_fresh, write, rows, later_write, later_rows,
        query.reshape(-1, WIDTH), query_conv, rim, gates, keys, later_keys, after,
    )


def read_kernel(
    q_ref, qw_ref, gate_ref, late_key_ref, pair_ref, old_low_ref, old_wide_ref, after_ref,
    low_ref, wide_ref, mark_ref,
):
    mark_ref[...] = jnp.zeros_like(mark_ref)
    chunks = gate_ref.shape[0]
    count = chunks // 2
    done = (chunks - count) * CHUNK
    low_ref[:, :done, :] = old_low_ref[:, :done, :]
    wide_ref[:, :done, :] = old_wide_ref[:, :done, :]

    def some(step, carry):
        for inner in range(READ):
            i = step * READ + inner
            chunk = chunks - count + i
            read_chunk(
                chunk, chunk, q_ref, chunk * CHUNK - PAD, qw_ref, gate_ref, late_key_ref, pair_ref,
                low_ref, wide_ref,
            )
        return carry

    lax.fori_loop(0, count // READ, some, 0)


def read_call(query, query_conv, gates, late_keys, pairs, low, wide, after, interpret=False):
    return pl.pallas_call(
        read_kernel,
        out_shape=(
            jax.ShapeDtypeStruct(low.shape, f32),
            jax.ShapeDtypeStruct(wide.shape, bf16),
            jax.ShapeDtypeStruct((8, WIDTH), f32),
        ),
        in_specs=[INSIDE] * 7 + [pl.BlockSpec(memory_space=pl.ANY)],
        out_specs=(INSIDE,) * 3,
        compiler_params=pltpu.CompilerParams(vmem_limit_bytes=20 * MIB),
        cost_estimate=pl.CostEstimate(flops=1 << 32, transcendentals=0, bytes_accessed=0),
        interpret=interpret,
        name="read_out",
    )(query.reshape(-1, WIDTH), query_conv, gates, late_keys, pairs, low, wide, after)


def rim_kernel(q_hbm, k_hbm, v_hbm, rim_ref, sems):
    first = 0
    copies = []
    for i, (source, heads) in enumerate(((q_hbm, 2), (k_hbm, 2), (v_hbm, 4))):
        rows = RIM * heads
        copies.append(
            pltpu.make_async_copy(
                source.at[pl.ds(source.shape[0] - rows, rows), :],
                rim_ref.at[pl.ds(first, rows), :],
                sems.at[i],
            )
        )
        first += rows
    for copy in copies:
        copy.start()
    for copy in copies:
        copy.wait()


def rim_call(query, key, value):
    flat = [stay(x.reshape(-1, WIDTH)) for x in (query, key, value)]
    rows = RIM * (query.shape[1] + key.shape[1] + value.shape[1])
    return pl.pallas_call(
        rim_kernel,
        out_shape=jax.ShapeDtypeStruct((rows, WIDTH), f32),
        in_specs=[pl.BlockSpec(memory_space=pltpu.HBM)] * 3,
        out_specs=pl.BlockSpec(memory_space=pltpu.VMEM),
        scratch_shapes=[pltpu.SemaphoreType.DMA((3,))],
        compiler_params=pltpu.CompilerParams(vmem_limit_bytes=1024 * 1024),
        name="rim",
    )(*flat)


def total_kernel(place_ref, mine_ref, other_ref, total_ref, first_ref):
    core = place_ref[2]
    for h in range(mine_ref.shape[0]):
        mine, other = mine_ref[h], other_ref[h]
        first = jnp.where(core == 0, mine, other)
        second = jnp.where(core == 0, other, mine)
        joined = mm(second[:, :WIDTH], first)
        total_ref[h] = jnp.concatenate(
            [joined[:, :WIDTH], joined[:, WIDTH:] + second[:, WIDTH:].astype(f32)], axis=1
        ).astype(bf16)
        first_ref[h] = first


def row_kernel(place_ref, a_ref, b_ref, c_ref, d_ref, mark_ref, total_ref, before_ref, all_ref, sum_ref):
    here = place_ref[1]
    heads = a_ref.shape[0]
    for k, ref in enumerate((a_ref, b_ref, c_ref, d_ref)):
        all_ref[(here + 4 - k) % 4] = ref[...]
    eye = lax.broadcasted_iota(jnp.int32, (WIDTH, 2 * WIDTH), 0) == lax.broadcasted_iota(
        jnp.int32, (WIDTH, 2 * WIDTH), 1
    )
    for h in range(heads):
        sum_ref[0, h] = eye.astype(f32).astype(bf16)
        sum_ref[1, h] = all_ref[0, h]
    for j in range(1, 4):
        for h in range(heads):
            joined = mm(all_ref[j, h, :, :WIDTH], sum_ref[j, h])
            value = jnp.concatenate(
                [joined[:, :WIDTH], joined[:, WIDTH:] + all_ref[j, h, :, WIDTH:].astype(f32)],
                axis=1,
            ).astype(bf16)
            if j < 3:
                sum_ref[j + 1, h] = value
            else:
                total_ref[h] = value
    before_ref[...] = sum_ref[here]


def prefix_kernel(
    place_ref, b_ref, c_ref, d_ref, before_ref, first_ref, mark_ref,
    mine_ref, send_ref, all_ref, sum_ref,
):
    here = place_ref[0]
    core = place_ref[2]
    heads = b_ref.shape[0]
    for k, ref in enumerate((b_ref, c_ref, d_ref)):
        all_ref[(here + 3 - k) % 4] = ref[...]
    for h in range(heads):
        sum_ref[0, h] = jnp.zeros((WIDTH, WIDTH), bf16)
        sum_ref[1, h] = all_ref[0, h, :, WIDTH:]
    for j in range(1, 3):
        for h in range(heads):
            moved = mm(all_ref[j, h, :, :WIDTH], sum_ref[j, h])
            sum_ref[j + 1, h] = (moved + all_ref[j, h, :, WIDTH:].astype(f32)).astype(bf16)
    for h in range(heads):
        row = sum_ref[here, h]
        before = (
            mm(before_ref[h, :, :WIDTH], row) + before_ref[h, :, WIDTH:].astype(f32)
        ).astype(bf16)
        after = mm(first_ref[h, :, :WIDTH], before) + first_ref[h, :, WIDTH:].astype(f32)
        wide = before.astype(f32)
        mine_ref[h] = jnp.where(core == 0, wide, after).astype(bf16)
        send_ref[h] = jnp.where(core == 0, after, wide).astype(bf16)


def small_call(kernel, outs, scratch, name, place, *arrays):
    inside = pl.BlockSpec(memory_space=pltpu.VMEM)
    return pl.pallas_call(
        kernel,
        out_shape=tuple(jax.ShapeDtypeStruct(shape, bf16) for shape in outs),
        in_specs=[pl.BlockSpec(memory_space=pltpu.SMEM)] + [inside] * len(arrays),
        out_specs=(inside,) * len(outs),
        scratch_shapes=[pltpu.VMEM(shape, bf16) for shape in scratch],
        compiler_params=pltpu.CompilerParams(vmem_limit_bytes=8 * 1024 * 1024),
        name=name,
    )(place, *arrays)


def output_kernel(
    place_ref, low_ref, wide_ref, near_ref, far_ref, gate_ref, gain_ref, weight_ref,
    *out_refs, slots
):
    core = place_ref[2]
    heads = low_ref.shape[0]
    half = heads // 2
    rows = out_refs[0].shape[0]
    for index, slot in enumerate(slots):
        start = pl.multiple_of(place_ref[3 + slot] * rows, rows)
        pieces = []
        for h in range(heads):
            entering = jnp.where(core == h // half, near_ref[h % half], far_ref[h % half])
            recurrent = low_ref[h, pl.ds(start, rows), :] + mm(
                wide_ref[h, pl.ds(start, rows), :], entering
            )
            scaled = recurrent * lax.rsqrt(
                jnp.mean(recurrent * recurrent, axis=1, keepdims=True) + norm_epsilon
            )
            gate = gate_ref[pl.ds(start * heads + h, rows, stride=heads), :]
            pieces.append((scaled * gain_ref[...] * silu(gate)).astype(bf16))
        normed = jnp.concatenate(pieces, axis=1)
        side = out_refs[0].shape[1]
        for k in range(2):
            out_refs[2 * index + k][...] = mm(
                normed, weight_ref[:, k * side : (k + 1) * side]
            ).astype(bf16)


def output_call(place, slots, low, wide, near, far, gate_in, norm_gain, out_weight):
    heads, tokens, _ = low.shape
    model = out_weight.shape[1]
    rows = tokens // 8
    inside = pl.BlockSpec(memory_space=pltpu.VMEM)
    piece = jax.ShapeDtypeStruct((rows, model // 2), bf16)
    return pl.pallas_call(
        functools.partial(output_kernel, slots=slots),
        out_shape=(piece,) * (2 * len(slots)),
        in_specs=[pl.BlockSpec(memory_space=pltpu.SMEM)] + [inside] * 7,
        out_specs=(inside,) * (2 * len(slots)),
        compiler_params=pltpu.CompilerParams(vmem_limit_bytes=16 * 1024 * 1024),
        cost_estimate=pl.CostEstimate(
            flops=2 * rows * heads * WIDTH * model * len(slots), transcendentals=0, bytes_accessed=0
        ),
        name="gated_output",
    )(
        place, low, wide, near, far,
        gate_in.reshape(tokens * heads, WIDTH), norm_gain.reshape(1, WIDTH), out_weight,
    )


def add_kernel(left_ref, right_ref, out_ref):
    out_ref[...] = (left_ref[...].astype(f32) + right_ref[...].astype(f32)).astype(bf16)


def add(left, right):
    inside = pl.BlockSpec(memory_space=pltpu.VMEM)
    return pl.pallas_call(
        add_kernel,
        out_shape=jax.ShapeDtypeStruct(left.shape, bf16),
        in_specs=[inside] * 2,
        out_specs=inside,
        compiler_params=pltpu.CompilerParams(vmem_limit_bytes=2 * 1024 * 1024),
        name="add",
    )(left, right)


def sum_kernel(left_ref, right_ref, out_ref):
    out_ref[...] = left_ref[...].astype(f32) + right_ref[...].astype(f32)


def sum_call(left, right):
    return pl.pallas_call(
        sum_kernel,
        out_shape=jax.ShapeDtypeStruct(left.shape, f32),
        in_specs=[INSIDE] * 2,
        out_specs=INSIDE,
        compiler_params=pltpu.CompilerParams(vmem_limit_bytes=2 * MIB),
        name="early_sum",
    )(left, right)


def last_kernel(*refs):
    out_ref = refs[-1]
    side = refs[0].shape[1]
    for k in range(2):
        out_ref[:, k * side : (k + 1) * side] = refs[k][...] + refs[2 + k][...].astype(f32)


def last_call(*arrays):
    rows, side = arrays[0].shape
    return pl.pallas_call(
        last_kernel,
        out_shape=jax.ShapeDtypeStruct((rows, 2 * side), f32),
        in_specs=[INSIDE] * 4,
        out_specs=INSIDE,
        compiler_params=pltpu.CompilerParams(vmem_limit_bytes=4 * MIB),
        name="last_add",
    )(*arrays)


def shifted(value, axis, steps, around=True):
    count = lax.axis_size(axis)
    pairs = [(i, (i + steps) % count) for i in range(count) if around or 0 <= i + steps < count]
    return lax.ppermute(value, axis, pairs)


def head_sum(parts):
    def right(value):
        return shifted(value, "head", 1)

    def left(value):
        return shifted(value, "head", -1)

    far, up_parts, down_parts, own = parts[0], parts[1:7:2], parts[2:7:2], parts[7]
    up = [right(far[0]), right(up_parts[0][1])]
    down = [left(down_parts[0][0]), left(far[1])]
    up = [right(add(up_parts[0][0], up[0])), up[1]]
    down = [down[0], left(add(down_parts[0][1], down[1]))]
    for step in (1, 2):
        for side in (1, 0):
            up[side] = right(add(up_parts[step][side], up[side]))
            down[1 - side] = left(add(down_parts[step][1 - side], down[1 - side]))
    early = [sum_call(own[0], down[0]), sum_call(own[1], up[1])]
    return last_call(*early, up[0], down[1])


def on_device(
    query_in, key_in, value_in, gate_in, log_gate, strength,
    query_conv, key_conv, value_conv, norm_gain, out_weight,
):
    z = lax.axis_index("head")
    order = [(z + shift) & 7 for shift in (4, 3, 5, 2, 6, 1, 7, 0)]
    place = jnp.stack(
        [lax.axis_index("ctx_0"), lax.axis_index("ctx_1"), lax.axis_index("ctx_2")] + order
    ).astype(jnp.int32)
    rim = shifted(rim_call(query_in, key_in, value_in), CTX, 1, around=False)
    vheads, tokens = log_gate.shape
    gates = jnp.concatenate(
        [
            log_gate.reshape(vheads, tokens // CHUNK, CHUNK),
            strength.reshape(vheads, tokens // CHUNK, CHUNK),
        ],
        axis=0,
    ).transpose(1, 0, 2)
    later = first_call(place, key_in, value_in, key_conv, value_conv, gates)
    keys, write, ends, solved, fresh, mine, other = local_call(
        place, key_in, value_in, key_conv, value_conv, rim, gates, later
    )
    other = shifted(other, "ctx_2", 1)
    half = vheads // 2
    maps = (half, WIDTH, 2 * WIDTH)
    states = (half, WIDTH, WIDTH)
    total, first = small_call(total_kernel, (maps, maps), (), "chip_total", place, mine, other)
    pairs, low, wide, mark = chain_call(
        solved, fresh, write, ends, later, query_in, query_conv, rim, gates, keys, first
    )
    row = [shifted(total, "ctx_1", k) for k in range(1, 4)]
    row_total, before = small_call(
        row_kernel, (maps, maps), ((4,) + maps, (4,) + maps), "row_total", place, total, *row, mark
    )
    rows = [shifted(row_total, "ctx_0", k, around=False) for k in range(1, 4)]
    low, wide, mark = read_call(
        query_in, query_conv, gates, later[0], pairs, low, wide, before
    )
    near, send = small_call(
        prefix_kernel, (states, states), ((4,) + maps, (4,) + states), "prefix",
        place, *rows, before, first, mark,
    )
    far = shifted(send, "ctx_2", 1)
    tail = (low, wide, near, far, gate_in, norm_gain, out_weight)
    parts = []
    for slots in ((0,), (1, 2), (3, 4), (5, 6, 7)):
        pieces = output_call(place, slots, *tail)
        parts += [pieces[2 * i : 2 * i + 2] for i in range(len(slots))]
    return head_sum(parts)


def solution(mesh):
    split = Mesh(
        mesh.devices.reshape(4, 4, 2, mesh.shape["head"]), ("ctx_0", "ctx_1", "ctx_2", "head")
    )
    in_specs = (
        P(CTX, "head", None),
        P(CTX, "head", None),
        P(CTX, "head", None),
        P(CTX, "head", None),
        P("head", CTX),
        P("head", CTX),
        P(None, "head", None),
        P(None, "head", None),
        P(None, "head", None),
        P(),
        P("head", None),
    )
    return jax.shard_map(
        on_device, mesh=split, in_specs=in_specs, out_specs=P(CTX_HEAD, None), check_vma=False
    )
```
